32 devices in a mesh: dp: 8 (over z, core), row: 2 (over x), col: 2 (over y).
Axes of the slice: x: 2, y: 2, z: 4, core: 2. Of those that a mesh axis runs over, the one named last changes fastest.
Arguments:
- tokens: bfloat16 [24576, 960], P(('dp', 'row'), 'col'), may hold values from -6 to 6
- doc_ids: int32 [32, 768], P(('dp', 'row', 'col')), may hold values from 0 to 5, never falling along the last dimension, each value on 1 to 384 neighbouring positions
- norm_gain: bfloat16 [960], replicated, may hold values from 0.5 to 1.5
- w_qkv: bfloat16 [960, 1600], P('row', 'col'), may hold values from -0.1875 to 0.1875
- w_out: bfloat16 [960, 960], P('row', 'col'), may hold values from -1 to 1
- ffn_gain: bfloat16 [960], replicated, may hold values from 0.5 to 1.5
- w_gate_up: bfloat16 [2, 960, 2560], P(None, 'row', 'col'), may hold values from -0.1875 to 0.1875
- w_down: bfloat16 [2560, 960], P('row', 'col'), may hold values from -0.125 to 0.125
- grad_out: bfloat16 [24576, 960], P(('dp', 'row'), 'col'), may hold values from -6 to 6
Outputs:
- out_tokens: bfloat16 [24576, 960], P(('dp', 'row'), 'col')
- grad_tokens: float32 [24576, 960], P(('dp', 'row'), 'col')
- grad_norm_gain: float32 [960], replicated
- grad_w_qkv: float32 [960, 1600], P('row', 'col')
- grad_w_out: float32 [960, 960], P('row', 'col')
- grad_ffn_gain: float32 [960], replicated
- grad_w_gate_up: float32 [2, 960, 2560], P(None, 'row', 'col')
- grad_w_down: float32 [2560, 960], P('row', 'col')
The draws below stay inside these ranges and needn't reach their ends.
Inputs may be any that keep to these rules, and one draw needn't show every extreme that they name: `doc_ids`: in each row (the tokens of one group) the sequence numbers never fall; each of the 6 sequences has 1 to 384 tokens and some sequence has exactly 384.
All inputs are finite; a program needn't handle non-finite values.
Results may differ from the reference program's by a relative error of at most 0.012.
Values may be sent and summed in bfloat16 or wider, within the bound.
A program may use at most 256 MiB of HBM per device.

```python
import math
import jax
import jax.numpy as jnp
import numpy as np
from jax import lax

D = 960
HEADS = 15
KV_HEADS = 5
HD = 64
FF = 2560
TOK_DEV = 768
SEQ_MAX = 384
SEQS_DEV = 6
TOKENS = 24576
QKVW = 1600
N_DP = 8
N_ROW = 2
N_COL = 2


def levels(stream_key, extent, shards, least, top_value):
    def one(dim, blocks):
        heights = jax.random.uniform(jax.random.fold_in(jax.random.fold_in(stream_key, 6), dim), (blocks,), jnp.float32, least / len(shards), top_value / len(shards))
        return jnp.repeat(jnp.exp(heights), extent[dim] // blocks).reshape((-1,) + (1,) * (len(extent) - dim - 1))

    gain = one(*shards[0])
    for cut in shards[1:]:
        gain = gain * one(*cut)
    return gain


def split_up(number_of, total, limit, skew):
    portions = [(1 << 20) // math.isqrt(rank ** skew) + 1 for rank in range(2, number_of + 1)]
    spare, holding = total - limit - (number_of - 1), [1] * (number_of - 1)
    while spare > 0:
        free = [i for i in range(number_of - 1) if holding[i] < limit]
        pool, budget = sum([portions[i] for i in free]), spare
        for i in free:
            addition = min(limit - holding[i], max(1, budget * portions[i] // pool), spare)
            holding[i] = holding[i] + addition
            spare = spare - addition
    return np.array([limit] + holding)


def uneven_parts(own_key, count, total, reach, lean):
    if count == 2:
        one = jax.random.randint(own_key, (), max(1, total - reach), min(reach, total - 1) + 1)
        return jnp.stack([one, total - one])
    tallies = jnp.asarray(split_up(count, total, reach, lean), jnp.int32)
    pairs = (count - 1) // 2
    source_of, receiver = tallies[1:1 + 2 * pairs:2], tallies[2:2 + 2 * pairs:2]
    room = jnp.minimum(source_of - 1, reach - receiver)
    passed = jax.random.randint(jax.random.fold_in(own_key, 1), (pairs,), 0, 1 << 20) % (room + 1)
    tallies = tallies.at[1:1 + 2 * pairs:2].set(source_of - passed).at[2:2 + 2 * pairs:2].set(receiver + passed)
    return tallies[jax.random.permutation(jax.random.fold_in(own_key, 2), count)]


def noise(own_key, extent, deviation, most, pieces=(), held_as=jnp.bfloat16):
    factor_of = levels(own_key, extent, pieces, -0.22, 0.18) if pieces else 1.0
    array = jax.random.normal(own_key, extent, jnp.float32) * deviation * factor_of
    return jnp.minimum(jnp.maximum(array, -most), most).astype(held_as)


def setup_inputs(seed: int = 0) -> dict:
    key_list = jax.random.split(jax.random.key(seed), 10)
    tokens = noise(key_list[0], (TOKENS, D), 1.0, 6.0, ((0, 16), (1, 2)))
    doc_ids = jax.vmap(lambda own: jnp.searchsorted(jnp.cumsum(uneven_parts(own, SEQS_DEV, TOK_DEV, SEQ_MAX, 2)), jnp.arange(TOK_DEV), side="right"))(jax.random.split(key_list[1], (N_DP * N_ROW * N_COL))).reshape((N_DP * N_ROW * N_COL, TOK_DEV)).astype(jnp.int32)
    norm_gain = jnp.clip(1.0 + 0.1 * jax.random.normal(key_list[2], (D,), jnp.float32), 0.5, 1.5).astype(jnp.bfloat16)
    w_qkv = noise(key_list[3], (D, QKVW), D ** -0.5, 0.1875, ((0, 2), (1, 2)))
    w_out = noise(key_list[4], (D, D), (max(D // 32, 1)) ** -0.5, 1.0, ((0, 2), (1, 2)))
    ffn_gain = jnp.clip(1.0 + 0.1 * jax.random.normal(key_list[5], (D,), jnp.float32), 0.5, 1.5).astype(jnp.bfloat16)
    w_gate_up = noise(key_list[6], (2, D, FF), D ** -0.5, 0.1875, ((1, 2), (2, 2)))
    w_down = noise(key_list[7], (FF, D), FF ** -0.5, 0.125, ((0, 2), (1, 2)))
    grad_out = noise(key_list[8], (TOKENS, D), 1.0, 6.0, ((0, 16), (1, 2)))
    return dict(tokens=tokens, doc_ids=doc_ids, norm_gain=norm_gain, w_qkv=w_qkv, w_out=w_out, ffn_gain=ffn_gain, w_gate_up=w_gate_up, w_down=w_down, grad_out=grad_out)


@jax.custom_vjp
def low(v):
    return lax.optimization_barrier(v.astype(jnp.bfloat16)).astype(jnp.float32)

@jax.custom_vjp
def low_back(v):
    return v

def low_keep(v):
    return (low(v), None)

def low_pass(kept, grad):
    return (grad,)

def back_keep(v):
    return (v, None)

def back_low(kept, grad):
    return (low(grad),)
low.defvjp(low_keep, low_pass)
low_back.defvjp(back_keep, back_low)

def frequencies(head_width):
    return jnp.exp(jnp.arange(head_width // 2, dtype=jnp.float32) * (-2.0 * math.log(10000.0) / head_width))

def rotate(values, angles, direction):
    row_count = values.shape[0]
    paired = values.reshape(row_count, values.shape[1], -1, 2)
    cosine = jnp.cos(angles)[:, None, :]
    sines = direction * jnp.sin(angles)[:, None, :]
    former = paired[..., 0]
    latter = paired[..., 1]
    turned = jnp.stack((former * cosine - latter * sines, former * sines + latter * cosine), axis=-1)
    return turned.reshape(values.shape)

def rms_scale(values):
    return lax.rsqrt(lax.optimization_barrier(jnp.mean(values * values, axis=-1, keepdims=True)) + 1e-05)

def slot_layer(inputs, doc_row, norm_gain, w_qkv, w_out, ffn_gain, w_gate_up, w_down):
    highest = lax.Precision.HIGHEST
    row_count = inputs.shape[0]
    position = jnp.arange(row_count, dtype=jnp.int32)
    first_index = lax.optimization_barrier(jnp.sum((doc_row[None, :] < doc_row[:, None]).astype(jnp.int32), axis=1))
    angles = (position - first_index).astype(jnp.float32)[:, None] * frequencies(HD)[None, :]
    normed_one = low(inputs * rms_scale(inputs) * norm_gain)
    projected = low_back(jnp.dot(normed_one, w_qkv, precision=highest))
    query_width = HEADS * HD
    pair_width = KV_HEADS * HD
    query_rows = low(rotate(projected[:, :query_width].reshape(row_count, HEADS, HD), angles, 1.0))
    key_rows = low(rotate(projected[:, query_width:query_width + pair_width].reshape(row_count, KV_HEADS, HD), angles, 1.0))
    value_rows = low(projected[:, query_width + pair_width:]).reshape(row_count, KV_HEADS, HD)
    allowed = (doc_row[:, None] == doc_row[None, :]) & (position[None, :] <= position[:, None])
    score_scale = HD ** (-0.5)

    def attend(query_block, key_block, value_block):
        scores = low_back(jnp.einsum('qhjd,khd->hjqk', query_block, key_block, precision=highest) * score_scale)
        shares = low(jax.nn.softmax(jnp.where(allowed, scores, -1e+30), axis=-1))
        return jnp.einsum('hjqk,khd->qhjd', shares, value_block, precision=highest)
    grouped = query_rows.reshape(row_count, KV_HEADS, HEADS // KV_HEADS, HD)
    blended = jax.checkpoint(attend)(grouped, key_rows, value_rows)
    attended = low_back(low(blended.reshape(row_count, query_width)))
    middle = inputs + low_back(jnp.dot(attended, w_out, precision=highest))
    normed_two = low(middle * rms_scale(middle) * ffn_gain)
    gate_up = jnp.einsum('ti,sij->stj', normed_two, w_gate_up, precision=highest)
    gate_rows = low_back(gate_up[0])
    up_rows = low_back(gate_up[1])
    hidden = low(gate_rows * jax.nn.sigmoid(gate_rows) * up_rows)
    return middle + jnp.dot(hidden, w_down, precision=highest)

def reference(tokens, doc_ids, norm_gain, w_qkv, w_out, ffn_gain, w_gate_up, w_down, grad_out):
    params = tuple((weight.astype(jnp.float32) for weight in (norm_gain, w_qkv, w_out, ffn_gain, w_gate_up, w_down)))
    groups = TOKENS // TOK_DEV
    slot_inputs = tokens.astype(jnp.float32).reshape(groups, TOK_DEV, D)
    slot_grads = grad_out.astype(jnp.float32).reshape(groups, TOK_DEV, D)

    def accumulate(totals, operands):
        inputs, doc_row, cotangent = operands

        def apply_layer(inputs_now, *weights):
            return slot_layer(inputs_now, doc_row, *weights)
        result, pullback = jax.vjp(apply_layer, inputs, *params)
        gradients = pullback(cotangent)
        summed = tuple((total_now + gradient for total_now, gradient in zip(totals, gradients[1:])))
        return (summed, (result.astype(jnp.bfloat16), gradients[0]))
    starting = tuple((jnp.zeros_like(weight) for weight in params))
    totals, (outputs, input_grads) = lax.scan(accumulate, starting, (slot_inputs, doc_ids, slot_grads))
    return (outputs.reshape(TOKENS, D), input_grads.reshape(TOKENS, D), totals[0], totals[1], totals[2], totals[3], totals[4], totals[5])
```

```python
import functools
import math

import jax
import jax.numpy as jnp
from jax import lax
from jax.experimental import pallas as pl
from jax.experimental.pallas import tpu as pltpu
from jax.sharding import PartitionSpec as P

HEADS = 15
KV_HEADS = 5
HD = 64
REP = HEADS // KV_HEADS
EPS = 1e-05
BF = jnp.bfloat16
F32 = jnp.float32
TB = 256
FB = 256
QB = 128
REACH = 384


def mm(a, b):
    return jnp.dot(a, b, preferred_element_type=F32)


def mm_nt(a, b):
    return lax.dot_general(a, b, (((1,), (1,)), ((), ())), preferred_element_type=F32)


def call(body, grid, ins, outs, scratch=(), flops=0, moved=0, prefetch=1):
    return pl.pallas_call(
        body,
        grid_spec=pltpu.PrefetchScalarGridSpec(
            num_scalar_prefetch=prefetch,
            grid=grid,
            in_specs=[pl.BlockSpec(block, index) for block, index in ins],
            out_specs=[pl.BlockSpec(block, index) for block, index, _, _ in outs],
            scratch_shapes=list(scratch),
        ),
        out_shape=[jax.ShapeDtypeStruct(shape, kind) for _, _, shape, kind in outs],
        compiler_params=pltpu.CompilerParams(
            dimension_semantics=("arbitrary",) * len(grid), vmem_limit_bytes=60 << 20
        ),
        cost_estimate=pl.CostEstimate(flops=flops, bytes_accessed=moved, transcendentals=0),
    )


def whole(shape):
    return (shape, lambda *_: (0,) * len(shape))


def swap_pairs(rows):
    count = rows.shape[0]
    after = pltpu.roll(rows, count - 1, 0)
    before = pltpu.roll(rows, 1, 0)
    even = lax.broadcasted_iota(jnp.int32, rows.shape, 0) % 2 == 0
    return jnp.where(even, after, before)


def flip(bit, static):
    return bit if static == 0 else 1 - bit


def project_body(at, own, other, gain, w, cos, sin, x, nt, qt, kt, vt, hold):
    col = at[1]
    width = own.shape[1]
    mine = own[...].astype(F32)
    theirs = other[...].astype(F32)
    square = jnp.sum(mine * mine, axis=1, keepdims=True) + jnp.sum(theirs * theirs, axis=1, keepdims=True)
    scale = lax.rsqrt(square / (2 * width) + EPS)
    x[col] = own[...]
    x[1 - col] = other[...]
    hold[col] = (mine * scale * gain[col]).astype(BF)
    hold[1 - col] = (theirs * scale * gain[1 - col]).astype(BF)
    low, high = hold[0], hold[1]
    nt[:width] = low.T
    nt[width:] = high.T
    half = w.shape[2]
    c, s = cos[...], sin[...]
    turned = KV_HEADS + HEADS
    rows = [None, None]
    for b in range(2):
        product = mm(low, w[b, :width]) + mm(high, w[b, width:])
        rows[b] = product.T
    flat = jnp.concatenate(rows, axis=0)
    for head in range(turned):
        part = flat[head * HD : (head + 1) * HD]
        part = part * c + swap_pairs(part) * s
        if head < HEADS:
            qt[head * HD : (head + 1) * HD] = (part.astype(BF).astype(F32) * HD**-0.5).astype(BF)
        else:
            kt[(head - HEADS) * HD : (head - HEADS + 1) * HD] = part.astype(BF)
    vt[...] = flat[turned * HD :].astype(BF)


def project(at, own, other, gain, w, cos, sin):
    tokens, width = own.shape
    feats, half = w.shape[1], w.shape[2]
    q, kv = HEADS * HD, KV_HEADS * HD
    return call(
        project_body,
        (tokens // TB,),
        [
            ((TB, width), lambda i, s: (i, 0)),
            ((TB, width), lambda i, s: (i, 0)),
            whole((2, 1, width)),
            whole(w.shape),
            ((HD, TB), lambda i, s: (0, i)),
            ((HD, TB), lambda i, s: (0, i)),
        ],
        [
            ((2, TB, width), lambda i, s: (0, i, 0), (2, tokens, width), BF),
            ((feats, TB), lambda i, s: (0, i), (feats, tokens), BF),
            ((q, TB), lambda i, s: (0, i), (q, tokens), BF),
            ((kv, TB), lambda i, s: (0, i), (kv, tokens), BF),
            ((kv, TB), lambda i, s: (0, i), (kv, tokens), BF),
        ],
        [pltpu.VMEM((2, TB, width), BF)],
        flops=4 * tokens * feats * half,
        moved=tokens * 8000,
    )(at, own, other, gain, w, cos, sin)


def blocks(tokens):
    for i in range(tokens // QB):
        first = max(0, i - REACH // QB)
        yield i, first * QB, (i + 1 - first) * QB


def fill_bias(drow, dcol, bias):
    for i, start, extent in blocks(drow.shape[1]):
        keys = lax.broadcasted_iota(jnp.int32, (extent, QB), 0) + start
        queries = lax.broadcasted_iota(jnp.int32, (extent, QB), 1) + i * QB
        same = dcol[start : start + extent, :] == drow[:, i * QB : (i + 1) * QB]
        bias[i, :extent] = jnp.where(same & (keys <= queries), 0.0, -1e30)


def side_by_side(ref, i):
    return jnp.concatenate([ref[j * HD : (j + 1) * HD, i * QB : (i + 1) * QB] for j in range(REP)], axis=1)


def attend_body(qt, kt, vt, drow, dcol, out, lse, bias):
    @pl.when(pl.program_id(0) == 0)
    def _():
        fill_bias(drow, dcol, bias)

    keys = kt[...].T
    for i, start, extent in blocks(kt.shape[1]):
        scores = mm(keys[start : start + extent], side_by_side(qt, i))
        scores = scores + jnp.concatenate([bias[i, :extent]] * REP, axis=1)
        top = jnp.max(scores, axis=0, keepdims=True)
        raised = jnp.exp(scores - top)
        total = jnp.sum(raised, axis=0, keepdims=True)
        shares = (raised * (1.0 / total)).astype(BF)
        blended = mm(vt[:, start : start + extent], shares).astype(BF)
        for j in range(REP):
            out[j * HD : (j + 1) * HD, i * QB : (i + 1) * QB] = blended[:, j * QB : (j + 1) * QB]
        lse[0, :, i * REP * QB : (i + 1) * REP * QB] = top + jnp.log(total)


def attend(qt, kt, vt, drow, dcol):
    tokens = qt.shape[1]
    return call(
        attend_body,
        (KV_HEADS,),
        [
            ((REP * HD, tokens), lambda g: (g, 0)),
            ((HD, tokens), lambda g: (g, 0)),
            ((HD, tokens), lambda g: (g, 0)),
            whole(drow.shape),
            whole(dcol.shape),
        ],
        [
            ((REP * HD, tokens), lambda g: (g, 0), qt.shape, BF),
            ((1, 1, REP * tokens), lambda g: (g, 0, 0), (KV_HEADS, 1, REP * tokens), F32),
        ],
        [pltpu.VMEM((tokens // QB, REACH + QB, QB), F32)],
        flops=HEADS * tokens * 512 * 256 * 4,
        moved=tokens * 6000,
        prefetch=0,
    )(qt, kt, vt, drow, dcol)


def attend_back_body(qt, kt, vt, dot, lse, drow, dcol, cos, sin, out, bias, dk, dv):
    group = pl.program_id(0)

    @pl.when(group == 0)
    def _():
        fill_bias(drow, dcol, bias)

    keys, values = kt[...].T, vt[...].T
    dk[...] = jnp.zeros_like(dk)
    dv[...] = jnp.zeros_like(dv)
    base = group * REP * HD
    for i, start, extent in blocks(kt.shape[1]):
        span = slice(start, start + extent)
        lanes = slice(i * QB, (i + 1) * QB)
        queries, upper = side_by_side(qt, i), side_by_side(dot, i)
        scores = mm(keys[span], queries)
        scores = scores + jnp.concatenate([bias[i, :extent]] * REP, axis=1)
        shares = jnp.exp(scores - lse[0, :, i * REP * QB : (i + 1) * REP * QB])
        dp = mm(values[span], upper)
        inner = jnp.sum(shares * dp, axis=0, keepdims=True)
        ds = (shares * (dp - inner)).astype(BF)
        dq = mm(kt[:, span], ds) * HD**-0.5
        dk[:, span] += mm_nt(queries, ds)
        dv[:, span] += mm_nt(upper, shares.astype(BF))
        c, s = cos[:, lanes], sin[:, lanes]
        for j in range(REP):
            part = dq[:, j * QB : (j + 1) * QB]
            part = part * c - swap_pairs(part) * s
            out[pl.ds(pl.multiple_of(base + j * HD, HD), HD), lanes] = part.astype(BF)
    part = dk[...]
    part = part * cos[...] - swap_pairs(part) * sin[...]
    out[pl.ds(pl.multiple_of((HEADS + group) * HD, HD), HD), :] = part.astype(BF)
    out[pl.ds(pl.multiple_of((HEADS + KV_HEADS + group) * HD, HD), HD), :] = dv[...].astype(BF)


def attend_back(qt, kt, vt, dot, lse, drow, dcol, cos, sin):
    tokens = qt.shape[1]
    rows = (HEADS + 2 * KV_HEADS) * HD
    return call(
        attend_back_body,
        (KV_HEADS,),
        [
            ((REP * HD, tokens), lambda g: (g, 0)),
            ((HD, tokens), lambda g: (g, 0)),
            ((HD, tokens), lambda g: (g, 0)),
            ((REP * HD, tokens), lambda g: (g, 0)),
            ((1, 1, REP * tokens), lambda g: (g, 0, 0)),
            whole(drow.shape),
            whole(dcol.shape),
            whole(cos.shape),
            whole(sin.shape),
        ],
        [whole((rows, tokens)) + ((rows, tokens), BF)],
        [
            pltpu.VMEM((tokens // QB, REACH + QB, QB), F32),
            pltpu.VMEM((HD, tokens), F32),
            pltpu.VMEM((HD, tokens), F32),
        ],
        flops=HEADS * tokens * 512 * 256 * 10,
        moved=tokens * 12000,
        prefetch=0,
    )(qt, kt, vt, dot, lse, drow, dcol, cos, sin)[0]


def mix_body(at, blended, x, w, gain, own, other, middle, n, nt, go, got):
    col = at[1]
    width = own.shape[1]
    attended = blended[...].T
    total = 0.0
    for b in range(2):
        part = x[b].astype(F32) + mm(attended, w[b])
        middle[b] = part
        total = total + jnp.sum(part * part, axis=1, keepdims=True)
    scale = lax.rsqrt(total / (2 * width) + EPS)
    go[col] = own[...]
    go[1 - col] = other[...]
    for b in range(2):
        rows = slice(b * width, (b + 1) * width)
        part = (middle[b] * scale * gain[b]).astype(BF)
        n[b] = part
        nt[rows] = part.T
        got[rows] = go[b].T


def mix(at, blended, x, w, gain, own, other):
    feats, tokens = blended.shape
    width = own.shape[1]
    rows = ((2, TB, width), lambda i, s: (0, i, 0))
    turned = ((feats, TB), lambda i, s: (0, i))
    flat = ((TB, width), lambda i, s: (i, 0))
    full = (2, tokens, width)
    return call(
        mix_body,
        (tokens // TB,),
        [turned, rows, whole(w.shape), whole((2, 1, width)), flat, flat],
        [
            rows + (full, F32),
            rows + (full, BF),
            turned + (blended.shape, BF),
            rows + (full, BF),
            turned + (blended.shape, BF),
        ],
        flops=2 * tokens * feats * feats,
        moved=tokens * 16000,
    )(at, blended, x, w, gain, own, other)


def gate_body(n, w, hidden, by_gate, by_up):
    width = n.shape[2]
    low, high = n[0], n[1]
    gate = mm(low, w[0, 0, :width]) + mm(high, w[0, 0, width:])
    up = mm(low, w[1, 0, :width]) + mm(high, w[1, 0, width:])
    sig = 1.0 / (1.0 + jnp.exp(-gate))
    act = gate * sig
    hidden[...] = (act * up).astype(BF)
    by_gate[...] = (up * sig * (1.0 + gate * (1.0 - sig))).astype(BF)
    by_up[...] = act.astype(BF)


def gate(n, w):
    tokens, width = n.shape[1:]
    half = w.shape[3]
    per = half // FB
    flat = ((tokens, FB), lambda j: (0, j), (tokens, 2 * half), BF)
    return call(
        gate_body,
        (2 * per,),
        [whole(n.shape), ((2, 1, 2 * width, FB), lambda j: (0, j // per, 0, j % per))],
        [flat, flat, flat],
        flops=16 * tokens * width * half,
        moved=tokens * half * 12 + w.size * 2,
        prefetch=0,
    )(n, w)


def down_body(at, hidden, by_gate, by_up, w, go, middle, d_gate, d_up, keep, send, total):
    @pl.when(pl.program_id(0) == 0)
    def _():
        total[...] = middle[...]

    back = mm_nt(go[0], w[0]) + mm_nt(go[1], w[1])
    d_gate[...] = (back * by_gate[...].astype(F32)).astype(BF)
    d_up[...] = (back * by_up[...].astype(F32)).astype(BF)
    for b in range(2):
        total[b] += mm(hidden[...], w[b])

    @pl.when(pl.program_id(0) == pl.num_programs(0) - 1)
    def _():
        keep[...] = total[at[1]].astype(BF)
        send[...] = total[1 - at[1]].astype(BF)


def down(at, hidden, by_gate, by_up, w, go, middle):
    tokens, units = hidden.shape
    width = w.shape[2]
    flat = ((tokens, FB), lambda j, s: (0, j))
    return call(
        down_body,
        (units // FB,),
        [flat, flat, flat, ((2, FB, width), lambda j, s: (0, j, 0)), whole(go.shape), whole(middle.shape)],
        [
            flat + (hidden.shape, BF),
            flat + (hidden.shape, BF),
            whole((tokens, width)) + ((tokens, width), BF),
            whole((tokens, width)) + ((tokens, width), BF),
        ],
        [pltpu.VMEM(middle.shape, F32)],
        flops=8 * tokens * width * units,
        moved=tokens * units * 10 + w.size * 2 + tokens * width * 14,
    )(at, hidden, by_gate, by_up, w, go, middle)


def norm_back_body(d_gate, d_up, w, middle, go, gain, d_middle, d_branch, d_gain, total):
    width = middle.shape[2]

    @pl.when(pl.program_id(0) == 0)
    def _():
        total[...] = jnp.zeros_like(total)

    for a in range(2):
        rows = slice(a * width, (a + 1) * width)
        total[a] += mm_nt(d_gate[...], w[0, 0, rows]) + mm_nt(d_up[...], w[1, 0, rows])

    @pl.when(pl.program_id(0) == pl.num_programs(0) - 1)
    def _():
        square, inner = 0.0, 0.0
        for b in range(2):
            m = middle[b]
            square = square + jnp.sum(m * m, axis=1, keepdims=True)
            inner = inner + jnp.sum(total[b] * gain[b] * m, axis=1, keepdims=True)
        scale = lax.rsqrt(square / (2 * width) + EPS)
        inner = scale * scale * scale * inner / (2 * width)
        for b in range(2):
            m = middle[b]
            out = go[b].astype(F32) + (scale * (total[b] * gain[b]) - m * inner)
            d_middle[b] = out
            d_branch[b] = out.astype(BF)
            d_gain[b] = jnp.sum(total[b] * m * scale, axis=0, keepdims=True)


def norm_back(d_gate, d_up, w, middle, go, gain):
    tokens, units = d_gate.shape
    width = middle.shape[2]
    per = units // 2 // FB
    flat = ((tokens, FB), lambda j: (0, j))
    full = middle.shape
    return call(
        norm_back_body,
        (units // FB,),
        [
            flat,
            flat,
            ((2, 1, 2 * width, FB), lambda j: (0, j // per, 0, j % per)),
            whole(full),
            whole(full),
            whole((2, 1, width)),
        ],
        [whole(full) + (full, F32), whole(full) + (full, BF), whole((2, 1, width)) + ((2, 1, width), F32)],
        [pltpu.VMEM(full, F32)],
        flops=8 * tokens * width * units,
        moved=tokens * units * 4 + w.size * 2 + tokens * width * 24,
        prefetch=0,
    )(d_gate, d_up, w, middle, go, gain)


def place(keep, send, core, h, put):
    @pl.when(core == h)
    def _():
        put(keep)

    @pl.when(core != h)
    def _():
        put(send)


def weight_grad_body(at, xt, dy, keep, send, *, row_first):
    rows = keep.shape[2]
    product = mm(xt[...], dy[...]).astype(BF)
    for a in range(2):
        where = flip(at[0], a)
        for h in range(2):
            q = (2 * a + h) * rows
            piece = product[q : q + rows]

            def put(ref, where=where, piece=piece):
                if row_first:
                    ref[where, 0] = piece
                else:
                    ref[0, where] = piece

            place(keep, send, at[2], h, put)


def weight_grad(at, xt, dy, row_first):
    feats, tokens = xt.shape
    units = dy.shape[1]
    per = units // 2 // FB
    shape = (2, 2, feats // 4, units // 2)
    if row_first:
        spec = ((2, 1, feats // 4, FB), lambda j, s: (0, (j // per) ^ s[1], 0, j % per), shape, BF)
    else:
        spec = ((1, 2, feats // 4, FB), lambda j, s: ((j // per) ^ s[1], 0, 0, j % per), shape, BF)
    return call(
        functools.partial(weight_grad_body, row_first=row_first),
        (units // FB,),
        [whole(xt.shape), ((tokens, FB), lambda j, s: (0, j))],
        [spec, spec],
        flops=2 * tokens * feats * units,
        moved=tokens * (units + feats) * 2 + feats * units * 2,
    )(at, xt, dy)


def last_grad_body(at, nt, dproj, blended, d_branch, gains, keep, send):
    rows = nt.shape[0] // 4
    half = dproj.shape[0] // 2
    for b in range(2):
        where_b = flip(at[1], b)
        first = mm_nt(nt[...], dproj[b * half : (b + 1) * half]).astype(BF)
        second = mm(blended[...], d_branch[b]).astype(BF)
        for a in range(2):
            where_a = flip(at[0], a)
            for h in range(2):
                q = (2 * a + h) * rows

                def put(ref, q=q, where_a=where_a, where_b=where_b, first=first, second=second):
                    ref[where_b, where_a, :rows, :half] = first[q : q + rows]
                    ref[where_b, where_a, :rows, half:] = second[q : q + rows]
                    ref[where_b, where_a, rows:] = gains[...]

                place(keep, send, at[2], h, put)


def last_grad(at, nt, dproj, blended, d_branch, gains):
    feats, tokens = nt.shape
    cols = dproj.shape[0] // 2 + d_branch.shape[2]
    shape = (2, 2, feats // 4 + gains.shape[0], cols)
    return call(
        last_grad_body,
        (1,),
        [whole(v.shape) for v in (nt, dproj, blended, d_branch, gains)],
        [whole(shape) + (shape, BF)] * 2,
        flops=4 * tokens * feats * cols,
        moved=4 * tokens * feats * 3 + 8 * feats * cols,
    )(at, nt, dproj, blended, d_branch, gains)


def branch_back_body(w, d_branch, out):
    out[...] = (mm_nt(w[0], d_branch[0]) + mm_nt(w[1], d_branch[1])).astype(BF)


def branch_back(w, d_branch):
    feats = w.shape[1]
    tokens = d_branch.shape[1]
    step = feats // 3
    return call(
        branch_back_body,
        (3,),
        [((2, step, w.shape[2]), lambda i: (0, i, 0)), whole(d_branch.shape)],
        [((step, tokens), lambda i: (i, 0), (feats, tokens), BF)],
        flops=2 * tokens * feats * feats,
        moved=tokens * feats * 4 + w.size * 2,
        prefetch=0,
    )(w, d_branch)[0]


def input_back_body(at, dproj, w, x, d_middle, gain, keep, send, d_gain, hold):
    col = at[1]
    width = x.shape[2]
    half = w.shape[2]

    @pl.when(pl.program_id(0) == 0)
    def _():
        d_gain[...] = jnp.zeros_like(d_gain)

    square, inner = 0.0, 0.0
    for b in range(2):
        rows = slice(b * width, (b + 1) * width)
        turned = mm(w[0, rows], dproj[:half]) + mm(w[1, rows], dproj[half:])
        hold[b] = turned.T
        v = x[b].astype(F32)
        square = square + jnp.sum(v * v, axis=1, keepdims=True)
        inner = inner + jnp.sum(hold[b] * gain[b] * v, axis=1, keepdims=True)
    scale = lax.rsqrt(square / (2 * width) + EPS)
    inner = scale * scale * scale * inner / (2 * width)
    for b in range(2):
        v = x[b].astype(F32)
        d_gain[b] += jnp.sum(hold[b] * v * scale, axis=0, keepdims=True)
        hold[b] = d_middle[b] + (scale * (hold[b] * gain[b]) - v * inner)
    keep[...] = hold[col]
    send[...] = hold[1 - col].astype(BF)


def input_back(at, dproj, w, x, d_middle, gain):
    tokens, width = x.shape[1:]
    rows = ((2, TB, width), lambda i, s: (0, i, 0))
    flat = ((TB, width), lambda i, s: (i, 0))
    return call(
        input_back_body,
        (tokens // TB,),
        [
            ((dproj.shape[0], TB), lambda i, s: (0, i)),
            whole(w.shape),
            rows,
            rows,
            whole((2, 1, width)),
        ],
        [
            flat + ((tokens, width), F32),
            flat + ((tokens, width), BF),
            whole((2, 1, width)) + ((2, 1, width), F32),
        ],
        [pltpu.VMEM((2, TB, width), F32)],
        flops=2 * w.size * tokens,
        moved=tokens * 16000 + w.size * 2,
    )(at, dproj, w, x, d_middle, gain)


def add(a, b):
    return lax.optimization_barrier((a.astype(F32) + b.astype(F32)).astype(BF))


def shards(tokens, doc_ids, norm_gain, w_qkv, w_out, ffn_gain, w_gate_up, w_down, grad_out):
    row, col, dp = (lax.axis_index(name) for name in ("row", "col", "dp"))
    core, line = dp % 2, dp // 2
    lines = lax.axis_size("dp") // 2
    at = jnp.stack((row, col, core)).astype(jnp.int32)
    at_turned = jnp.stack((col, row, core)).astype(jnp.int32)
    pairs = [(0, 1), (1, 0)]

    def over_x(v):
        return lax.ppermute(v, "row", pairs)

    def over_y(v):
        return lax.ppermute(v, "col", pairs)

    def over_core(v):
        return lax.ppermute(v, "dp", [(i, i ^ 1) for i in range(2 * lines)])

    def along(v, moves):
        return lax.ppermute(v, "dp", [(2 * a + c, 2 * b + c) for a, b in moves for c in (0, 1)])

    def rows_of(v, index, count):
        return lax.dynamic_slice_in_dim(v, index * count, count, 0)

    group = tokens.shape[0] // 2
    width = tokens.shape[1]

    def spread(cell, mine, lead, last_over_x):
        across, beside = over_x(mine), over_y(mine)
        corner = over_x(beside) if last_over_x else over_y(across)
        places = ((across, 1 - row, col), (beside, row, 1 - col), (corner, 1 - row, 1 - col))
        full = cell
        for part, r, c in places:
            spot = lead(core, r, c)
            full = lax.dynamic_update_slice(full, part.reshape((1,) * (full.ndim - 2) + part.shape), spot)
        for part, r, c in places:
            spot = lead(1 - core, r, c)
            part = over_core(part)
            full = lax.dynamic_update_slice(full, part.reshape((1,) * (full.ndim - 2) + part.shape), spot)
        return full

    def gather(w, last_over_x):
        half = w.shape[0] // 2
        cell = lax.dynamic_update_slice(
            jnp.zeros((2, 2, 2, half, w.shape[1]), w.dtype), w.reshape(1, 1, 2, half, -1), (col, row, 0, 0, 0)
        )
        full = spread(cell, rows_of(w, core, half), lambda k, r, c: (c, r, k, 0, 0), last_over_x)
        return full.reshape(2, 4 * half, w.shape[1])

    def gather_pair(w, last_over_x):
        cell = lax.dynamic_update_slice(
            jnp.zeros((2, 2, 2) + w.shape[1:], w.dtype), w[:, None, None], (0, col, row, 0, 0)
        )
        full = spread(
            cell,
            lax.dynamic_index_in_dim(w, core, 0, keepdims=False),
            lambda k, r, c: (k, c, r, 0, 0),
            last_over_x,
        )
        return full.reshape(2, 2, 2 * w.shape[1], w.shape[2])

    x_own = rows_of(tokens, col, group)
    x_other = over_y(rows_of(tokens, 1 - col, group))
    qkv = gather(w_qkv, True)
    go_own = rows_of(grad_out, col, group)
    go_other = over_y(rows_of(grad_out, 1 - col, group))
    out_w = gather(w_out, True)
    gate_up = gather_pair(w_gate_up, True)
    down_w = gather(w_down, False)

    gain_one = norm_gain.astype(F32).reshape(2, 1, width)
    gain_two = ffn_gain.astype(F32).reshape(2, 1, width)
    doc = doc_ids[0]
    first = jnp.sum((doc[None, :] < doc[:, None]).astype(jnp.int32), axis=1)
    place_in = (jnp.arange(group, dtype=jnp.int32) - first).astype(F32)
    rate = jnp.exp(jnp.arange(HD // 2, dtype=F32) * (-2.0 * math.log(10000.0) / HD))
    angles = jnp.repeat(rate, 2)[:, None] * place_in[None, :]
    sign = jnp.where(jnp.arange(HD) % 2 == 0, -1.0, 1.0).astype(F32)[:, None]
    cos, sin = jnp.cos(angles), jnp.sin(angles) * sign
    drow, dcol = doc.reshape(1, group), jnp.broadcast_to(doc[:, None], (group, QB))

    x, nt, qt, kt, vt = project(at, x_own, x_other, gain_one, qkv, cos, sin)
    blended, lse = attend(qt, kt, vt, drow, dcol)
    middle, n2, n2t, go, got = mix(at, blended, x, out_w, gain_two, go_own, go_other)
    hidden, by_gate, by_up = gate(n2, gate_up)

    def fold(keep, send, one, two):
        near = over_core(send)
        far = one(add(keep[1], near[1]))
        kept = add(keep[0], near[0])
        beyond = two(add(kept[1], far[1]))
        total = add(add(kept[0], far[0]), beyond)
        for step in range(lines // 2 - 1):
            total = add(total, along(total, [(step, step + 1), (lines - 1 - step, lines - 2 - step)]))
        if lines > 1:
            total = add(total, along(total, [(lines // 2 - 1, lines // 2), (lines // 2, lines // 2 - 1)]))
        for step in reversed(range(lines // 2 - 1)):
            came = along(total, [(step + 1, step), (lines - 2 - step, lines - 1 - step)])
            total = jnp.where((line == step) | (line == lines - 1 - step), came, total)
        return total, over_core(total)

    def join(own, other, rows):
        own, other = own[:rows].astype(F32), other[:rows].astype(F32)
        return jnp.where(
            core == 0, jnp.concatenate((own, other), axis=0), jnp.concatenate((other, own), axis=0)
        )

    down_parts = fold(*weight_grad(at_turned, got, hidden, False), over_x, over_y)
    d_gate, d_up, y_keep, y_send = down(at, hidden, by_gate, by_up, down_w, go, middle)
    gate_parts = fold(*weight_grad(at, n2t, d_gate, True), over_x, over_y)
    up_parts = fold(*weight_grad(at, n2t, d_up, False), over_y, over_x)
    y_came = over_y(y_send)
    d_middle, d_branch, gain_two_grad = norm_back(d_gate, d_up, gate_up, middle, go, gain_two)
    dot = branch_back(out_w, d_branch)
    dproj = attend_back(qt, kt, vt, dot, lse, drow, dcol, cos, sin)
    g_keep, g_send, gain_one_grad = input_back(at, dproj, qkv, x, d_middle, gain_one)
    g_came = over_y(g_send)
    gains = jnp.concatenate((gain_one_grad.reshape(2, width), gain_two_grad.reshape(2, width)), axis=0)
    cols = w_qkv.shape[1] + w_out.shape[1]
    gains = jnp.pad(gains, ((0, 12), (0, cols - width))).astype(BF)
    last_parts = fold(*last_grad(at, nt, dproj, blended, d_branch, gains), over_y, over_x)

    quarter = w_qkv.shape[0] // 2
    last = join(*last_parts, quarter)
    gain_rows = last_parts[0][quarter : quarter + 4, :width].astype(F32)

    def both_rows(own, other):
        return jnp.where(
            col == 0, jnp.concatenate((own, other), axis=0), jnp.concatenate((other, own), axis=0)
        )

    return (
        both_rows(y_keep, y_came),
        both_rows(g_keep, g_came.astype(F32)),
        gain_rows[:2].reshape(-1),
        last[:, : w_qkv.shape[1]],
        last[:, w_qkv.shape[1] :],
        gain_rows[2:].reshape(-1),
        jnp.stack((join(*gate_parts, quarter), join(*up_parts, quarter))),
        join(*down_parts, quarter).T,
    )


def solution(mesh):
    placed = (
        P(("dp", "row"), "col"),
        P(("dp", "row", "col"), None),
        P(),
        P("row", "col"),
        P("row", "col"),
        P(),
        P(None, "row", "col"),
        P("row", "col"),
        P(("dp", "row"), "col"),
    )
    return jax.shard_map(
        shards,
        mesh=mesh,
        in_specs=placed,
        out_specs=(
            P(("dp", "row"), "col"),
            P(("dp", "row"), "col"),
            P(),
            P("row", "col"),
            P("row", "col"),
            P(),
            P(None, "row", "col"),
            P("row", "col"),
        ),
        check_vma=False,
    )
```

```python
import functools
import math

import jax
import jax.numpy as jnp
from jax import lax
from jax.experimental import pallas as pl
from jax.experimental.pallas import tpu as pltpu
from jax.sharding import PartitionSpec as P

HEADS = 15
KV_HEADS = 5
HD = 64
REP = HEADS // KV_HEADS
EPS = 1e-05
BF = jnp.bfloat16
F32 = jnp.float32
TB = 256
FB = 256
QB = 128
REACH = 384
MESH = pl.DeviceIdType.MESH
ANY = pl.BlockSpec(memory_space=pl.ANY)


def mm(a, b):
    return jnp.dot(a, b, preferred_element_type=F32)


def mm_nt(a, b):
    return lax.dot_general(a, b, (((1,), (1,)), ((), ())), preferred_element_type=F32)


def call(body, grid, ins, outs, scratch=(), flops=0, moved=0, prefetch=1):
    return pl.pallas_call(
        body,
        grid_spec=pltpu.PrefetchScalarGridSpec(
            num_scalar_prefetch=prefetch,
            grid=grid,
            in_specs=[pl.BlockSpec(block, index) for block, index in ins],
            out_specs=[pl.BlockSpec(block, index) for block, index, _, _ in outs],
            scratch_shapes=list(scratch),
        ),
        out_shape=[jax.ShapeDtypeStruct(shape, kind) for _, _, shape, kind in outs],
        compiler_params=pltpu.CompilerParams(
            dimension_semantics=("arbitrary",) * len(grid), vmem_limit_bytes=60 << 20
        ),
        cost_estimate=pl.CostEstimate(flops=flops, bytes_accessed=moved, transcendentals=0),
    )


def whole(shape):
    return (shape, lambda *_: (0,) * len(shape))


def columns(rows, step=TB):
    return ((rows, step), lambda i, *_: (0, i))


def swap_pairs(rows):
    count = rows.shape[0]
    after = pltpu.roll(rows, count - 1, 0)
    before = pltpu.roll(rows, 1, 0)
    even = lax.broadcasted_iota(jnp.int32, rows.shape, 0) % 2 == 0
    return jnp.where(even, after, before)


def flip(bit, static):
    return bit if static == 0 else 1 - bit


def project_body(x, gain, w, cos, sin, nt, qt, kt, vt):
    feats = x.shape[0]
    v = x[...].astype(F32)
    square = jnp.sum(v * v, axis=0, keepdims=True)
    scale = lax.rsqrt(square / feats + EPS)
    normed = (v * scale * gain[...]).astype(BF)
    nt[...] = normed
    half = feats // 2
    flat = mm(w[0], normed[:half]) + mm(w[1], normed[half:])
    c, s = cos[...], sin[...]
    turned = KV_HEADS + HEADS
    for head in range(turned):
        part = flat[head * HD : (head + 1) * HD]
        part = part * c + swap_pairs(part) * s
        if head < HEADS:
            qt[head * HD : (head + 1) * HD] = (part.astype(BF).astype(F32) * HD**-0.5).astype(BF)
        else:
            kt[(head - HEADS) * HD : (head - HEADS + 1) * HD] = part.astype(BF)
    vt[...] = flat[turned * HD :].astype(BF)


def project(x, gain, w, cos, sin):
    feats, tokens = x.shape
    q, kv = HEADS * HD, KV_HEADS * HD
    return call(
        project_body,
        (tokens // TB,),
        [columns(feats), whole(gain.shape), whole(w.shape), columns(HD), columns(HD)],
        [columns(n) + ((n, tokens), BF) for n in (feats, q, kv, kv)],
        flops=2 * tokens * w.size,
        moved=tokens * 7000 + w.size * 2,
        prefetch=0,
    )(x, gain, w, cos, sin)


def blocks(tokens):
    for i in range(tokens // QB):
        first = max(0, i - REACH // QB)
        yield i, first * QB, (i + 1 - first) * QB


def fill_bias(drow, dcol, bias):
    for i, start, extent in blocks(drow.shape[1]):
        keys = lax.broadcasted_iota(jnp.int32, (extent, QB), 0) + start
        queries = lax.broadcasted_iota(jnp.int32, (extent, QB), 1) + i * QB
        same = dcol[start : start + extent, :] == drow[:, i * QB : (i + 1) * QB]
        bias[i, :extent] = jnp.where(same & (keys <= queries), 0.0, -1e30)


def side_by_side(ref, i):
    return jnp.concatenate([ref[j * HD : (j + 1) * HD, i * QB : (i + 1) * QB] for j in range(REP)], axis=1)


def attend_body(qt, kt, vt, drow, dcol, out, lse, bias):
    @pl.when(pl.program_id(0) == 0)
    def _():
        fill_bias(drow, dcol, bias)

    keys = kt[...].T
    for i, start, extent in blocks(kt.shape[1]):
        scores = mm(keys[start : start + extent], side_by_side(qt, i))
        scores = scores + jnp.concatenate([bias[i, :extent]] * REP, axis=1)
        top = jnp.max(scores, axis=0, keepdims=True)
        raised = jnp.exp(scores - top)
        total = jnp.sum(raised, axis=0, keepdims=True)
        shares = (raised * (1.0 / total)).astype(BF)
        blended = mm(vt[:, start : start + extent], shares).astype(BF)
        for j in range(REP):
            out[j * HD : (j + 1) * HD, i * QB : (i + 1) * QB] = blended[:, j * QB : (j + 1) * QB]
        lse[0, :, i * REP * QB : (i + 1) * REP * QB] = top + jnp.log(total)


def attend(qt, kt, vt, drow, dcol):
    tokens = qt.shape[1]
    return call(
        attend_body,
        (KV_HEADS,),
        [
            ((REP * HD, tokens), lambda g: (g, 0)),
            ((HD, tokens), lambda g: (g, 0)),
            ((HD, tokens), lambda g: (g, 0)),
            whole(drow.shape),
            whole(dcol.shape),
        ],
        [
            ((REP * HD, tokens), lambda g: (g, 0), qt.shape, BF),
            ((1, 1, REP * tokens), lambda g: (g, 0, 0), (KV_HEADS, 1, REP * tokens), F32),
        ],
        [pltpu.VMEM((tokens // QB, REACH + QB, QB), F32)],
        flops=HEADS * tokens * 512 * 256 * 4,
        moved=tokens * 6000,
        prefetch=0,
    )(qt, kt, vt, drow, dcol)


def attend_back_body(qt, kt, vt, dot, lse, drow, dcol, cos, sin, out, bias, dk, dv):
    group = pl.program_id(0)

    @pl.when(group == 0)
    def _():
        fill_bias(drow, dcol, bias)

    keys, values = kt[...].T, vt[...].T
    dk[...] = jnp.zeros_like(dk)
    dv[...] = jnp.zeros_like(dv)
    base = group * REP * HD
    for i, start, extent in blocks(kt.shape[1]):
        span = slice(start, start + extent)
        lanes = slice(i * QB, (i + 1) * QB)
        queries, upper = side_by_side(qt, i), side_by_side(dot, i)
        scores = mm(keys[span], queries)
        scores = scores + jnp.concatenate([bias[i, :extent]] * REP, axis=1)
        shares = jnp.exp(scores - lse[0, :, i * REP * QB : (i + 1) * REP * QB])
        dp = mm(values[span], upper)
        inner = jnp.sum(shares * dp, axis=0, keepdims=True)
        ds = (shares * (dp - inner)).astype(BF)
        dq = mm(kt[:, span], ds) * HD**-0.5
        dk[:, span] += mm_nt(queries, ds)
        dv[:, span] += mm_nt(upper, shares.astype(BF))
        c, s = cos[:, lanes], sin[:, lanes]
        for j in range(REP):
            part = dq[:, j * QB : (j + 1) * QB]
            part = part * c - swap_pairs(part) * s
            out[pl.ds(pl.multiple_of(base + j * HD, HD), HD), lanes] = part.astype(BF)
    part = dk[...]
    part = part * cos[...] - swap_pairs(part) * sin[...]
    out[pl.ds(pl.multiple_of((HEADS + group) * HD, HD), HD), :] = part.astype(BF)
    out[pl.ds(pl.multiple_of((HEADS + KV_HEADS + group) * HD, HD), HD), :] = dv[...].astype(BF)


def attend_back(qt, kt, vt, dot, lse, drow, dcol, cos, sin):
    tokens = qt.shape[1]
    rows = (HEADS + 2 * KV_HEADS) * HD
    return call(
        attend_back_body,
        (KV_HEADS,),
        [
            ((REP * HD, tokens), lambda g: (g, 0)),
            ((HD, tokens), lambda g: (g, 0)),
            ((HD, tokens), lambda g: (g, 0)),
            ((REP * HD, tokens), lambda g: (g, 0)),
            ((1, 1, REP * tokens), lambda g: (g, 0, 0)),
            whole(drow.shape),
            whole(dcol.shape),
            whole(cos.shape),
            whole(sin.shape),
        ],
        [whole((rows, tokens)) + ((rows, tokens), BF)],
        [
            pltpu.VMEM((tokens // QB, REACH + QB, QB), F32),
            pltpu.VMEM((HD, tokens), F32),
            pltpu.VMEM((HD, tokens), F32),
        ],
        flops=HEADS * tokens * 512 * 256 * 10,
        moved=tokens * 12000,
        prefetch=0,
    )(qt, kt, vt, dot, lse, drow, dcol, cos, sin)[0]


def mix_body(blended, x, w, gain, go_t, middle, nt, n, go, turned):
    feats = x.shape[0]
    half = feats // 2

    @pl.when(pl.program_id(0) == 0)
    def _():
        turned[:half] = w[0].T
        turned[half:] = w[1].T

    m = x[...].astype(F32) + mm(turned[...], blended[...])
    middle[...] = m
    scale = lax.rsqrt(jnp.sum(m * m, axis=0, keepdims=True) / feats + EPS)
    normed = (m * scale * gain[...]).astype(BF)
    nt[...] = normed
    n[...] = normed.T
    go[...] = go_t[...].T


def mix(blended, x, w, gain, go_t):
    feats, tokens = x.shape
    rows = ((TB, feats), lambda i: (i, 0))
    return call(
        mix_body,
        (tokens // TB,),
        [columns(feats), columns(feats), whole(w.shape), whole(gain.shape), columns(feats)],
        [
            columns(feats) + (x.shape, F32),
            columns(feats) + (x.shape, BF),
            rows + ((tokens, feats), BF),
            rows + ((tokens, feats), BF),
        ],
        [pltpu.VMEM((feats, feats), BF)],
        flops=2 * tokens * feats * feats,
        moved=tokens * 16000,
        prefetch=0,
    )(blended, x, w, gain, go_t)


def gate_body(n, w, hidden, by_gate, by_up):
    gate = mm(n[...], w[0, 0])
    up = mm(n[...], w[1, 0])
    sig = 1.0 / (1.0 + jnp.exp(-gate))
    act = gate * sig
    hidden[...] = (act * up).astype(BF)
    by_gate[...] = (up * sig * (1.0 + gate * (1.0 - sig))).astype(BF)
    by_up[...] = act.astype(BF)


def gate(n, w):
    tokens, feats = n.shape
    half = w.shape[3]
    per = half // FB
    flat = ((tokens, FB), lambda j: (0, j), (tokens, 2 * half), BF)
    return call(
        gate_body,
        (2 * per,),
        [whole(n.shape), ((2, 1, feats, FB), lambda j: (0, j // per, 0, j % per))],
        [flat, flat, flat],
        flops=8 * tokens * feats * half,
        moved=tokens * half * 12 + w.size * 2,
        prefetch=0,
    )(n, w)


def down_body(at, hidden, by_gate, by_up, w, go, middle, d_gate, d_up, keep, send, total):
    @pl.when(pl.program_id(0) == 0)
    def _():
        total[...] = middle[...]

    back = mm(go[...], w[0])
    d_gate[...] = (back * by_gate[...].astype(F32)).astype(BF)
    d_up[...] = (back * by_up[...].astype(F32)).astype(BF)
    total[...] += mm_nt(w[0], hidden[...])

    @pl.when(pl.program_id(0) == pl.num_programs(0) - 1)
    def _():
        width = keep.shape[0]
        keep[...] = total[pl.ds(pl.multiple_of(at[1] * width, 16), width), :].astype(BF)
        send[...] = total[pl.ds(pl.multiple_of((1 - at[1]) * width, 16), width), :].astype(BF)


def down(at, hidden, by_gate, by_up, w, go, middle):
    tokens, units = hidden.shape
    feats = w.shape[1]
    per = units // 2 // FB
    flat = ((tokens, FB), lambda j, s: (0, j))
    own = whole((feats // 2, tokens)) + ((feats // 2, tokens), BF)
    return call(
        down_body,
        (units // FB,),
        [
            flat,
            flat,
            flat,
            ((1, feats, FB), lambda j, s: (j // per, 0, j % per)),
            whole(go.shape),
            whole(middle.shape),
        ],
        [flat + (hidden.shape, BF), flat + (hidden.shape, BF), own, own],
        [pltpu.VMEM(middle.shape, F32)],
        flops=4 * tokens * feats * units,
        moved=tokens * units * 10 + w.size * 2 + tokens * feats * 10,
    )(at, hidden, by_gate, by_up, w, go, middle)


def norm_back_body(d_gate, d_up, w, middle, go, gain, d_middle, d_branch, d_gain, total):
    feats = middle.shape[0]

    @pl.when(pl.program_id(0) == 0)
    def _():
        total[...] = jnp.zeros_like(total)

    total[...] += mm_nt(w[0, 0], d_gate[...]) + mm_nt(w[1, 0], d_up[...])

    @pl.when(pl.program_id(0) == pl.num_programs(0) - 1)
    def _():
        m, u = middle[...], total[...]
        scale = lax.rsqrt(jnp.sum(m * m, axis=0, keepdims=True) / feats + EPS)
        weighted = u * gain[...]
        inner = jnp.sum(weighted * m, axis=0, keepdims=True) / feats
        out = go[...].astype(F32) + (scale * weighted - m * (scale * scale * scale * inner))
        d_middle[...] = out
        d_branch[...] = out.astype(BF)
        d_gain[...] = jnp.sum(u * m * scale, axis=1, keepdims=True)


def norm_back(d_gate, d_up, w, middle, go, gain):
    tokens, units = d_gate.shape
    feats = middle.shape[0]
    per = units // 2 // FB
    flat = ((tokens, FB), lambda j: (0, j))
    full = middle.shape
    return call(
        norm_back_body,
        (units // FB,),
        [
            flat,
            flat,
            ((2, 1, feats, FB), lambda j: (0, j // per, 0, j % per)),
            whole(full),
            whole(full),
            whole(gain.shape),
        ],
        [whole(full) + (full, F32), whole(full) + (full, BF), whole(gain.shape) + (gain.shape, F32)],
        [pltpu.VMEM(full, F32)],
        flops=4 * tokens * feats * units,
        moved=tokens * units * 4 + w.size * 2 + tokens * feats * 12,
        prefetch=0,
    )(d_gate, d_up, w, middle, go, gain)


def place(keep, send, core, h, put):
    @pl.when(core == h)
    def _():
        put(keep)

    @pl.when(core != h)
    def _():
        put(send)


def weight_grad_body(at, xt, dy, keep, send, *, rows_over_x):
    rows = keep.shape[2]
    product = mm(xt[...], dy[...]).astype(BF)
    for a in range(2):
        where = flip(at[0] if rows_over_x else at[1], a)
        for h in range(2):
            q = (2 * a + h) * rows
            piece = product[q : q + rows]

            def put(ref, where=where, piece=piece):
                if rows_over_x:
                    ref[where, 0] = piece
                else:
                    ref[0, where] = piece

            place(keep, send, at[2], h, put)


def weight_grad(at, xt, dy, rows_over_x):
    feats, tokens = xt.shape
    units = dy.shape[1]
    per = units // 2 // FB
    shape = (2, 2, feats // 4, units // 2)
    if rows_over_x:
        spec = ((2, 1, feats // 4, FB), lambda j, s: (0, (j // per) ^ s[1], 0, j % per), shape, BF)
    else:
        spec = ((1, 2, feats // 4, FB), lambda j, s: ((j // per) ^ s[0], 0, 0, j % per), shape, BF)
    return call(
        functools.partial(weight_grad_body, rows_over_x=rows_over_x),
        (units // FB,),
        [whole(xt.shape), ((tokens, FB), lambda j, s: (0, j))],
        [spec, spec],
        flops=2 * tokens * feats * units,
        moved=tokens * (units + feats) * 2 + feats * units * 2,
    )(at, xt, dy)


def last_grad_body(at, nt, dproj, blended, d_branch, gains, keep, send):
    width = nt.shape[0] // 2
    half = dproj.shape[0] // 2
    top, low = half // 2, width // 2
    for a in range(2):
        where_a = flip(at[0], a)
        for b in range(2):
            where_b = flip(at[1], b)
            first = mm_nt(dproj[b * half : (b + 1) * half], nt[a * width : (a + 1) * width]).astype(BF)
            second = mm_nt(blended[a * width : (a + 1) * width], d_branch[b * width : (b + 1) * width])
            second = second.astype(BF)
            for h in range(2):

                def put(ref, h=h, where_a=where_a, where_b=where_b, first=first, second=second):
                    ref[where_a, where_b, :top] = first[h * top : (h + 1) * top]
                    ref[where_a, where_b, top : top + low] = second[h * low : (h + 1) * low]
                    ref[where_a, where_b, top + low :] = gains[...]

                place(keep, send, at[2], h, put)


def last_grad(at, nt, dproj, blended, d_branch, gains):
    feats, tokens = nt.shape
    rows = dproj.shape[0] // 4 + feats // 4 + gains.shape[0]
    shape = (2, 2, rows, feats // 2)
    return call(
        last_grad_body,
        (1,),
        [whole(v.shape) for v in (nt, dproj, blended, d_branch, gains)],
        [whole(shape) + (shape, BF)] * 2,
        flops=2 * tokens * feats * (dproj.shape[0] + feats),
        moved=4 * tokens * feats * 3 + 8 * feats * feats,
    )(at, nt, dproj, blended, d_branch, gains)


def branch_back_body(w, d_branch, out):
    half = d_branch.shape[0] // 2
    out[...] = (mm(w[0], d_branch[:half]) + mm(w[1], d_branch[half:])).astype(BF)


def branch_back(w, d_branch):
    feats, tokens = d_branch.shape
    step = feats // 3
    return call(
        branch_back_body,
        (3,),
        [((2, step, w.shape[2]), lambda i: (0, i, 0)), whole(d_branch.shape)],
        [((step, tokens), lambda i: (i, 0), (feats, tokens), BF)],
        flops=2 * tokens * feats * feats,
        moved=tokens * feats * 4 + w.size * 2,
        prefetch=0,
    )(w, d_branch)[0]


def input_back_body(at, dproj, w, x, d_middle, gain, keep, send, d_gain, turned, hold):
    feats = x.shape[0]
    half = feats // 2

    @pl.when(pl.program_id(0) == 0)
    def _():
        d_gain[...] = jnp.zeros_like(d_gain)
        turned[:half] = w[0].T
        turned[half:] = w[1].T

    v = x[...].astype(F32)
    u = mm(turned[...], dproj[...])
    scale = lax.rsqrt(jnp.sum(v * v, axis=0, keepdims=True) / feats + EPS)
    weighted = u * gain[...]
    inner = jnp.sum(weighted * v, axis=0, keepdims=True) / feats
    d_gain[...] += jnp.sum(u * v * scale, axis=1, keepdims=True)
    hold[...] = d_middle[...] + (scale * weighted - v * (scale * scale * scale * inner))
    keep[...] = hold[pl.ds(pl.multiple_of(at[1] * half, 16), half), :]
    send[...] = hold[pl.ds(pl.multiple_of((1 - at[1]) * half, 16), half), :].astype(BF)


def input_back(at, dproj, w, x, d_middle, gain):
    feats, tokens = x.shape
    half = feats // 2
    return call(
        input_back_body,
        (tokens // TB,),
        [
            columns(dproj.shape[0]),
            whole(w.shape),
            columns(feats),
            columns(feats),
            whole(gain.shape),
        ],
        [
            columns(half) + ((half, tokens), F32),
            columns(half) + ((half, tokens), BF),
            whole(gain.shape) + (gain.shape, F32),
        ],
        [pltpu.VMEM((feats, dproj.shape[0]), BF), pltpu.VMEM((feats, TB), F32)],
        flops=2 * w.size * tokens,
        moved=tokens * 16000 + w.size * 2,
    )(at, dproj, w, x, d_middle, gain)


def greet(devices):
    barrier = pltpu.get_barrier_semaphore()
    for device in devices:
        pl.semaphore_signal(barrier, inc=1, device_id=device, device_id_type=MESH)
    pl.semaphore_wait(barrier, len(devices))


def gather_body(xt, gt, wq, wo, wg, wd, x, g, q, o, gu, d, bx, bg, bq, bo, bw, bd, here, there, send, recv):
    row, col, dp = (lax.axis_index(name) for name in ("row", "col", "dp"))
    core = lax.rem(dp, 2)
    over_x, over_y, over_core = {"row": 1 - row}, {"col": 1 - col}, {"dp": dp + 1 - 2 * core}
    group = x.shape[1]
    width = xt.shape[0]

    def rows_q(k, r, c):
        return q.at[r, pl.ds(pl.multiple_of(c * 2 * nq + k * nq, 16), nq), :]

    def rows_o(k, r, c):
        return o.at[c, pl.ds(pl.multiple_of(r * 2 * no + k * no, 16), no), :]

    def rows_g(part):
        def at(k, r, c):
            return gu.at[k, c, pl.ds(pl.multiple_of(r * 2 * ng + part * ng, 16), ng), :]

        return at

    def rows_d(k, r, c):
        return d.at[r, pl.ds(pl.multiple_of(c * 2 * nd + k * nd, 16), nd), :]

    nq, no, ng, nd = wq.shape[0] // 2, wo.shape[0] // 2, wg.shape[1] // 2, wd.shape[0] // 2

    def lanes(c):
        return pl.ds(pl.multiple_of(c * group, 128), group)

    def feats(c):
        return pl.ds(pl.multiple_of(c * width, 16), width)

    own = (
        (xt.at[:, lanes(col)], bx, x.at[feats(col), :]),
        (gt.at[:, lanes(col)], bg, g.at[feats(col), :]),
        (wq, bq, q.at[row, pl.ds(pl.multiple_of(col * 2 * nq, 16), 2 * nq), :]),
        (wo, bo, o.at[col, pl.ds(pl.multiple_of(row * 2 * no, 16), 2 * no), :]),
        (wg, bw, gu.at[:, col, pl.ds(pl.multiple_of(row * 2 * ng, 16), 2 * ng), :]),
        (wd, bd, d.at[row, pl.ds(pl.multiple_of(col * 2 * nd, 16), 2 * nd), :]),
    )
    loads = [pltpu.make_async_copy(a, b, here.at[i]) for i, (a, b, _) in enumerate(own)]
    stores = [pltpu.make_async_copy(b, c, there.at[i]) for i, (_, b, c) in enumerate(own)]
    for load in loads:
        load.start()

    greet((over_x, over_y, over_core))
    begun = []

    def go(src, dst, device):
        i = len(begun)
        copy = pltpu.make_async_remote_copy(
            src_ref=src, dst_ref=dst, send_sem=send.at[i], recv_sem=recv.at[i], device_id=device, device_id_type=MESH
        )
        copy.start()
        begun.append(copy)
        return copy

    landed = []

    def arrive(copy):
        copy.wait_recv()
        landed.append(copy)

    def out(mine, at):
        return go(mine, at(core, row, col), over_x), go(mine, at(core, row, col), over_y)

    def pass_on(copy, at, r, c):
        arrive(copy)
        return go(at(core, r, c), at(core, r, c), over_core)

    mine_q = wq.at[pl.ds(pl.multiple_of(core * nq, 16), nq), :]
    mine_o = wo.at[pl.ds(pl.multiple_of(core * no, 16), no), :]
    mine_d = wd.at[pl.ds(pl.multiple_of(core * nd, 16), nd), :]
    at_g = (rows_g(0), rows_g(1))
    mine_g = [wg.at[core, pl.ds(part * ng, ng), :] for part in range(2)]

    q_x, q_y = out(mine_q, rows_q)
    tok = go(xt.at[:, lanes(1 - col)], x.at[feats(col), :], over_y)
    for load, store in zip(loads, stores):
        load.wait()
        store.start()
    arrive(q_y)
    q_c = go(rows_q(core, row, 1 - col), rows_q(core, row, 1 - col), over_x)
    ends = [go(rows_q(core, row, 1 - col), rows_q(core, row, 1 - col), over_core)]
    o_x, o_y = out(mine_o, rows_o)
    g_x, g_y = [None, None], [None, None]
    g_x[0], g_y[0] = out(mine_g[0], at_g[0])
    ends.append(pass_on(q_x, rows_q, 1 - row, col))
    ends.append(pass_on(q_c, rows_q, 1 - row, 1 - col))
    arrive(tok)
    arrive(o_y)
    o_c = go(rows_o(core, row, 1 - col), rows_o(core, row, 1 - col), over_x)
    ends.append(go(rows_o(core, row, 1 - col), rows_o(core, row, 1 - col), over_core))
    ends.append(pass_on(o_x, rows_o, 1 - row, col))
    g_x[1], g_y[1] = out(mine_g[1], at_g[1])
    ends.append(pass_on(o_c, rows_o, 1 - row, 1 - col))
    arrive(g_y[0])
    g_c = [go(at_g[0](core, row, 1 - col), at_g[0](core, row, 1 - col), over_x), None]
    ends.append(go(at_g[0](core, row, 1 - col), at_g[0](core, row, 1 - col), over_core))
    ends.append(pass_on(g_x[0], at_g[0], 1 - row, col))
    arrive(g_x[1])
    g_c[1] = go(at_g[1](core, 1 - row, col), at_g[1](core, 1 - row, col), over_y)
    ends.append(go(at_g[1](core, 1 - row, col), at_g[1](core, 1 - row, col), over_core))
    ends.append(pass_on(g_y[1], at_g[1], row, 1 - col))
    grads = go(gt.at[:, lanes(1 - col)], g.at[feats(col), :], over_y)
    d_x, d_y = out(mine_d, rows_d)
    ends.append(pass_on(g_c[0], at_g[0], 1 - row, 1 - col))
    ends.append(pass_on(g_c[1], at_g[1], 1 - row, 1 - col))
    arrive(grads)
    arrive(d_y)
    d_c = go(rows_d(core, row, 1 - col), rows_d(core, row, 1 - col), over_x)
    ends.append(go(rows_d(core, row, 1 - col), rows_d(core, row, 1 - col), over_core))
    ends.append(pass_on(d_x, rows_d, 1 - row, col))
    ends.append(pass_on(d_c, rows_d, 1 - row, 1 - col))
    for copy in ends:
        arrive(copy)
    for copy in begun:
        copy.wait_send()
    for store in stores:
        store.wait()


def gather(xt, gt, wq, wo, wg, wd):
    width, group = xt.shape[0], xt.shape[1] // 2
    full = (2 * width, group)
    shapes = (
        full,
        full,
        (2, 2 * wq.shape[0], wq.shape[1]),
        (2, 2 * wo.shape[0], wo.shape[1]),
        (2, 2, 2 * wg.shape[1], wg.shape[2]),
        (2, 2 * wd.shape[0], wd.shape[1]),
    )
    held = ((width, group), (width, group), wq.shape, wo.shape, wg.shape, wd.shape)
    copies = 2 + 6 * 5
    return pl.pallas_call(
        gather_body,
        in_specs=[ANY] * 6,
        out_specs=[ANY] * 6,
        out_shape=[jax.ShapeDtypeStruct(shape, BF) for shape in shapes],
        scratch_shapes=[pltpu.VMEM(shape, BF) for shape in held]
        + [pltpu.SemaphoreType.DMA((6,))] * 2
        + [pltpu.SemaphoreType.DMA((copies,))] * 2,
        compiler_params=pltpu.CompilerParams(
            collective_id=0, has_side_effects=True, vmem_limit_bytes=60 << 20
        ),
    )(xt, gt, wq, wo, wg, wd)


def reduce_body(*refs, groups, rows, cols, wide, count, lines):
    per = count // groups
    sources, refs = refs[: 2 * groups], refs[2 * groups :]
    out, refs = refs[0], refs[1:]
    kept, near, far, came, turn, met, total, joined, middle, final = refs[:10]
    loads, stores, sent, recv = refs[10:]
    row, col, dp = (lax.axis_index(name) for name in ("row", "col", "dp"))
    core, line = lax.rem(dp, 2), lax.div(dp, 2)
    over_core = {"dp": dp + 1 - 2 * core}
    over = ({"row": 1 - row}, {"col": 1 - col})
    left = line < lines // 2
    step = jnp.where(left, 2, -2)
    inner, outer = {"dp": dp + step}, {"dp": dp - step}
    is_end = (line == 0) | (line == lines - 1)
    is_mid = (line == lines // 2 - 1) | (line == lines // 2)

    barrier = pltpu.get_barrier_semaphore()
    for device in (over_core, over[0], over[1]) + ((inner,) if lines > 1 else ()):
        pl.semaphore_signal(barrier, inc=1, device_id=device, device_id_type=MESH)

    @pl.when(jnp.logical_not(is_end))
    def _():
        pl.semaphore_signal(barrier, inc=1, device_id=outer, device_id_type=MESH)

    pl.semaphore_wait(barrier, jnp.where(is_end, 3 + (lines > 1), 5))

    def region(p, i):
        if wide:
            return pl.ds(i * rows, rows), pl.ds(p * cols, cols)
        return pl.ds((p * per + i) * rows, rows), pl.ds(0, cols)

    def copy(stage, q, p, src, dst, device):
        return pltpu.make_async_remote_copy(
            src_ref=src,
            dst_ref=dst,
            send_sem=sent.at[stage, q, p],
            recv_sem=recv.at[stage, q, p],
            device_id=device,
            device_id_type=MESH,
        )

    def load(q, p):
        a, b = region(p, q % per)
        return pltpu.make_async_copy(sources[2 * (q // per)].at[:, :, a, b], kept.at[q, p], loads.at[q, p])

    def c_copy(q, p, src):
        return copy(0, q, p, src, near.at[q, p], over_core)

    def a_copy(q, p):
        return copy(1, q, p, far.at[q, p], came.at[q, p], over[p])

    def b_copy(q, p):
        return copy(2, q, p, turn.at[q, p], met.at[q, p], over[1 - p])

    def in_copy(q, p):
        return copy(3, q, p, total.at[q, p], joined.at[q, p], inner)

    def mid_copy(q, p):
        return copy(4, q, p, total.at[q, p], middle.at[q, p], inner)

    def out_copy(q, p):
        return copy(5, q, p, final.at[q, p], final.at[q, p], outer)

    def landing(q, p, k):
        group = q // per if isinstance(q, int) else lax.div(q, per)
        index = q % per if isinstance(q, int) else lax.rem(q, per)
        if wide:
            a, b = pl.ds(pl.multiple_of(index * rows, 16), rows), pl.ds(p * cols, cols)
        else:
            a, b = pl.ds(pl.multiple_of((p * per + index) * rows, 16), rows), pl.ds(0, cols)
        return out.at[group, k, a, b]

    def d_copy(q, p):
        return copy(6, q, p, final.at[q, p], landing(q, p, core), over_core)

    def store(q, p):
        return pltpu.make_async_copy(final.at[q, p], landing(q, p, core), stores.at[q, p])

    for q in range(count):
        for p in range(2):
            a, b = region(p, q % per)
            load(q, p).start()
            c_copy(q, p, sources[2 * (q // per) + 1].at[:, :, a, b]).start()

    def add(a, b):
        return (a.astype(F32) + b.astype(F32)).astype(BF)

    def stage_a(q):
        for p in range(2):
            pltpu.make_async_copy(kept.at[q, p], kept.at[q, p], loads.at[q, p]).wait()
            c_copy(q, p, near.at[q, p]).wait_recv()
            for j in range(2):
                i = (1, j) if p == 0 else (j, 1)
                far[q, p, j] = add(kept[(q, p) + i], near[(q, p) + i])
            a_copy(q, p).start()

    def stage_b(q):
        for p in range(2):
            a_copy(q, p).wait_recv()
            for j in range(2):
                i = (0, j) if p == 0 else (j, 0)
                value = add(add(kept[(q, p) + i], near[(q, p) + i]), came[q, p, j])
                if j == 0:
                    kept[(q, p) + i] = value
                else:
                    turn[q, p] = value
            b_copy(q, p).start()

    def stage_sum(q):
        for p in range(2):
            b_copy(q, p).wait_recv()
            value = add(kept[q, p, 0, 0], met[q, p])
            if lines == 1:
                final[q, p] = value
                d_copy(q, p).start()
                store(q, p).start()
            else:
                total[q, p] = value

                @pl.when(is_end)
                def _():
                    in_copy_end(q, p).start()

    def in_copy_end(q, p):
        return in_copy(q, p) if lines > 2 else mid_copy(q, p)

    def stage_in(q):
        if lines <= 2:
            return
        for p in range(2):

            @pl.when(jnp.logical_not(is_end))
            def _():
                in_copy(q, p).wait_recv()
                total[q, p] = add(total[q, p], joined[q, p])

                @pl.when(is_mid)
                def _():
                    mid_copy(q, p).start()

                @pl.when(jnp.logical_not(is_mid))
                def _():
                    in_copy(q, p).start()

    def stage_mid(q):
        if lines == 1:
            return
        for p in range(2):

            @pl.when(is_mid)
            def _():
                mid_copy(q, p).wait_recv()
                final[q, p] = add(total[q, p], middle[q, p])

                @pl.when(jnp.logical_not(is_end))
                def _():
                    out_copy(q, p).start()

                d_copy(q, p).start()
                store(q, p).start()

    def stage_out(q):
        if lines <= 2:
            return
        for p in range(2):

            @pl.when(jnp.logical_not(is_mid))
            def _():
                out_copy(q, p).wait_recv()

                @pl.when(jnp.logical_not(is_end))
                def _():
                    out_copy(q, p).start()

                d_copy(q, p).start()
                store(q, p).start()

    stages = ((0, stage_a), (2, stage_sum), (3, stage_in), (4, stage_mid), (5, stage_out), (1, stage_b))

    def tick(t, carry):
        for lag, stage in stages:
            q = t - lag

            @pl.when((q >= 0) & (q < count))
            def _():
                stage(q)

        return carry

    lax.fori_loop(0, count + 5, tick, 0)

    def finish(q, carry):
        for p in range(2):
            d_copy(q, p).wait_recv()
            c_copy(q, p, near.at[q, p]).wait_send()
            a_copy(q, p).wait_send()
            b_copy(q, p).wait_send()
            d_copy(q, p).wait_send()
            store(q, p).wait()
            if lines > 2:

                @pl.when(jnp.logical_not(is_mid))
                def _():
                    in_copy(q, p).wait_send()

                @pl.when(jnp.logical_not(is_end))
                def _():
                    out_copy(q, p).wait_send()

            if lines > 1:

                @pl.when(is_mid)
                def _():
                    mid_copy(q, p).wait_send()

        return carry

    lax.fori_loop(0, count, finish, 0)


def reduce_pieces(pairs, rows, wide, collective):
    shape = pairs[0][0].shape
    groups = len(pairs)
    lines = lax.axis_size("dp") // 2
    if wide:
        cols, per = shape[3] // 2, shape[2] // rows
    else:
        cols, per = shape[3], shape[2] // rows // 2
    count = groups * per
    unit = (rows, cols)
    sizes = ((2, 2), (2, 2), (2,), (2,), (), (), (), (), (), ())
    return pl.pallas_call(
        functools.partial(
            reduce_body, groups=groups, rows=rows, cols=cols, wide=wide, count=count, lines=lines
        ),
        in_specs=[ANY] * (2 * groups),
        out_specs=ANY,
        out_shape=jax.ShapeDtypeStruct((groups, 2) + shape[2:], BF),
        scratch_shapes=[pltpu.VMEM((count, 2) + size + unit, BF) for size in sizes]
        + [pltpu.SemaphoreType.DMA((count, 2))] * 2
        + [pltpu.SemaphoreType.DMA((7, count, 2))] * 2,
        compiler_params=pltpu.CompilerParams(
            collective_id=collective, has_side_effects=True, vmem_limit_bytes=62 << 20
        ),
    )(*[v for pair in pairs for v in pair])


def shards(tokens, doc_ids, norm_gain, w_qkv, w_out, ffn_gain, w_gate_up, w_down, grad_out):
    row, col, dp = (lax.axis_index(name) for name in ("row", "col", "dp"))
    at = jnp.stack((row, col, dp % 2)).astype(jnp.int32)
    group = tokens.shape[0] // 2
    width = tokens.shape[1]

    x, go_t, qkv, out_w, gate_up, down_w = gather(
        tokens.T, grad_out.T, w_qkv.T, w_out, w_gate_up, w_down.T
    )
    gain_one = norm_gain.astype(F32).reshape(2 * width, 1)
    gain_two = ffn_gain.astype(F32).reshape(2 * width, 1)
    doc = doc_ids[0]
    first = jnp.sum((doc[None, :] < doc[:, None]).astype(jnp.int32), axis=1)
    place_in = (jnp.arange(group, dtype=jnp.int32) - first).astype(F32)
    rate = jnp.exp(jnp.arange(HD // 2, dtype=F32) * (-2.0 * math.log(10000.0) / HD))
    angles = jnp.repeat(rate, 2)[:, None] * place_in[None, :]
    sign = jnp.where(jnp.arange(HD) % 2 == 0, -1.0, 1.0).astype(F32)[:, None]
    cos, sin = jnp.cos(angles), jnp.sin(angles) * sign
    drow, dcol = doc.reshape(1, group), jnp.broadcast_to(doc[:, None], (group, QB))

    nt, qt, kt, vt = project(x, gain_one, qkv, cos, sin)
    blended, lse = attend(qt, kt, vt, drow, dcol)
    middle, n2t, n2, go = mix(blended, x, out_w, gain_two, go_t)
    hidden, by_gate, by_up = gate(n2, gate_up)
    pieces = [weight_grad(at, go_t, hidden, False)]
    d_gate, d_up, y_keep, y_send = down(at, hidden, by_gate, by_up, down_w, go, middle)
    pairs = [(0, 1), (1, 0)]
    y_came = lax.ppermute(y_send, "col", pairs)
    pieces.append(weight_grad(at, n2t, d_gate, True))
    pieces.append(weight_grad(at, n2t, d_up, True))
    d_middle, d_branch, gain_two_grad = norm_back(d_gate, d_up, gate_up, middle, go_t, gain_two)
    dot = branch_back(out_w, d_branch)
    dproj = attend_back(qt, kt, vt, dot, lse, drow, dcol, cos, sin)
    g_keep, g_send, gain_one_grad = input_back(at, dproj, qkv, x, d_middle, gain_one)
    g_came = lax.ppermute(g_send, "col", pairs)
    gains = jnp.concatenate((gain_one_grad.reshape(2, width), gain_two_grad.reshape(2, width)), axis=0)
    gains = jnp.pad(gains, ((0, 28), (0, 0))).astype(BF)
    last = [last_grad(at, nt, dproj, blended, d_branch, gains)]

    sums = reduce_pieces(pieces, 80, True, 1).astype(F32)
    tail = reduce_pieces(last, 48, False, 2)[0]
    nq, no = w_qkv.shape[1] // 2, w_out.shape[0] // 2
    gain_rows = tail[0, nq + no : nq + no + 4].astype(F32)

    def both(own, other):
        return jnp.where(
            col == 0, jnp.concatenate((own, other), axis=1), jnp.concatenate((other, own), axis=1)
        ).T

    sums = sums.reshape(3, *w_down.T.shape)
    return (
        both(y_keep, y_came),
        both(g_keep, g_came.astype(F32)),
        gain_rows[:2].reshape(-1),
        tail[:, :nq].astype(F32).reshape(2 * nq, -1).T,
        tail[:, nq : nq + no].astype(F32).reshape(2 * no, -1),
        gain_rows[2:].reshape(-1),
        sums[1:],
        sums[0].T,
    )


def solution(mesh):
    placed = (
        P(("dp", "row"), "col"),
        P(("dp", "row", "col"), None),
        P(),
        P("row", "col"),
        P("row", "col"),
        P(),
        P(None, "row", "col"),
        P("row", "col"),
        P(("dp", "row"), "col"),
    )
    return jax.shard_map(
        shards,
        mesh=mesh,
        in_specs=placed,
        out_specs=(
            P(("dp", "row"), "col"),
            P(("dp", "row"), "col"),
            P(),
            P("row", "col"),
            P("row", "col"),
            P(),
            P(None, "row", "col"),
            P("row", "col"),
        ),
        check_vma=False,
    )
```

```python
import functools
import math

import jax
import jax.numpy as jnp
from jax import lax
from jax.experimental import pallas as pl
from jax.experimental.pallas import tpu as pltpu
from jax.sharding import PartitionSpec as P

HEADS = 15
KV_HEADS = 5
HD = 64
REP = HEADS // KV_HEADS
EPS = 1e-05
BF = jnp.bfloat16
F32 = jnp.float32
TB = 256
FB = 256
QB = 128
REACH = 384
MESH = pl.DeviceIdType.MESH
ANY = pl.BlockSpec(memory_space=pl.ANY)


def mm(a, b):
    return jnp.dot(a, b, preferred_element_type=F32)


def mm_nt(a, b):
    return lax.dot_general(a, b, (((1,), (1,)), ((), ())), preferred_element_type=F32)


def call(body, grid, ins, outs, scratch=(), flops=0, moved=0, prefetch=1):
    return pl.pallas_call(
        body,
        grid_spec=pltpu.PrefetchScalarGridSpec(
            num_scalar_prefetch=prefetch,
            grid=grid,
            in_specs=[pl.BlockSpec(block, index) for block, index in ins],
            out_specs=[pl.BlockSpec(block, index) for block, index, _, _ in outs],
            scratch_shapes=list(scratch),
        ),
        out_shape=[jax.ShapeDtypeStruct(shape, kind) for _, _, shape, kind in outs],
        compiler_params=pltpu.CompilerParams(
            dimension_semantics=("arbitrary",) * len(grid), vmem_limit_bytes=60 << 20
        ),
        cost_estimate=pl.CostEstimate(flops=flops, bytes_accessed=moved, transcendentals=0),
    )


def whole(shape):
    return (shape, lambda *_: (0,) * len(shape))


def columns(rows, step=TB):
    return ((rows, step), lambda i, *_: (0, i))


def swap_pairs(rows):
    count = rows.shape[0]
    after = pltpu.roll(rows, count - 1, 0)
    before = pltpu.roll(rows, 1, 0)
    even = lax.broadcasted_iota(jnp.int32, rows.shape, 0) % 2 == 0
    return jnp.where(even, after, before)


def flip(bit, static):
    return bit if static == 0 else 1 - bit


def project_body(x, gain, w, cos, sin, nt, qt, kt, vt):
    feats = x.shape[0]
    v = x[...].astype(F32)
    square = jnp.sum(v * v, axis=0, keepdims=True)
    scale = lax.rsqrt(square / feats + EPS)
    normed = (v * scale * gain[...]).astype(BF)
    nt[...] = normed
    half = feats // 2
    flat = mm(w[0], normed[:half]) + mm(w[1], normed[half:])
    c, s = cos[...], sin[...]
    turned = KV_HEADS + HEADS
    for head in range(turned):
        part = flat[head * HD : (head + 1) * HD]
        part = part * c + swap_pairs(part) * s
        if head < HEADS:
            qt[head * HD : (head + 1) * HD] = (part.astype(BF).astype(F32) * HD**-0.5).astype(BF)
        else:
            kt[(head - HEADS) * HD : (head - HEADS + 1) * HD] = part.astype(BF)
    vt[...] = flat[turned * HD :].astype(BF)


def project(x, gain, w, cos, sin):
    feats, tokens = x.shape
    q, kv = HEADS * HD, KV_HEADS * HD
    return call(
        project_body,
        (tokens // TB,),
        [columns(feats), whole(gain.shape), whole(w.shape), columns(HD), columns(HD)],
        [columns(n) + ((n, tokens), BF) for n in (feats, q, kv, kv)],
        flops=2 * tokens * w.size,
        moved=tokens * 7000 + w.size * 2,
        prefetch=0,
    )(x, gain, w, cos, sin)


def blocks(tokens):
    for i in range(tokens // QB):
        first = max(0, i - REACH // QB)
        yield i, first * QB, (i + 1 - first) * QB


def fill_bias(drow, dcol, bias):
    for i, start, extent in blocks(drow.shape[1]):
        keys = lax.broadcasted_iota(jnp.int32, (extent, QB), 0) + start
        queries = lax.broadcasted_iota(jnp.int32, (extent, QB), 1) + i * QB
        same = dcol[start : start + extent, :] == drow[:, i * QB : (i + 1) * QB]
        bias[i, :extent] = jnp.where(same & (keys <= queries), 0.0, -1e30)


def side_by_side(ref, i):
    return jnp.concatenate([ref[j * HD : (j + 1) * HD, i * QB : (i + 1) * QB] for j in range(REP)], axis=1)


def attend_body(qt, kt, vt, drow, dcol, out, lse, bias):
    @pl.when(pl.program_id(0) == 0)
    def _():
        fill_bias(drow, dcol, bias)

    keys = kt[...].T
    for i, start, extent in blocks(kt.shape[1]):
        scores = mm(keys[start : start + extent], side_by_side(qt, i))
        scores = scores + jnp.concatenate([bias[i, :extent]] * REP, axis=1)
        top = jnp.max(scores, axis=0, keepdims=True)
        raised = jnp.exp(scores - top)
        total = jnp.sum(raised, axis=0, keepdims=True)
        shares = (raised * (1.0 / total)).astype(BF)
        blended = mm(vt[:, start : start + extent], shares).astype(BF)
        for j in range(REP):
            out[j * HD : (j + 1) * HD, i * QB : (i + 1) * QB] = blended[:, j * QB : (j + 1) * QB]
        lse[0, :, i * REP * QB : (i + 1) * REP * QB] = top + jnp.log(total)


def attend(qt, kt, vt, drow, dcol):
    tokens = qt.shape[1]
    return call(
        attend_body,
        (KV_HEADS,),
        [
            ((REP * HD, tokens), lambda g: (g, 0)),
            ((HD, tokens), lambda g: (g, 0)),
            ((HD, tokens), lambda g: (g, 0)),
            whole(drow.shape),
            whole(dcol.shape),
        ],
        [
            ((REP * HD, tokens), lambda g: (g, 0), qt.shape, BF),
            ((1, 1, REP * tokens), lambda g: (g, 0, 0), (KV_HEADS, 1, REP * tokens), F32),
        ],
        [pltpu.VMEM((tokens // QB, REACH + QB, QB), F32)],
        flops=HEADS * tokens * 512 * 256 * 4,
        moved=tokens * 6000,
        prefetch=0,
    )(qt, kt, vt, drow, dcol)


def attend_back_group(group, qt, kt, vt, dot, lse, cos, sin, out, bias, dk, dv):
    keys, values = kt[...].T, vt[...].T
    dk[...] = jnp.zeros_like(dk)
    dv[...] = jnp.zeros_like(dv)
    base = group * REP * HD
    for i, start, extent in blocks(kt.shape[1]):
        span = slice(start, start + extent)
        lanes = slice(i * QB, (i + 1) * QB)
        queries, upper = side_by_side(qt, i), side_by_side(dot, i)
        scores = mm(keys[span], queries)
        scores = scores + jnp.concatenate([bias[i, :extent]] * REP, axis=1)
        shares = jnp.exp(scores - lse[0, :, i * REP * QB : (i + 1) * REP * QB])
        dp = mm(values[span], upper)
        inner = jnp.sum(shares * dp, axis=0, keepdims=True)
        ds = (shares * (dp - inner)).astype(BF)
        dq = mm(kt[:, span], ds) * HD**-0.5
        dk[:, span] += mm_nt(queries, ds)
        dv[:, span] += mm_nt(upper, shares.astype(BF))
        c, s = cos[:, lanes], sin[:, lanes]
        for j in range(REP):
            part = dq[:, j * QB : (j + 1) * QB]
            part = part * c - swap_pairs(part) * s
            out[pl.ds(pl.multiple_of(base + j * HD, HD), HD), lanes] = part.astype(BF)
    part = dk[...]
    part = part * cos[...] - swap_pairs(part) * sin[...]
    out[pl.ds(pl.multiple_of((HEADS + group) * HD, HD), HD), :] = part.astype(BF)
    out[pl.ds(pl.multiple_of((HEADS + KV_HEADS + group) * HD, HD), HD), :] = dv[...].astype(BF)


def mix_body(blended, x, w, gain, go_t, middle, nt, n, go, turned):
    feats = x.shape[0]
    half = feats // 2

    @pl.when(pl.program_id(0) == 0)
    def _():
        turned[:half] = w[0].T
        turned[half:] = w[1].T

    m = x[...].astype(F32) + mm(turned[...], blended[...])
    middle[...] = m
    scale = lax.rsqrt(jnp.sum(m * m, axis=0, keepdims=True) / feats + EPS)
    normed = (m * scale * gain[...]).astype(BF)
    nt[...] = normed
    n[...] = normed.T
    go[...] = go_t[...].T


def mix(blended, x, w, gain, go_t):
    feats, tokens = x.shape
    rows = ((TB, feats), lambda i: (i, 0))
    return call(
        mix_body,
        (tokens // TB,),
        [columns(feats), columns(feats), whole(w.shape), whole(gain.shape), columns(feats)],
        [
            columns(feats) + (x.shape, F32),
            columns(feats) + (x.shape, BF),
            rows + ((tokens, feats), BF),
            rows + ((tokens, feats), BF),
        ],
        [pltpu.VMEM((feats, feats), BF)],
        flops=2 * tokens * feats * feats,
        moved=tokens * 16000,
        prefetch=0,
    )(blended, x, w, gain, go_t)


def gate_body(n, w, hidden, by_gate, by_up):
    gate = mm(n[...], w[0, 0])
    up = mm(n[...], w[1, 0])
    sig = 1.0 / (1.0 + jnp.exp(-gate))
    act = gate * sig
    hidden[...] = (act * up).astype(BF)
    by_gate[...] = (up * sig * (1.0 + gate * (1.0 - sig))).astype(BF)
    by_up[...] = act.astype(BF)


def gate(n, w):
    tokens, feats = n.shape
    half = w.shape[3]
    per = half // FB
    flat = ((tokens, FB), lambda j: (0, j), (tokens, 2 * half), BF)
    return call(
        gate_body,
        (2 * per,),
        [whole(n.shape), ((2, 1, feats, FB), lambda j: (0, j // per, 0, j % per))],
        [flat, flat, flat],
        flops=8 * tokens * feats * half,
        moved=tokens * half * 12 + w.size * 2,
        prefetch=0,
    )(n, w)


def down_body(at, hidden, by_gate, by_up, w, go, middle, d_gate, d_up, keep, send, total):
    @pl.when(pl.program_id(0) == 0)
    def _():
        total[...] = middle[...]

    back = mm(go[...], w[0])
    d_gate[...] = (back * by_gate[...].astype(F32)).astype(BF)
    d_up[...] = (back * by_up[...].astype(F32)).astype(BF)
    total[...] += mm_nt(w[0], hidden[...])

    @pl.when(pl.program_id(0) == pl.num_programs(0) - 1)
    def _():
        width = keep.shape[0]
        keep[...] = total[pl.ds(pl.multiple_of(at[1] * width, 16), width), :].astype(BF)
        send[...] = total[pl.ds(pl.multiple_of((1 - at[1]) * width, 16), width), :].astype(BF)


def down(at, hidden, by_gate, by_up, w, go, middle):
    tokens, units = hidden.shape
    feats = w.shape[1]
    per = units // 2 // FB
    flat = ((tokens, FB), lambda j, s: (0, j))
    own = whole((feats // 2, tokens)) + ((feats // 2, tokens), BF)
    return call(
        down_body,
        (units // FB,),
        [
            flat,
            flat,
            flat,
            ((1, feats, FB), lambda j, s: (j // per, 0, j % per)),
            whole(go.shape),
            whole(middle.shape),
        ],
        [flat + (hidden.shape, BF), flat + (hidden.shape, BF), own, own],
        [pltpu.VMEM(middle.shape, F32)],
        flops=4 * tokens * feats * units,
        moved=tokens * units * 10 + w.size * 2 + tokens * feats * 10,
    )(at, hidden, by_gate, by_up, w, go, middle)


def place(keep, send, core, h, put):
    @pl.when(core == h)
    def _():
        put(keep)

    @pl.when(core != h)
    def _():
        put(send)


def weight_grad_body(at, xt, dy, keep, send, *, rows_over_x):
    rows = keep.shape[2]
    product = mm(xt[...], dy[...]).astype(BF)
    for a in range(2):
        where = flip(at[0] if rows_over_x else at[1], a)
        for h in range(2):
            q = (2 * a + h) * rows
            piece = product[q : q + rows]

            def put(ref, where=where, piece=piece):
                if rows_over_x:
                    ref[where, 0] = piece
                else:
                    ref[0, where] = piece

            place(keep, send, at[2], h, put)


def weight_grad(at, xt, dy, rows_over_x):
    feats, tokens = xt.shape
    units = dy.shape[1]
    per = units // 2 // FB
    shape = (2, 2, feats // 4, units // 2)
    if rows_over_x:
        spec = ((2, 1, feats // 4, FB), lambda j, s: (0, (j // per) ^ s[1], 0, j % per), shape, BF)
    else:
        spec = ((1, 2, feats // 4, FB), lambda j, s: ((j // per) ^ s[0], 0, 0, j % per), shape, BF)
    return call(
        functools.partial(weight_grad_body, rows_over_x=rows_over_x),
        (units // FB,),
        [whole(xt.shape), ((tokens, FB), lambda j, s: (0, j))],
        [spec, spec],
        flops=2 * tokens * feats * units,
        moved=tokens * (units + feats) * 2 + feats * units * 2,
    )(at, xt, dy)


def greet(devices):
    barrier = pltpu.get_barrier_semaphore()
    for device in devices:
        pl.semaphore_signal(barrier, inc=1, device_id=device, device_id_type=MESH)
    pl.semaphore_wait(barrier, len(devices))


def gather_body(xt, gt, wq, wo, wg, wd, x, g, q, o, gu, d, bx, bg, bq, bo, bw, bd, here, there, send, recv):
    row, col, dp = (lax.axis_index(name) for name in ("row", "col", "dp"))
    core = lax.rem(dp, 2)
    over_x, over_y, over_core = {"row": 1 - row}, {"col": 1 - col}, {"dp": dp + 1 - 2 * core}
    group = x.shape[1]
    width = xt.shape[0]

    def rows_q(k, r, c):
        return q.at[r, pl.ds(pl.multiple_of(c * 2 * nq + k * nq, 16), nq), :]

    def rows_o(k, r, c):
        return o.at[c, pl.ds(pl.multiple_of(r * 2 * no + k * no, 16), no), :]

    def rows_g(part):
        def at(k, r, c):
            return gu.at[k, c, pl.ds(pl.multiple_of(r * 2 * ng + part * ng, 16), ng), :]

        return at

    def rows_d(k, r, c):
        return d.at[r, pl.ds(pl.multiple_of(c * 2 * nd + k * nd, 16), nd), :]

    nq, no, ng, nd = wq.shape[0] // 2, wo.shape[0] // 2, wg.shape[1] // 2, wd.shape[0] // 2

    def lanes(c):
        return pl.ds(pl.multiple_of(c * group, 128), group)

    def feats(c):
        return pl.ds(pl.multiple_of(c * width, 16), width)

    own = (
        (xt.at[:, lanes(col)], bx, x.at[feats(col), :]),
        (gt.at[:, lanes(col)], bg, g.at[feats(col), :]),
        (wq, bq, q.at[row, pl.ds(pl.multiple_of(col * 2 * nq, 16), 2 * nq), :]),
        (wo, bo, o.at[col, pl.ds(pl.multiple_of(row * 2 * no, 16), 2 * no), :]),
        (wg, bw, gu.at[:, col, pl.ds(pl.multiple_of(row * 2 * ng, 16), 2 * ng), :]),
        (wd, bd, d.at[row, pl.ds(pl.multiple_of(col * 2 * nd, 16), 2 * nd), :]),
    )
    loads = [pltpu.make_async_copy(a, b, here.at[i]) for i, (a, b, _) in enumerate(own)]
    stores = [pltpu.make_async_copy(b, c, there.at[i]) for i, (_, b, c) in enumerate(own)]
    for load in loads:
        load.start()

    greet((over_x, over_y, over_core))
    begun = []

    def go(src, dst, device):
        i = len(begun)
        copy = pltpu.make_async_remote_copy(
            src_ref=src, dst_ref=dst, send_sem=send.at[i], recv_sem=recv.at[i], device_id=device, device_id_type=MESH
        )
        copy.start()
        begun.append(copy)
        return copy

    landed = []

    def arrive(copy):
        copy.wait_recv()
        landed.append(copy)

    def out(mine, at):
        return go(mine, at(core, row, col), over_x), go(mine, at(core, row, col), over_y)

    def pass_on(copy, at, r, c):
        arrive(copy)
        return go(at(core, r, c), at(core, r, c), over_core)

    mine_q = wq.at[pl.ds(pl.multiple_of(core * nq, 16), nq), :]
    mine_o = wo.at[pl.ds(pl.multiple_of(core * no, 16), no), :]
    mine_d = wd.at[pl.ds(pl.multiple_of(core * nd, 16), nd), :]
    at_g = (rows_g(0), rows_g(1))
    mine_g = [wg.at[core, pl.ds(part * ng, ng), :] for part in range(2)]

    q_x, q_y = out(mine_q, rows_q)
    tok = go(xt.at[:, lanes(1 - col)], x.at[feats(col), :], over_y)
    for load, store in zip(loads, stores):
        load.wait()
        store.start()
    arrive(q_y)
    q_c = go(rows_q(core, row, 1 - col), rows_q(core, row, 1 - col), over_x)
    ends = [go(rows_q(core, row, 1 - col), rows_q(core, row, 1 - col), over_core)]
    o_x, o_y = out(mine_o, rows_o)
    g_x, g_y = [None, None], [None, None]
    g_x[0], g_y[0] = out(mine_g[0], at_g[0])
    ends.append(pass_on(q_x, rows_q, 1 - row, col))
    ends.append(pass_on(q_c, rows_q, 1 - row, 1 - col))
    arrive(tok)
    arrive(o_y)
    o_c = go(rows_o(core, row, 1 - col), rows_o(core, row, 1 - col), over_x)
    ends.append(go(rows_o(core, row, 1 - col), rows_o(core, row, 1 - col), over_core))
    ends.append(pass_on(o_x, rows_o, 1 - row, col))
    g_x[1], g_y[1] = out(mine_g[1], at_g[1])
    ends.append(pass_on(o_c, rows_o, 1 - row, 1 - col))
    arrive(g_y[0])
    g_c = [go(at_g[0](core, row, 1 - col), at_g[0](core, row, 1 - col), over_x), None]
    ends.append(go(at_g[0](core, row, 1 - col), at_g[0](core, row, 1 - col), over_core))
    ends.append(pass_on(g_x[0], at_g[0], 1 - row, col))
    arrive(g_x[1])
    g_c[1] = go(at_g[1](core, 1 - row, col), at_g[1](core, 1 - row, col), over_y)
    ends.append(go(at_g[1](core, 1 - row, col), at_g[1](core, 1 - row, col), over_core))
    ends.append(pass_on(g_y[1], at_g[1], row, 1 - col))
    grads = go(gt.at[:, lanes(1 - col)], g.at[feats(col), :], over_y)
    d_x, d_y = out(mine_d, rows_d)
    ends.append(pass_on(g_c[0], at_g[0], 1 - row, 1 - col))
    ends.append(pass_on(g_c[1], at_g[1], 1 - row, 1 - col))
    arrive(grads)
    arrive(d_y)
    d_c = go(rows_d(core, row, 1 - col), rows_d(core, row, 1 - col), over_x)
    ends.append(go(rows_d(core, row, 1 - col), rows_d(core, row, 1 - col), over_core))
    ends.append(pass_on(d_x, rows_d, 1 - row, col))
    ends.append(pass_on(d_c, rows_d, 1 - row, 1 - col))
    for copy in ends:
        arrive(copy)
    for copy in begun:
        copy.wait_send()
    for store in stores:
        store.wait()


def gather(xt, gt, wq, wo, wg, wd):
    width, group = xt.shape[0], xt.shape[1] // 2
    full = (2 * width, group)
    shapes = (
        full,
        full,
        (2, 2 * wq.shape[0], wq.shape[1]),
        (2, 2 * wo.shape[0], wo.shape[1]),
        (2, 2, 2 * wg.shape[1], wg.shape[2]),
        (2, 2 * wd.shape[0], wd.shape[1]),
    )
    held = ((width, group), (width, group), wq.shape, wo.shape, wg.shape, wd.shape)
    copies = 2 + 6 * 5
    return pl.pallas_call(
        gather_body,
        in_specs=[ANY] * 6,
        out_specs=[ANY] * 6,
        out_shape=[jax.ShapeDtypeStruct(shape, BF) for shape in shapes],
        scratch_shapes=[pltpu.VMEM(shape, BF) for shape in held]
        + [pltpu.SemaphoreType.DMA((6,))] * 2
        + [pltpu.SemaphoreType.DMA((copies,))] * 2,
        compiler_params=pltpu.CompilerParams(
            collective_id=0, has_side_effects=True, vmem_limit_bytes=60 << 20
        ),
    )(xt, gt, wq, wo, wg, wd)


class Lines:
    def __init__(self, lines):
        row, col, dp = (lax.axis_index(name) for name in ("row", "col", "dp"))
        self.row, self.col, self.core, line = row, col, lax.rem(dp, 2), lax.div(dp, 2)
        self.over_core = {"dp": dp + 1 - 2 * self.core}
        self.over = ({"row": 1 - row}, {"col": 1 - col})
        step = jnp.where(line < lines // 2, 2, -2)
        self.inner, self.outer = {"dp": dp + step}, {"dp": dp - step}
        self.is_end = (line == 0) | (line == lines - 1)
        self.is_mid = (line == lines // 2 - 1) | (line == lines // 2)
        self.lines = lines

    def greet(self):
        barrier = pltpu.get_barrier_semaphore()
        for device in (self.over_core, *self.over) + ((self.inner,) if self.lines > 1 else ()):
            pl.semaphore_signal(barrier, inc=1, device_id=device, device_id_type=MESH)

        @pl.when(jnp.logical_not(self.is_end))
        def _():
            pl.semaphore_signal(barrier, inc=1, device_id=self.outer, device_id_type=MESH)

        pl.semaphore_wait(barrier, jnp.where(self.is_end, 3 + (self.lines > 1), 5))


class Reducer:
    BUFFERS = ((2, 2), (2,), (), (), (), ())

    def __init__(self, at, count, send, kept, landing, buffers, sems, load=None):
        self.at, self.count, self.send, self.kept, self.landing, self.load = at, count, send, kept, landing, load
        self.near, self.came, self.met, self.joined, self.middle, self.final = buffers
        self.stores, self.sent, self.recv = sems
        self.length = count + 5

    @staticmethod
    def scratch(count, unit):
        return [pltpu.VMEM((count, 2) + size + unit, BF) for size in Reducer.BUFFERS] + [
            pltpu.SemaphoreType.DMA((count, 2)),
            pltpu.SemaphoreType.DMA((7, count, 2)),
            pltpu.SemaphoreType.DMA((7, count, 2)),
        ]

    def copy(self, stage, q, p, src, dst, device):
        return pltpu.make_async_remote_copy(
            src_ref=src,
            dst_ref=dst,
            send_sem=self.sent.at[stage, q, p],
            recv_sem=self.recv.at[stage, q, p],
            device_id=device,
            device_id_type=MESH,
        )

    def c_copy(self, q, p, src):
        return self.copy(0, q, p, src, self.near.at[q, p], self.at.over_core)

    def a_copy(self, q, p):
        src = self.near.at[q, p, 1] if p == 0 else self.near.at[q, p, :, 1]
        return self.copy(1, q, p, src, self.came.at[q, p], self.at.over[p])

    def b_copy(self, q, p):
        src = self.near.at[q, p, 0, 1] if p == 0 else self.near.at[q, p, 1, 0]
        return self.copy(2, q, p, src, self.met.at[q, p], self.at.over[1 - p])

    def in_copy(self, q, p):
        return self.copy(3, q, p, self.near.at[q, p, 0, 0], self.joined.at[q, p], self.at.inner)

    def mid_copy(self, q, p):
        return self.copy(4, q, p, self.near.at[q, p, 0, 0], self.middle.at[q, p], self.at.inner)

    def out_copy(self, q, p):
        return self.copy(5, q, p, self.final.at[q, p], self.final.at[q, p], self.at.outer)

    def d_copy(self, q, p):
        return self.copy(6, q, p, self.final.at[q, p], self.landing(q, p, self.at.core), self.at.over_core)

    def store(self, q, p):
        return pltpu.make_async_copy(
            self.final.at[q, p], self.landing(q, p, self.at.core), self.stores.at[q, p]
        )

    def begin(self, chunks):
        for q in chunks:
            for p in range(2):
                if self.load is not None:
                    self.load(q, p).start()
                self.c_copy(q, p, self.send(q, p)).start()

    @staticmethod
    def add(a, b):
        return (a.astype(F32) + b.astype(F32)).astype(BF)

    def sum_core(self, q):
        for p in range(2):
            if self.load is not None:
                self.load(q, p).wait()
            self.c_copy(q, p, self.near.at[q, p]).wait_recv()
            for i in ((1, 0), (1, 1)) if p == 0 else ((0, 1), (1, 1)):
                self.near[(q, p) + i] = self.add(self.kept(q, p, *i)[...], self.near[(q, p) + i])
            self.a_copy(q, p).start()
            for i in ((0, 0), (0, 1)) if p == 0 else ((0, 0), (1, 0)):
                self.near[(q, p) + i] = self.add(self.kept(q, p, *i)[...], self.near[(q, p) + i])

    def sum_first(self, q):
        for p in range(2):
            self.a_copy(q, p).wait_recv()
            for j in (1, 0):
                i = (0, j) if p == 0 else (j, 0)
                self.near[(q, p) + i] = self.add(self.near[(q, p) + i], self.came[q, p, j])
                if j == 1:
                    self.b_copy(q, p).start()

    def sum_second(self, q):
        for p in range(2):
            self.b_copy(q, p).wait_recv()
            value = self.add(self.near[q, p, 0, 0], self.met[q, p])
            if self.at.lines == 1:
                self.final[q, p] = value
                self.done(q, p)
            else:
                self.near[q, p, 0, 0] = value

                @pl.when(self.at.is_end)
                def _():
                    (self.in_copy if self.at.lines > 2 else self.mid_copy)(q, p).start()

    def done(self, q, p):
        self.d_copy(q, p).start()
        self.store(q, p).start()

    def sum_in(self, q):
        if self.at.lines <= 2:
            return
        for p in range(2):

            @pl.when(jnp.logical_not(self.at.is_end))
            def _():
                self.in_copy(q, p).wait_recv()
                self.near[q, p, 0, 0] = self.add(self.near[q, p, 0, 0], self.joined[q, p])

                @pl.when(self.at.is_mid)
                def _():
                    self.mid_copy(q, p).start()

                @pl.when(jnp.logical_not(self.at.is_mid))
                def _():
                    self.in_copy(q, p).start()

    def sum_middle(self, q):
        if self.at.lines == 1:
            return
        for p in range(2):

            @pl.when(self.at.is_mid)
            def _():
                self.mid_copy(q, p).wait_recv()
                self.final[q, p] = self.add(self.near[q, p, 0, 0], self.middle[q, p])

                @pl.when(jnp.logical_not(self.at.is_end))
                def _():
                    self.out_copy(q, p).start()

                self.done(q, p)

    def bring_out(self, q):
        if self.at.lines <= 2:
            return
        for p in range(2):

            @pl.when(jnp.logical_not(self.at.is_mid))
            def _():
                self.out_copy(q, p).wait_recv()

                @pl.when(jnp.logical_not(self.at.is_end))
                def _():
                    self.out_copy(q, p).start()

                self.done(q, p)

    def tick(self, t):
        for lag, stage in (
            (0, self.sum_core),
            (2, self.sum_second),
            (3, self.sum_in),
            (4, self.sum_middle),
            (5, self.bring_out),
            (1, self.sum_first),
        ):
            q = t - lag

            @pl.when((q >= 0) & (q < self.count))
            def _():
                stage(q)

    def finish(self):
        lines = self.at.lines

        def one(q, carry):
            for p in range(2):
                self.d_copy(q, p).wait_recv()
                self.c_copy(q, p, self.near.at[q, p]).wait_send()
                self.a_copy(q, p).wait_send()
                self.b_copy(q, p).wait_send()
                self.d_copy(q, p).wait_send()
                self.store(q, p).wait()
                if lines > 2:

                    @pl.when(jnp.logical_not(self.at.is_mid))
                    def _():
                        self.in_copy(q, p).wait_send()

                    @pl.when(jnp.logical_not(self.at.is_end))
                    def _():
                        self.out_copy(q, p).wait_send()

                if lines > 1:

                    @pl.when(self.at.is_mid)
                    def _():
                        self.mid_copy(q, p).wait_send()

            return carry

        lax.fori_loop(0, self.count, one, 0)


def pipe(body, grid, ins, outs):
    return pltpu.emit_pipeline(
        body,
        grid=grid,
        in_specs=[pl.BlockSpec(*spec) for spec in ins],
        out_specs=[pl.BlockSpec(*spec) for spec in outs],
        _explicit_indices=True,
    )


def back_body(*refs, lines, wide_rows, last_rows, last_count):
    (d_gate, d_up, gate_up, middle, go_t, out_w, qt, kt, vt, lse, qkv, x, nt, blended, y_send), refs = refs[:15], refs[15:]
    sources, refs = refs[:6], refs[6:]
    (gain_one, gain_two, drow, dcol, cos, sin), refs = refs[:6], refs[6:]
    (d_middle, d_branch, dot, g_keep, g_send, g_came, y_came, sums, tail), refs = refs[:9], refs[9:]
    (total, dproj, turned, hold, bias, dk, dv, d_gain_one, d_gain_two, keep, send, wide_kept), refs = refs[:12], refs[12:]
    wide_loads, row_sems, refs = refs[0], refs[1], refs[2:]
    wide_bufs, wide_sems, last_bufs, last_sems = refs[:6], refs[6:9], refs[9:15], refs[15:18]

    at = Lines(lines)
    feats, tokens = middle.shape
    half = feats // 2
    units = d_gate.shape[1]
    per_half = units // 2 // FB

    wide_cols = sums.shape[3] // 2
    per = sums.shape[2] // wide_rows

    def wide_region(q, p):
        index = q % per if isinstance(q, int) else lax.rem(q, per)
        return pl.ds(pl.multiple_of(index * wide_rows, 16), wide_rows), pl.ds(p * wide_cols, wide_cols)

    def wide_load(q, p):
        if not isinstance(q, int):
            return pltpu.make_async_copy(wide_kept.at[q, p], wide_kept.at[q, p], wide_loads.at[q, p])
        return pltpu.make_async_copy(
            sources[2 * (q // per)].at[(slice(None), slice(None)) + wide_region(q, p)],
            wide_kept.at[q, p],
            wide_loads.at[q, p],
        )

    def wide_landing(q, p, k):
        return sums.at[(lax.div(q, per), k) + wide_region(q, p)]

    wide = Reducer(
        at,
        3 * per,
        lambda q, p: sources[2 * (q // per) + 1].at[(slice(None), slice(None)) + wide_region(q, p)],
        lambda q, p, i, j: wide_kept.at[q, p, i, j],
        wide_landing,
        wide_bufs,
        wide_sems,
        wide_load,
    )

    def last_region(q, p):
        return pl.ds(pl.multiple_of((p * last_count + q) * last_rows, 16), last_rows)

    last = Reducer(
        at,
        last_count,
        lambda q, p: send.at[:, :, last_region(q, p), :],
        lambda q, p, i, j: keep.at[i, j, last_region(q, p), :],
        lambda q, p, k: tail.at[0, k, last_region(q, p), :],
        last_bufs,
        last_sems,
    )

    def over_y(src, dst, i):
        return pltpu.make_async_remote_copy(
            src_ref=src,
            dst_ref=dst,
            send_sem=row_sems.at[0, i],
            recv_sem=row_sems.at[1, i],
            device_id=at.over[1],
            device_id_type=MESH,
        )

    at.greet()
    wide.begin(range(3 * per))
    y_copy = over_y(y_send, y_came, 0)
    y_copy.start()

    total[...] = jnp.zeros_like(total)

    def feed(step, d_gate, d_up, w):
        (j,) = step.index
        total[...] += mm_nt(w[0, 0], d_gate[...]) + mm_nt(w[1, 0], d_up[...])

        @pl.when((lax.rem(j, 3) == 2))
        def _():
            wide.tick(lax.div(j, 3))

    pipe(
        feed,
        (units // FB,),
        [
            ((tokens, FB), lambda j: (0, j)),
            ((tokens, FB), lambda j: (0, j)),
            ((2, 1, feats, FB), lambda j: (0, j // per_half, 0, j % per_half)),
        ],
        [],
    )(d_gate, d_up, gate_up)
    d_gain_two[...] = jnp.zeros_like(d_gain_two)
    d_gain_one[...] = jnp.zeros_like(d_gain_one)

    def second_norm(step, middle, go_t, d_middle, d_branch):
        (i,) = step.index
        m, u = middle[...], total[:, pl.ds(pl.multiple_of(i * TB, TB), TB)]
        scale = lax.rsqrt(jnp.sum(m * m, axis=0, keepdims=True) / feats + EPS)
        weighted = u * gain_two[...]
        inner = jnp.sum(weighted * m, axis=0, keepdims=True) / feats
        out = go_t[...].astype(F32) + (scale * weighted - m * (scale * scale * scale * inner))
        d_middle[...] = out
        d_branch[...] = out.astype(BF)
        d_gain_two[...] += jnp.sum(u * m * scale, axis=1, keepdims=True)

    column = ((feats, TB), lambda i: (0, i))
    pipe(second_norm, (tokens // TB,), [column, column], [column, column])(middle, go_t, d_middle, d_branch)

    def branch(step, w, d_branch, out):
        out[...] = (mm(w[0], d_branch[:half]) + mm(w[1], d_branch[half:])).astype(BF)

    third = feats // 3
    pipe(
        branch,
        (3,),
        [((2, third, half), lambda i: (0, i, 0)), ((feats, tokens), lambda i: (0, 0))],
        [((third, tokens), lambda i: (i, 0))],
    )(out_w, d_branch, dot)
    fill_bias(drow, dcol, bias)
    wide.tick(jnp.int32(3))

    def attention(step, qt, kt, vt, dot, lse):
        (g,) = step.index
        attend_back_group(g, qt, kt, vt, dot, lse, cos, sin, dproj, bias, dk, dv)
        wide.tick(4 + g)

    pipe(
        attention,
        (KV_HEADS,),
        [
            ((REP * HD, tokens), lambda g: (g, 0)),
            ((HD, tokens), lambda g: (g, 0)),
            ((HD, tokens), lambda g: (g, 0)),
            ((REP * HD, tokens), lambda g: (g, 0)),
            ((1, 1, REP * tokens), lambda g: (g, 0, 0)),
        ],
        [],
    )(qt, kt, vt, dot, lse)

    def first_norm(step, w, x, d_middle, g_keep, g_send):
        (i,) = step.index

        @pl.when(i == 0)
        def _():
            turned[:half] = w[0].T
            turned[half:] = w[1].T

        v = x[...].astype(F32)
        u = mm(turned[...], dproj[:, pl.ds(pl.multiple_of(i * TB, TB), TB)])
        scale = lax.rsqrt(jnp.sum(v * v, axis=0, keepdims=True) / feats + EPS)
        weighted = u * gain_one[...]
        inner = jnp.sum(weighted * v, axis=0, keepdims=True) / feats
        d_gain_one[...] += jnp.sum(u * v * scale, axis=1, keepdims=True)
        hold[...] = d_middle[...] + (scale * weighted - v * (scale * scale * scale * inner))
        g_keep[...] = hold[pl.ds(pl.multiple_of(at.col * half, 16), half), :]
        g_send[...] = hold[pl.ds(pl.multiple_of((1 - at.col) * half, 16), half), :].astype(BF)

        @pl.when(i == 1)
        def _():
            wide.tick(jnp.int32(9))

    part = ((half, TB), lambda i: (0, i))
    pipe(
        first_norm,
        (tokens // TB,),
        [(qkv.shape, lambda i: (0, 0, 0)), column, column],
        [part, part],
    )(qkv, x, d_middle, g_keep, g_send)
    g_copy = over_y(g_send, g_came, 1)
    g_copy.start()

    lanes = []
    for gain in (d_gain_one, d_gain_two):
        for b in range(2):
            wide_gain = jnp.broadcast_to(gain[b * half : (b + 1) * half], (half, 128))
            lanes.append(wide_gain.T[:1])
    nq, no = dproj.shape[0] // 4, half // 2
    spare = keep.shape[2] - nq - no
    rows = lax.broadcasted_iota(jnp.int32, (spare, half), 0)
    gains = jnp.zeros((spare, half), F32)
    for n, lane in enumerate(lanes):
        gains = jnp.where(rows == n, lane, gains)
    gains = gains.astype(BF)

    def last_weights(step, nt, blended, d_branch):
        (a,) = step.index
        where_a = jnp.where(a == 0, at.row, 1 - at.row)
        for b in range(2):
            where_b = flip(at.col, b)
            first = mm_nt(dproj[b * 2 * nq : (b + 1) * 2 * nq], nt[...]).astype(BF)
            second = mm_nt(blended[...], d_branch[b * half : (b + 1) * half]).astype(BF)
            for h in range(2):

                def put(ref, h=h, where_b=where_b, first=first, second=second):
                    ref[where_a, where_b, :nq] = first[h * nq : (h + 1) * nq]
                    ref[where_a, where_b, nq : nq + no] = second[h * no : (h + 1) * no]
                    ref[where_a, where_b, nq + no :] = gains

                place(keep, send, at.core, h, put)

        wide.tick(10 + a)

    pipe(
        last_weights,
        (2,),
        [
            ((half, tokens), lambda a: (a, 0)),
            ((half, tokens), lambda a: (a, 0)),
            ((feats, tokens), lambda a: (0, 0)),
        ],
        [],
    )(nt, blended, d_branch)

    last.begin(range(last_count))

    def both(t, carry):
        last.tick(t)
        wide.tick(t + 12)
        return carry

    lax.fori_loop(0, last.length, both, 0)
    wide.finish()
    last.finish()
    for copy in (y_copy, g_copy):
        copy.wait()


def back(mesh, *args, pieces, smalls, wide_rows, last_rows):
    (d_gate, d_up, gate_up, middle, go_t, out_w, qt, kt, vt, lse, qkv, x, nt, blended, y_send) = args
    feats, tokens = middle.shape
    half = feats // 2
    lines = mesh.shape["dp"] // 2
    piece = pieces[0].shape
    need = qkv.shape[1] // 4 + half // 2 + 16
    last_total = -(-need // (2 * last_rows)) * 2 * last_rows
    last_count = last_total // 2 // last_rows
    wide_count = 3 * (piece[2] // wide_rows)
    wide_unit, last_unit = (wide_rows, piece[3] // 2), (last_rows, half)
    proj = 2 * qkv.shape[1] // 2
    vmem = pl.BlockSpec(memory_space=pltpu.VMEM)
    shapes = [
        ((feats, tokens), F32),
        ((feats, tokens), BF),
        ((feats, tokens), BF),
        ((half, tokens), F32),
        ((half, tokens), BF),
        ((half, tokens), BF),
        ((half, tokens), BF),
        ((3, 2) + piece[2:], BF),
        ((1, 2, last_total, half), BF),
    ]
    return pl.pallas_call(
        functools.partial(
            back_body, lines=lines, wide_rows=wide_rows, last_rows=last_rows, last_count=last_count
        ),
        in_specs=[ANY] * (len(args) + len(pieces)) + [vmem] * len(smalls),
        out_specs=[ANY] * len(shapes),
        out_shape=[jax.ShapeDtypeStruct(*shape) for shape in shapes],
        scratch_shapes=[
            pltpu.VMEM((feats, tokens), F32),
            pltpu.VMEM((proj, tokens), BF),
            pltpu.VMEM((feats, proj), BF),
            pltpu.VMEM((feats, TB), F32),
            pltpu.VMEM((tokens // QB, REACH + QB, QB), F32),
            pltpu.VMEM((HD, tokens), F32),
            pltpu.VMEM((HD, tokens), F32),
            pltpu.VMEM((feats, 1), F32),
            pltpu.VMEM((feats, 1), F32),
            pltpu.VMEM((2, 2, last_total, half), BF),
            pltpu.VMEM((2, 2, last_total, half), BF),
            pltpu.VMEM((wide_count, 2, 2, 2) + wide_unit, BF),
            pltpu.SemaphoreType.DMA((wide_count, 2)),
            pltpu.SemaphoreType.DMA((2, 2)),
        ]
        + Reducer.scratch(wide_count, wide_unit)
        + Reducer.scratch(last_count, last_unit),
        compiler_params=pltpu.CompilerParams(
            collective_id=1, has_side_effects=True, vmem_limit_bytes=63 << 20
        ),
    )(*args, *pieces, *smalls)


def shards(mesh, tokens, doc_ids, norm_gain, w_qkv, w_out, ffn_gain, w_gate_up, w_down, grad_out):
    row, col, dp = (lax.axis_index(name) for name in ("row", "col", "dp"))
    at = jnp.stack((row, col, dp % 2)).astype(jnp.int32)
    group = tokens.shape[0] // 2
    width = tokens.shape[1]

    x, go_t, qkv, out_w, gate_up, down_w = gather(
        tokens.T, grad_out.T, w_qkv.T, w_out, w_gate_up, w_down.T
    )
    gain_one = norm_gain.astype(F32).reshape(2 * width, 1)
    gain_two = ffn_gain.astype(F32).reshape(2 * width, 1)
    doc = doc_ids[0]
    first = jnp.sum((doc[None, :] < doc[:, None]).astype(jnp.int32), axis=1)
    place_in = (jnp.arange(group, dtype=jnp.int32) - first).astype(F32)
    rate = jnp.exp(jnp.arange(HD // 2, dtype=F32) * (-2.0 * math.log(10000.0) / HD))
    angles = jnp.repeat(rate, 2)[:, None] * place_in[None, :]
    sign = jnp.where(jnp.arange(HD) % 2 == 0, -1.0, 1.0).astype(F32)[:, None]
    cos, sin = jnp.cos(angles), jnp.sin(angles) * sign
    drow, dcol = doc.reshape(1, group), jnp.broadcast_to(doc[:, None], (group, QB))

    nt, qt, kt, vt = project(x, gain_one, qkv, cos, sin)
    blended, lse = attend(qt, kt, vt, drow, dcol)
    middle, n2t, n2, go = mix(blended, x, out_w, gain_two, go_t)
    hidden, by_gate, by_up = gate(n2, gate_up)
    pieces = list(weight_grad(at, go_t, hidden, False))
    d_gate, d_up, y_keep, y_send = down(at, hidden, by_gate, by_up, down_w, go, middle)
    pieces += weight_grad(at, n2t, d_gate, True)
    pieces += weight_grad(at, n2t, d_up, True)
    _, _, _, g_keep, _, g_came, y_came, sums, tail = back(
        mesh,
        *(d_gate, d_up, gate_up, middle, go_t, out_w, qt, kt, vt, lse, qkv, x, nt, blended, y_send),
        pieces=pieces,
        smalls=(gain_one, gain_two, drow, dcol, cos, sin),
        wide_rows=80,
        last_rows=48,
    )
    sums, tail = sums.astype(F32), tail[0]
    nq, no = w_qkv.shape[1] // 2, w_out.shape[0] // 2
    gain_rows = tail[0, nq + no : nq + no + 4].astype(F32)

    def both(own, other):
        return jnp.where(
            col == 0, jnp.concatenate((own, other), axis=1), jnp.concatenate((other, own), axis=1)
        ).T

    sums = sums.reshape(3, *w_down.T.shape)
    return (
        both(y_keep, y_came),
        both(g_keep, g_came.astype(F32)),
        gain_rows[:2].reshape(-1),
        tail[:, :nq].astype(F32).reshape(2 * nq, -1).T,
        tail[:, nq : nq + no].astype(F32).reshape(2 * no, -1),
        gain_rows[2:].reshape(-1),
        sums[1:],
        sums[0].T,
    )


def solution(mesh):
    placed = (
        P(("dp", "row"), "col"),
        P(("dp", "row", "col"), None),
        P(),
        P("row", "col"),
        P("row", "col"),
        P(),
        P(None, "row", "col"),
        P("row", "col"),
        P(("dp", "row"), "col"),
    )
    return jax.shard_map(
        functools.partial(shards, mesh),
        mesh=mesh,
        in_specs=placed,
        out_specs=(
            P(("dp", "row"), "col"),
            P(("dp", "row"), "col"),
            P(),
            P("row", "col"),
            P("row", "col"),
            P(),
            P(None, "row", "col"),
            P("row", "col"),
        ),
        check_vma=False,
    )
```

```python
import functools
import math

import jax
import jax.numpy as jnp
from jax import lax
from jax.experimental import pallas as pl
from jax.experimental.pallas import tpu as pltpu
from jax.sharding import PartitionSpec as P

HEADS = 15
KV_HEADS = 5
HD = 64
REP = HEADS // KV_HEADS
EPS = 1e-05
BF = jnp.bfloat16
F32 = jnp.float32
TB = 256
FB = 256
QB = 128
REACH = 384
MESH = pl.DeviceIdType.MESH
ANY = pl.BlockSpec(memory_space=pl.ANY)


def mm(a, b):
    return jnp.dot(a, b, preferred_element_type=F32)


def mm_nt(a, b):
    return lax.dot_general(a, b, (((1,), (1,)), ((), ())), preferred_element_type=F32)


def call(body, grid, ins, outs, scratch=(), flops=0, moved=0, prefetch=1):
    return pl.pallas_call(
        body,
        grid_spec=pltpu.PrefetchScalarGridSpec(
            num_scalar_prefetch=prefetch,
            grid=grid,
            in_specs=[pl.BlockSpec(block, index) for block, index in ins],
            out_specs=[pl.BlockSpec(block, index) for block, index, _, _ in outs],
            scratch_shapes=list(scratch),
        ),
        out_shape=[jax.ShapeDtypeStruct(shape, kind) for _, _, shape, kind in outs],
        compiler_params=pltpu.CompilerParams(
            dimension_semantics=("arbitrary",) * len(grid), vmem_limit_bytes=60 << 20
        ),
        cost_estimate=pl.CostEstimate(flops=flops, bytes_accessed=moved, transcendentals=0),
    )


def whole(shape):
    return (shape, lambda *_: (0,) * len(shape))


def columns(rows, step=TB):
    return ((rows, step), lambda i, *_: (0, i))


def swap_pairs(rows):
    count = rows.shape[0]
    after = pltpu.roll(rows, count - 1, 0)
    before = pltpu.roll(rows, 1, 0)
    even = lax.broadcasted_iota(jnp.int32, rows.shape, 0) % 2 == 0
    return jnp.where(even, after, before)


def flip(bit, static):
    return bit if static == 0 else 1 - bit


def project_chunk(x, gain, w, c, s, nt, qt, kt, vt):
    feats = x.shape[0]
    v = x[...].astype(F32)
    square = jnp.sum(v * v, axis=0, keepdims=True)
    scale = lax.rsqrt(square / feats + EPS)
    normed = (v * scale * gain[...]).astype(BF)
    nt[...] = normed
    half = feats // 2
    flat = mm(w[0], normed[:half]) + mm(w[1], normed[half:])
    turned = KV_HEADS + HEADS
    for head in range(turned):
        part = flat[head * HD : (head + 1) * HD]
        part = part * c + swap_pairs(part) * s
        if head < HEADS:
            qt[head * HD : (head + 1) * HD] = (part.astype(BF).astype(F32) * HD**-0.5).astype(BF)
        else:
            kt[(head - HEADS) * HD : (head - HEADS + 1) * HD] = part.astype(BF)
    vt[...] = flat[turned * HD :].astype(BF)


def blocks(tokens):
    for i in range(tokens // QB):
        first = max(0, i - REACH // QB)
        yield i, first * QB, (i + 1 - first) * QB


def fill_bias(drow, dcol, bias):
    for i, start, extent in blocks(drow.shape[1]):
        keys = lax.broadcasted_iota(jnp.int32, (extent, QB), 0) + start
        queries = lax.broadcasted_iota(jnp.int32, (extent, QB), 1) + i * QB
        same = dcol[start : start + extent, :] == drow[:, i * QB : (i + 1) * QB]
        bias[i, :extent] = jnp.where(same & (keys <= queries), 0.0, -1e30)


def side_by_side(ref, i):
    return jnp.concatenate([ref[j * HD : (j + 1) * HD, i * QB : (i + 1) * QB] for j in range(REP)], axis=1)


def attend_group(qt, kt, vt, out, lse, bias):
    keys = kt[...].T
    for i, start, extent in blocks(kt.shape[1]):
        scores = mm(keys[start : start + extent], side_by_side(qt, i))
        scores = scores + jnp.concatenate([bias[i, :extent]] * REP, axis=1)
        top = jnp.max(scores, axis=0, keepdims=True)
        raised = jnp.exp(scores - top)
        total = jnp.sum(raised, axis=0, keepdims=True)
        shares = (raised * (1.0 / total)).astype(BF)
        blended = mm(vt[:, start : start + extent], shares).astype(BF)
        for j in range(REP):
            out[j * HD : (j + 1) * HD, i * QB : (i + 1) * QB] = blended[:, j * QB : (j + 1) * QB]
        lse[0, :, i * REP * QB : (i + 1) * REP * QB] = top + jnp.log(total)


def attend_back_group(group, qt, kt, vt, dot, lse, cos, sin, out, bias, dk, dv):
    keys, values = kt[...].T, vt[...].T
    dk[...] = jnp.zeros_like(dk)
    dv[...] = jnp.zeros_like(dv)
    base = group * REP * HD
    for i, start, extent in blocks(kt.shape[1]):
        span = slice(start, start + extent)
        lanes = slice(i * QB, (i + 1) * QB)
        queries, upper = side_by_side(qt, i), side_by_side(dot, i)
        scores = mm(keys[span], queries)
        scores = scores + jnp.concatenate([bias[i, :extent]] * REP, axis=1)
        shares = jnp.exp(scores - lse[0, :, i * REP * QB : (i + 1) * REP * QB])
        dp = mm(values[span], upper)
        inner = jnp.sum(shares * dp, axis=0, keepdims=True)
        ds = (shares * (dp - inner)).astype(BF)
        dq = mm(kt[:, span], ds) * HD**-0.5
        dk[:, span] += mm_nt(queries, ds)
        dv[:, span] += mm_nt(upper, shares.astype(BF))
        c, s = cos[:, lanes], sin[:, lanes]
        for j in range(REP):
            part = dq[:, j * QB : (j + 1) * QB]
            part = part * c - swap_pairs(part) * s
            out[pl.ds(pl.multiple_of(base + j * HD, HD), HD), lanes] = part.astype(BF)
    part = dk[...]
    part = part * cos[...] - swap_pairs(part) * sin[...]
    out[pl.ds(pl.multiple_of((HEADS + group) * HD, HD), HD), :] = part.astype(BF)
    out[pl.ds(pl.multiple_of((HEADS + KV_HEADS + group) * HD, HD), HD), :] = dv[...].astype(BF)


def gate_chunk(n, w, hidden, by_gate, by_up):
    gate = mm(n[...], w[0, 0])
    up = mm(n[...], w[1, 0])
    sig = 1.0 / (1.0 + jnp.exp(-gate))
    act = gate * sig
    hidden[...] = (act * up).astype(BF)
    by_gate[...] = (up * sig * (1.0 + gate * (1.0 - sig))).astype(BF)
    by_up[...] = act.astype(BF)


def down_body(at, hidden, by_gate, by_up, w, go, middle, d_gate, d_up, keep, send, total):
    @pl.when(pl.program_id(0) == 0)
    def _():
        total[...] = middle[...]

    back = mm(go[...], w[0])
    d_gate[...] = (back * by_gate[...].astype(F32)).astype(BF)
    d_up[...] = (back * by_up[...].astype(F32)).astype(BF)
    total[...] += mm_nt(w[0], hidden[...])

    @pl.when(pl.program_id(0) == pl.num_programs(0) - 1)
    def _():
        width = keep.shape[0]
        keep[...] = total[pl.ds(pl.multiple_of(at[1] * width, 16), width), :].astype(BF)
        send[...] = total[pl.ds(pl.multiple_of((1 - at[1]) * width, 16), width), :].astype(BF)


def down(at, hidden, by_gate, by_up, w, go, middle):
    tokens, units = hidden.shape
    feats = w.shape[1]
    per = units // 2 // FB
    flat = ((tokens, FB), lambda j, s: (0, j))
    own = whole((feats // 2, tokens)) + ((feats // 2, tokens), BF)
    return call(
        down_body,
        (units // FB,),
        [
            flat,
            flat,
            flat,
            ((1, feats, FB), lambda j, s: (j // per, 0, j % per)),
            whole(go.shape),
            whole(middle.shape),
        ],
        [flat + (hidden.shape, BF), flat + (hidden.shape, BF), own, own],
        [pltpu.VMEM(middle.shape, F32)],
        flops=4 * tokens * feats * units,
        moved=tokens * units * 10 + w.size * 2 + tokens * feats * 10,
    )(at, hidden, by_gate, by_up, w, go, middle)


def place(keep, send, core, h, put):
    @pl.when(core == h)
    def _():
        put(keep)

    @pl.when(core != h)
    def _():
        put(send)


def weight_grad_body(at, xt, dy, keep, send, *, rows_over_x):
    rows = keep.shape[2]
    product = mm(xt[...], dy[...]).astype(BF)
    for a in range(2):
        where = flip(at[0] if rows_over_x else at[1], a)
        for h in range(2):
            q = (2 * a + h) * rows
            piece = product[q : q + rows]

            def put(ref, where=where, piece=piece):
                if rows_over_x:
                    ref[where, 0] = piece
                else:
                    ref[0, where] = piece

            place(keep, send, at[2], h, put)


def weight_grad(at, xt, dy, rows_over_x):
    feats, tokens = xt.shape
    units = dy.shape[1]
    per = units // 2 // FB
    shape = (2, 2, feats // 4, units // 2)
    if rows_over_x:
        spec = ((2, 1, feats // 4, FB), lambda j, s: (0, (j // per) ^ s[1], 0, j % per), shape, BF)
    else:
        spec = ((1, 2, feats // 4, FB), lambda j, s: ((j // per) ^ s[0], 0, 0, j % per), shape, BF)
    return call(
        functools.partial(weight_grad_body, rows_over_x=rows_over_x),
        (units // FB,),
        [whole(xt.shape), ((tokens, FB), lambda j, s: (0, j))],
        [spec, spec],
        flops=2 * tokens * feats * units,
        moved=tokens * (units + feats) * 2 + feats * units * 2,
    )(at, xt, dy)


def greet(devices):
    barrier = pltpu.get_barrier_semaphore()
    for device in devices:
        pl.semaphore_signal(barrier, inc=1, device_id=device, device_id_type=MESH)
    pl.semaphore_wait(barrier, len(devices))


def pipe(body, grid, ins, outs):
    return pltpu.emit_pipeline(
        body,
        grid=grid,
        in_specs=[pl.BlockSpec(*spec) for spec in ins],
        out_specs=[pl.BlockSpec(*spec) for spec in outs],
        _explicit_indices=True,
    )


def column_of(row, out):
    lanes = jnp.broadcast_to(row.astype(F32), (128, row.shape[1])).T
    out[...] = lanes[:, : out.shape[1]].astype(out.dtype)


def forward_body(*refs):
    (xt, gt, wq, wo, wg, wd, doc, gain_one_row, gain_two_row), refs = refs[:9], refs[9:]
    (x, g, q, o, gu, d, nt, qt, kt, vt, blended, lse, middle, n2t, n2, go_n, hidden, by_gate, by_up), refs = refs[:19], refs[19:]
    (gain_one, gain_two, dcol, cos, sin), refs = refs[:5], refs[5:]
    bx, bg, bq, bo, bw, bd, bias, turned, here, there, send, recv = refs
    row, col, dp = (lax.axis_index(name) for name in ("row", "col", "dp"))
    core = lax.rem(dp, 2)
    over_x, over_y, over_core = {"row": 1 - row}, {"col": 1 - col}, {"dp": dp + 1 - 2 * core}
    feats_all, group = x.shape
    width = xt.shape[0]
    nq, no, ng, nd = wq.shape[0] // 2, wo.shape[0] // 2, wg.shape[1] // 2, wd.shape[0] // 2

    def rows_q(k, r, c):
        return q.at[r, pl.ds(pl.multiple_of(c * 2 * nq + k * nq, 16), nq), :]

    def rows_o(k, r, c):
        return o.at[c, pl.ds(pl.multiple_of(r * 2 * no + k * no, 16), no), :]

    def rows_g(part):
        def at(k, r, c):
            return gu.at[k, c, pl.ds(pl.multiple_of(r * 2 * ng + part * ng, 16), ng), :]

        return at

    def rows_d(k, r, c):
        return d.at[r, pl.ds(pl.multiple_of(c * 2 * nd + k * nd, 16), nd), :]

    def lanes(c):
        return pl.ds(pl.multiple_of(c * group, 128), group)

    def feats(c):
        return pl.ds(pl.multiple_of(c * width, 16), width)

    own = (
        (xt.at[:, lanes(col)], bx, x.at[feats(col), :]),
        (wq, bq, q.at[row, pl.ds(pl.multiple_of(col * 2 * nq, 16), 2 * nq), :]),
        (wo, bo, o.at[col, pl.ds(pl.multiple_of(row * 2 * no, 16), 2 * no), :]),
        (wg, bw, gu.at[:, col, pl.ds(pl.multiple_of(row * 2 * ng, 16), 2 * ng), :]),
        (gt.at[:, lanes(col)], bg, g.at[feats(col), :]),
        (wd, bd, d.at[row, pl.ds(pl.multiple_of(col * 2 * nd, 16), 2 * nd), :]),
    )
    loads = [pltpu.make_async_copy(a, b, here.at[i]) for i, (a, b, _) in enumerate(own)]
    stores = [pltpu.make_async_copy(b, c, there.at[i]) for i, (_, b, c) in enumerate(own)]
    for load in loads:
        load.start()

    greet((over_x, over_y, over_core))
    begun = []

    def go(src, dst, device):
        i = len(begun)
        copy = pltpu.make_async_remote_copy(
            src_ref=src, dst_ref=dst, send_sem=send.at[i], recv_sem=recv.at[i], device_id=device, device_id_type=MESH
        )
        copy.start()
        begun.append(copy)
        return copy

    def out(mine, at):
        return go(mine, at(core, row, col), over_x), go(mine, at(core, row, col), over_y)

    def again(at, r, c, device):
        return go(at(core, r, c), at(core, r, c), device)

    def pass_on(copy, at, r, c):
        copy.wait_recv()
        return again(at, r, c, over_core)

    def arrive(copies):
        for copy in copies:
            copy.wait_recv()

    mine_q = wq.at[pl.ds(pl.multiple_of(core * nq, 16), nq), :]
    mine_o = wo.at[pl.ds(pl.multiple_of(core * no, 16), no), :]
    mine_d = wd.at[pl.ds(pl.multiple_of(core * nd, 16), nd), :]
    at_g = (rows_g(0), rows_g(1))
    mine_g = [wg.at[core, pl.ds(part * ng, ng), :] for part in range(2)]

    q_x, q_y = out(mine_q, rows_q)
    tok = go(xt.at[:, lanes(1 - col)], x.at[feats(col), :], over_y)
    for load, store in zip(loads, stores):
        load.wait()
        store.start()

    column_of(gain_one_row[...], gain_one)
    column_of(gain_two_row[...], gain_two)
    column_of(doc[...], dcol)
    rate = jnp.exp(
        (lax.broadcasted_iota(jnp.int32, (HD, 1), 0) // 2).astype(F32) * (-2.0 * math.log(10000.0) / HD)
    )
    sign = jnp.where(lax.broadcasted_iota(jnp.int32, (HD, QB), 0) % 2 == 0, -1.0, 1.0)
    for i in range(group // QB):
        span = slice(i * QB, (i + 1) * QB)
        first = jnp.sum((dcol[...] < doc[:, span]).astype(F32), axis=0, keepdims=True)
        position = (lax.broadcasted_iota(jnp.int32, (1, QB), 1) + i * QB).astype(F32) - first
        angles = rate * position
        cos[:, span] = jnp.cos(angles)
        sin[:, span] = jnp.sin(angles) * sign
    fill_bias(doc, dcol, bias)

    q_y.wait_recv()
    q_c = again(rows_q, row, 1 - col, over_x)
    q_ends = [again(rows_q, row, 1 - col, over_core)]
    o_x, o_y = out(mine_o, rows_o)
    g_x, g_y = [None, None], [None, None]
    g_x[0], g_y[0] = out(mine_g[0], at_g[0])
    q_ends.append(pass_on(q_x, rows_q, 1 - row, col))
    q_ends.append(pass_on(q_c, rows_q, 1 - row, 1 - col))
    arrive(q_ends + [tok])
    stores[0].wait()
    stores[1].wait()

    column = ((feats_all, TB), lambda i: (0, i))
    qrows, krows = HEADS * HD, KV_HEADS * HD

    def project(step, x, w, nt, qt, kt, vt):
        (i,) = step.index
        here = pl.ds(pl.multiple_of(i * TB, TB), TB)
        project_chunk(x, gain_one, w, cos[:, here], sin[:, here], nt, qt, kt, vt)

    pipe(
        project,
        (group // TB,),
        [column, (q.shape, lambda i: (0, 0, 0))],
        [((n, TB), lambda i: (0, i)) for n in (feats_all, qrows, krows, krows)],
    )(x, q, nt, qt, kt, vt)

    o_y.wait_recv()
    o_c = again(rows_o, row, 1 - col, over_x)
    o_ends = [again(rows_o, row, 1 - col, over_core), pass_on(o_x, rows_o, 1 - row, col)]
    g_x[1], g_y[1] = out(mine_g[1], at_g[1])

    def attend(step, qt, kt, vt, blended, lse):
        attend_group(qt, kt, vt, blended, lse, bias)

    def attend_some(start, count):
        pipe(
            attend,
            (count,),
            [
                ((REP * HD, group), lambda i: (i + start, 0)),
                ((HD, group), lambda i: (i + start, 0)),
                ((HD, group), lambda i: (i + start, 0)),
            ],
            [
                ((REP * HD, group), lambda i: (i + start, 0)),
                ((1, 1, REP * group), lambda i: (i + start, 0, 0)),
            ],
        )(qt, kt, vt, blended, lse)

    attend_some(0, 3)
    o_ends.append(pass_on(o_c, rows_o, 1 - row, 1 - col))
    g_y[0].wait_recv()
    g_c = [again(at_g[0], row, 1 - col, over_x), None]
    g_ends = [again(at_g[0], row, 1 - col, over_core), pass_on(g_x[0], at_g[0], 1 - row, col)]
    attend_some(3, KV_HEADS - 3)
    arrive(o_ends)
    stores[2].wait()

    def mix(step, blended, x, w, middle, nt, n):
        (i,) = step.index

        @pl.when(i == 0)
        def _():
            turned[:width] = w[0].T
            turned[width:] = w[1].T

        m = x[...].astype(F32) + mm(turned[...], blended[...])
        middle[...] = m
        scale = lax.rsqrt(jnp.sum(m * m, axis=0, keepdims=True) / feats_all + EPS)
        normed = (m * scale * gain_two[...]).astype(BF)
        nt[...] = normed
        n[...] = normed.T

    across = ((TB, feats_all), lambda i: (i, 0))
    pipe(
        mix,
        (group // TB,),
        [column, column, (o.shape, lambda i: (0, 0, 0))],
        [column, column, across],
    )(blended, x, o, middle, n2t, n2)

    g_x[1].wait_recv()
    g_c[1] = again(at_g[1], 1 - row, col, over_y)
    g_ends += [again(at_g[1], 1 - row, col, over_core), pass_on(g_y[1], at_g[1], row, 1 - col)]
    d_x, d_y = out(mine_d, rows_d)
    grads = go(gt.at[:, lanes(1 - col)], g.at[feats(col), :], over_y)
    g_ends += [pass_on(g_c[i], at_g[i], 1 - row, 1 - col) for i in range(2)]
    arrive(g_ends)
    stores[3].wait()

    per = wg.shape[2] // FB
    later = []

    def gate(step, n, w, hidden, by_gate, by_up):
        gate_chunk(n, w, hidden, by_gate, by_up)

    def gate_some(start, count):
        pipe(
            gate,
            (count,),
            [
                ((group, feats_all), lambda i: (0, 0)),
                ((2, 1, feats_all, FB), lambda i: (0, (i + start) // per, 0, (i + start) % per)),
            ],
            [((group, FB), lambda i: (0, i + start))] * 3,
        )(n2, gu, hidden, by_gate, by_up)

    gate_some(0, per)
    d_y.wait_recv()
    d_c = again(rows_d, row, 1 - col, over_x)
    d_ends = [again(rows_d, row, 1 - col, over_core), pass_on(d_x, rows_d, 1 - row, col)]
    gate_some(per, per)
    grads.wait_recv()
    stores[4].wait()

    def turn(step, g, go_n):
        go_n[...] = g[...].T

    pipe(turn, (group // TB,), [column], [across])(g, go_n)
    d_ends.append(pass_on(d_c, rows_d, 1 - row, 1 - col))
    arrive(d_ends)
    stores[5].wait()
    for copy in begun:
        copy.wait_send()


def forward(xt, gt, wq, wo, wg, wd, doc, gain_one, gain_two):
    width, group = xt.shape[0], xt.shape[1] // 2
    feats = 2 * width
    full = (feats, group)
    units = 2 * wg.shape[2]
    qrows, krows = HEADS * HD, KV_HEADS * HD
    shapes = (
        (full, BF),
        (full, BF),
        ((2, 2 * wq.shape[0], wq.shape[1]), BF),
        ((2, 2 * wo.shape[0], wo.shape[1]), BF),
        ((2, 2, 2 * wg.shape[1], wg.shape[2]), BF),
        ((2, 2 * wd.shape[0], wd.shape[1]), BF),
        (full, BF),
        ((qrows, group), BF),
        ((krows, group), BF),
        ((krows, group), BF),
        (full, BF),
        ((KV_HEADS, 1, REP * group), F32),
        (full, F32),
        (full, BF),
        ((group, feats), BF),
        ((group, feats), BF),
        ((group, units), BF),
        ((group, units), BF),
        ((group, units), BF),
        ((feats, 1), F32),
        ((feats, 1), F32),
        ((group, QB), jnp.int32),
        ((HD, group), F32),
        ((HD, group), F32),
    )
    held = ((width, group), (width, group), wq.shape, wo.shape, wg.shape, wd.shape)
    copies = 2 + 6 * 5
    vmem = pl.BlockSpec(memory_space=pltpu.VMEM)
    return pl.pallas_call(
        forward_body,
        in_specs=[ANY] * 6 + [vmem] * 3,
        out_specs=[ANY] * 19 + [vmem] * 5,
        out_shape=[jax.ShapeDtypeStruct(*shape) for shape in shapes],
        scratch_shapes=[pltpu.VMEM(shape, BF) for shape in held]
        + [pltpu.VMEM((group // QB, REACH + QB, QB), F32), pltpu.VMEM((feats, feats), BF)]
        + [pltpu.SemaphoreType.DMA((6,))] * 2
        + [pltpu.SemaphoreType.DMA((copies,))] * 2,
        compiler_params=pltpu.CompilerParams(
            collective_id=0, has_side_effects=True, vmem_limit_bytes=62 << 20
        ),
    )(xt, gt, wq, wo, wg, wd, doc, gain_one, gain_two)


class Lines:
    def __init__(self, lines):
        row, col, dp = (lax.axis_index(name) for name in ("row", "col", "dp"))
        self.row, self.col, self.core, line = row, col, lax.rem(dp, 2), lax.div(dp, 2)
        self.over_core = {"dp": dp + 1 - 2 * self.core}
        self.over = ({"row": 1 - row}, {"col": 1 - col})
        step = jnp.where(line < lines // 2, 2, -2)
        self.inner, self.outer = {"dp": dp + step}, {"dp": dp - step}
        self.is_end = (line == 0) | (line == lines - 1)
        self.is_mid = (line == lines // 2 - 1) | (line == lines // 2)
        self.lines = lines

    def greet(self):
        barrier = pltpu.get_barrier_semaphore()
        for device in (self.over_core, *self.over) + ((self.inner,) if self.lines > 1 else ()):
            pl.semaphore_signal(barrier, inc=1, device_id=device, device_id_type=MESH)

        @pl.when(jnp.logical_not(self.is_end))
        def _():
            pl.semaphore_signal(barrier, inc=1, device_id=self.outer, device_id_type=MESH)

        pl.semaphore_wait(barrier, jnp.where(self.is_end, 3 + (self.lines > 1), 5))


class Reducer:
    BUFFERS = ((2, 2), (2,), (), (), (), ())

    def __init__(self, at, count, send, kept, landing, buffers, sems, load=None):
        self.at, self.count, self.send, self.kept, self.landing, self.load = at, count, send, kept, landing, load
        self.near, self.came, self.met, self.joined, self.middle, self.final = buffers
        self.stores, self.sent, self.recv = sems
        self.length = count + 5

    @staticmethod
    def scratch(count, unit):
        return [pltpu.VMEM((count, 2) + size + unit, BF) for size in Reducer.BUFFERS] + [
            pltpu.SemaphoreType.DMA((count, 2)),
            pltpu.SemaphoreType.DMA((7, count, 2)),
            pltpu.SemaphoreType.DMA((7, count, 2)),
        ]

    def copy(self, stage, q, p, src, dst, device):
        return pltpu.make_async_remote_copy(
            src_ref=src,
            dst_ref=dst,
            send_sem=self.sent.at[stage, q, p],
            recv_sem=self.recv.at[stage, q, p],
            device_id=device,
            device_id_type=MESH,
        )

    def c_copy(self, q, p, src):
        return self.copy(0, q, p, src, self.near.at[q, p], self.at.over_core)

    def a_copy(self, q, p):
        src = self.near.at[q, p, 1] if p == 0 else self.near.at[q, p, :, 1]
        return self.copy(1, q, p, src, self.came.at[q, p], self.at.over[p])

    def b_copy(self, q, p):
        src = self.near.at[q, p, 0, 1] if p == 0 else self.near.at[q, p, 1, 0]
        return self.copy(2, q, p, src, self.met.at[q, p], self.at.over[1 - p])

    def in_copy(self, q, p):
        return self.copy(3, q, p, self.near.at[q, p, 0, 0], self.joined.at[q, p], self.at.inner)

    def mid_copy(self, q, p):
        return self.copy(4, q, p, self.near.at[q, p, 0, 0], self.middle.at[q, p], self.at.inner)

    def out_copy(self, q, p):
        return self.copy(5, q, p, self.final.at[q, p], self.final.at[q, p], self.at.outer)

    def d_copy(self, q, p):
        return self.copy(6, q, p, self.final.at[q, p], self.landing(q, p, self.at.core), self.at.over_core)

    def store(self, q, p):
        return pltpu.make_async_copy(
            self.final.at[q, p], self.landing(q, p, self.at.core), self.stores.at[q, p]
        )

    def begin(self, chunks):
        for q in chunks:
            for p in range(2):
                if self.load is not None:
                    self.load(q, p).start()
                self.c_copy(q, p, self.send(q, p)).start()

    @staticmethod
    def add(a, b):
        return (a.astype(F32) + b.astype(F32)).astype(BF)

    def sum_core(self, q):
        for p in range(2):
            if self.load is not None:
                self.load(q, p).wait()
            self.c_copy(q, p, self.near.at[q, p]).wait_recv()
            for i in ((1, 0), (1, 1)) if p == 0 else ((0, 1), (1, 1)):
                self.near[(q, p) + i] = self.add(self.kept(q, p, *i)[...], self.near[(q, p) + i])
            self.a_copy(q, p).start()
            for i in ((0, 0), (0, 1)) if p == 0 else ((0, 0), (1, 0)):
                self.near[(q, p) + i] = self.add(self.kept(q, p, *i)[...], self.near[(q, p) + i])

    def sum_first(self, q):
        for p in range(2):
            self.a_copy(q, p).wait_recv()
            for j in (1, 0):
                i = (0, j) if p == 0 else (j, 0)
                self.near[(q, p) + i] = self.add(self.near[(q, p) + i], self.came[q, p, j])
                if j == 1:
                    self.b_copy(q, p).start()

    def sum_second(self, q):
        for p in range(2):
            self.b_copy(q, p).wait_recv()
            value = self.add(self.near[q, p, 0, 0], self.met[q, p])
            if self.at.lines == 1:
                self.final[q, p] = value
                self.done(q, p)
            else:
                self.near[q, p, 0, 0] = value

                @pl.when(self.at.is_end)
                def _():
                    (self.in_copy if self.at.lines > 2 else self.mid_copy)(q, p).start()

    def done(self, q, p):
        self.d_copy(q, p).start()
        self.store(q, p).start()

    def sum_in(self, q):
        if self.at.lines <= 2:
            return
        for p in range(2):

            @pl.when(jnp.logical_not(self.at.is_end))
            def _():
                self.in_copy(q, p).wait_recv()
                self.near[q, p, 0, 0] = self.add(self.near[q, p, 0, 0], self.joined[q, p])

                @pl.when(self.at.is_mid)
                def _():
                    self.mid_copy(q, p).start()

                @pl.when(jnp.logical_not(self.at.is_mid))
                def _():
                    self.in_copy(q, p).start()

    def sum_middle(self, q):
        if self.at.lines == 1:
            return
        for p in range(2):

            @pl.when(self.at.is_mid)
            def _():
                self.mid_copy(q, p).wait_recv()
                self.final[q, p] = self.add(self.near[q, p, 0, 0], self.middle[q, p])

                @pl.when(jnp.logical_not(self.at.is_end))
                def _():
                    self.out_copy(q, p).start()

                self.done(q, p)

    def bring_out(self, q):
        if self.at.lines <= 2:
            return
        for p in range(2):

            @pl.when(jnp.logical_not(self.at.is_mid))
            def _():
                self.out_copy(q, p).wait_recv()

                @pl.when(jnp.logical_not(self.at.is_end))
                def _():
                    self.out_copy(q, p).start()

                self.done(q, p)

    def tick(self, t):
        for lag, stage in (
            (0, self.sum_core),
            (2, self.sum_second),
            (3, self.sum_in),
            (4, self.sum_middle),
            (5, self.bring_out),
            (1, self.sum_first),
        ):
            q = t - lag

            @pl.when((q >= 0) & (q < self.count))
            def _():
                stage(q)

    def finish(self):
        lines = self.at.lines

        def one(q, carry):
            for p in range(2):
                self.d_copy(q, p).wait_recv()
                self.c_copy(q, p, self.near.at[q, p]).wait_send()
                self.a_copy(q, p).wait_send()
                self.b_copy(q, p).wait_send()
                self.d_copy(q, p).wait_send()
                self.store(q, p).wait()
                if lines > 2:

                    @pl.when(jnp.logical_not(self.at.is_mid))
                    def _():
                        self.in_copy(q, p).wait_send()

                    @pl.when(jnp.logical_not(self.at.is_end))
                    def _():
                        self.out_copy(q, p).wait_send()

                if lines > 1:

                    @pl.when(self.at.is_mid)
                    def _():
                        self.mid_copy(q, p).wait_send()

            return carry

        lax.fori_loop(0, self.count, one, 0)


def back_body(*refs, lines, wide_rows, last_rows, last_count):
    (d_gate, d_up, gate_up, middle, go_t, out_w, qt, kt, vt, lse, qkv, x, nt, blended, y_send), refs = refs[:15], refs[15:]
    sources, refs = refs[:6], refs[6:]
    (gain_one, gain_two, drow, dcol, cos, sin), refs = refs[:6], refs[6:]
    (d_middle, d_branch, dot, g_keep, g_send, g_came, y_came, sums, tail), refs = refs[:9], refs[9:]
    (total, dproj, turned, hold, bias, dk, dv, d_gain_one, d_gain_two, keep, send, wide_kept), refs = refs[:12], refs[12:]
    wide_loads, row_sems, refs = refs[0], refs[1], refs[2:]
    wide_bufs, wide_sems, last_bufs, last_sems = refs[:6], refs[6:9], refs[9:15], refs[15:18]

    at = Lines(lines)
    feats, tokens = middle.shape
    half = feats // 2
    units = d_gate.shape[1]
    per_half = units // 2 // FB

    wide_cols = sums.shape[3] // 2
    per = sums.shape[2] // wide_rows

    def wide_region(q, p):
        index = q % per if isinstance(q, int) else lax.rem(q, per)
        return pl.ds(pl.multiple_of(index * wide_rows, 16), wide_rows), pl.ds(p * wide_cols, wide_cols)

    def wide_load(q, p):
        if not isinstance(q, int):
            return pltpu.make_async_copy(wide_kept.at[q, p], wide_kept.at[q, p], wide_loads.at[q, p])
        return pltpu.make_async_copy(
            sources[2 * (q // per)].at[(slice(None), slice(None)) + wide_region(q, p)],
            wide_kept.at[q, p],
            wide_loads.at[q, p],
        )

    def wide_landing(q, p, k):
        return sums.at[(lax.div(q, per), k) + wide_region(q, p)]

    wide = Reducer(
        at,
        3 * per,
        lambda q, p: sources[2 * (q // per) + 1].at[(slice(None), slice(None)) + wide_region(q, p)],
        lambda q, p, i, j: wide_kept.at[q, p, i, j],
        wide_landing,
        wide_bufs,
        wide_sems,
        wide_load,
    )

    def last_region(q, p):
        return pl.ds(pl.multiple_of((p * last_count + q) * last_rows, 16), last_rows)

    last = Reducer(
        at,
        last_count,
        lambda q, p: send.at[:, :, last_region(q, p), :],
        lambda q, p, i, j: keep.at[i, j, last_region(q, p), :],
        lambda q, p, k: tail.at[0, k, last_region(q, p), :],
        last_bufs,
        last_sems,
    )

    def over_y(src, dst, i):
        return pltpu.make_async_remote_copy(
            src_ref=src,
            dst_ref=dst,
            send_sem=row_sems.at[0, i],
            recv_sem=row_sems.at[1, i],
            device_id=at.over[1],
            device_id_type=MESH,
        )

    at.greet()
    wide.begin(range(3 * per))
    y_copy = over_y(y_send, y_came, 0)
    y_copy.start()

    total[...] = jnp.zeros_like(total)

    def feed(step, d_gate, d_up, w):
        (j,) = step.index
        total[...] += mm_nt(w[0, 0], d_gate[...]) + mm_nt(w[1, 0], d_up[...])

        @pl.when((lax.rem(j, 3) == 2))
        def _():
            wide.tick(lax.div(j, 3))

    pipe(
        feed,
        (units // FB,),
        [
            ((tokens, FB), lambda j: (0, j)),
            ((tokens, FB), lambda j: (0, j)),
            ((2, 1, feats, FB), lambda j: (0, j // per_half, 0, j % per_half)),
        ],
        [],
    )(d_gate, d_up, gate_up)
    d_gain_two[...] = jnp.zeros_like(d_gain_two)
    d_gain_one[...] = jnp.zeros_like(d_gain_one)

    def second_norm(step, middle, go_t, d_middle, d_branch):
        (i,) = step.index
        m, u = middle[...], total[:, pl.ds(pl.multiple_of(i * TB, TB), TB)]
        scale = lax.rsqrt(jnp.sum(m * m, axis=0, keepdims=True) / feats + EPS)
        weighted = u * gain_two[...]
        inner = jnp.sum(weighted * m, axis=0, keepdims=True) / feats
        out = go_t[...].astype(F32) + (scale * weighted - m * (scale * scale * scale * inner))
        d_middle[...] = out
        d_branch[...] = out.astype(BF)
        d_gain_two[...] += jnp.sum(u * m * scale, axis=1, keepdims=True)

    column = ((feats, TB), lambda i: (0, i))
    pipe(second_norm, (tokens // TB,), [column, column], [column, column])(middle, go_t, d_middle, d_branch)

    def branch(step, w, d_branch, out):
        out[...] = (mm(w[0], d_branch[:half]) + mm(w[1], d_branch[half:])).astype(BF)

    third = feats // 3
    pipe(
        branch,
        (3,),
        [((2, third, half), lambda i: (0, i, 0)), ((feats, tokens), lambda i: (0, 0))],
        [((third, tokens), lambda i: (i, 0))],
    )(out_w, d_branch, dot)
    fill_bias(drow, dcol, bias)
    wide.tick(jnp.int32(3))

    def attention(step, qt, kt, vt, dot, lse):
        (g,) = step.index
        attend_back_group(g, qt, kt, vt, dot, lse, cos, sin, dproj, bias, dk, dv)
        wide.tick(4 + g)

    pipe(
        attention,
        (KV_HEADS,),
        [
            ((REP * HD, tokens), lambda g: (g, 0)),
            ((HD, tokens), lambda g: (g, 0)),
            ((HD, tokens), lambda g: (g, 0)),
            ((REP * HD, tokens), lambda g: (g, 0)),
            ((1, 1, REP * tokens), lambda g: (g, 0, 0)),
        ],
        [],
    )(qt, kt, vt, dot, lse)

    def first_norm(step, w, x, d_middle, g_keep, g_send):
        (i,) = step.index

        @pl.when(i == 0)
        def _():
            turned[:half] = w[0].T
            turned[half:] = w[1].T

        v = x[...].astype(F32)
        u = mm(turned[...], dproj[:, pl.ds(pl.multiple_of(i * TB, TB), TB)])
        scale = lax.rsqrt(jnp.sum(v * v, axis=0, keepdims=True) / feats + EPS)
        weighted = u * gain_one[...]
        inner = jnp.sum(weighted * v, axis=0, keepdims=True) / feats
        d_gain_one[...] += jnp.sum(u * v * scale, axis=1, keepdims=True)
        hold[...] = d_middle[...] + (scale * weighted - v * (scale * scale * scale * inner))
        g_keep[...] = hold[pl.ds(pl.multiple_of(at.col * half, 16), half), :]
        g_send[...] = hold[pl.ds(pl.multiple_of((1 - at.col) * half, 16), half), :].astype(BF)

        @pl.when(i == 1)
        def _():
            wide.tick(jnp.int32(9))

    part = ((half, TB), lambda i: (0, i))
    pipe(
        first_norm,
        (tokens // TB,),
        [(qkv.shape, lambda i: (0, 0, 0)), column, column],
        [part, part],
    )(qkv, x, d_middle, g_keep, g_send)
    g_copy = over_y(g_send, g_came, 1)
    g_copy.start()

    lanes = []
    for gain in (d_gain_one, d_gain_two):
        for b in range(2):
            wide_gain = jnp.broadcast_to(gain[b * half : (b + 1) * half], (half, 128))
            lanes.append(wide_gain.T[:1])
    nq, no = dproj.shape[0] // 4, half // 2
    spare = keep.shape[2] - nq - no
    rows = lax.broadcasted_iota(jnp.int32, (spare, half), 0)
    gains = jnp.zeros((spare, half), F32)
    for n, lane in enumerate(lanes):
        gains = jnp.where(rows == n, lane, gains)
    gains = gains.astype(BF)

    def last_weights(step, nt, blended, d_branch):
        (a,) = step.index
        where_a = jnp.where(a == 0, at.row, 1 - at.row)
        for b in range(2):
            where_b = flip(at.col, b)
            first = mm_nt(dproj[b * 2 * nq : (b + 1) * 2 * nq], nt[...]).astype(BF)
            second = mm_nt(blended[...], d_branch[b * half : (b + 1) * half]).astype(BF)
            for h in range(2):

                def put(ref, h=h, where_b=where_b, first=first, second=second):
                    ref[where_a, where_b, :nq] = first[h * nq : (h + 1) * nq]
                    ref[where_a, where_b, nq : nq + no] = second[h * no : (h + 1) * no]
                    ref[where_a, where_b, nq + no :] = gains

                place(keep, send, at.core, h, put)

        wide.tick(10 + a)

    pipe(
        last_weights,
        (2,),
        [
            ((half, tokens), lambda a: (a, 0)),
            ((half, tokens), lambda a: (a, 0)),
            ((feats, tokens), lambda a: (0, 0)),
        ],
        [],
    )(nt, blended, d_branch)

    last.begin(range(last_count))

    def both(t, carry):
        last.tick(t)
        wide.tick(t + 12)
        return carry

    lax.fori_loop(0, last.length, both, 0)
    wide.finish()
    last.finish()
    for copy in (y_copy, g_copy):
        copy.wait()


def back(mesh, *args, pieces, smalls, wide_rows, last_rows):
    (d_gate, d_up, gate_up, middle, go_t, out_w, qt, kt, vt, lse, qkv, x, nt, blended, y_send) = args
    feats, tokens = middle.shape
    half = feats // 2
    lines = mesh.shape["dp"] // 2
    piece = pieces[0].shape
    need = qkv.shape[1] // 4 + half // 2 + 16
    last_total = -(-need // (2 * last_rows)) * 2 * last_rows
    last_count = last_total // 2 // last_rows
    wide_count = 3 * (piece[2] // wide_rows)
    wide_unit, last_unit = (wide_rows, piece[3] // 2), (last_rows, half)
    proj = 2 * qkv.shape[1] // 2
    vmem = pl.BlockSpec(memory_space=pltpu.VMEM)
    shapes = [
        ((feats, tokens), F32),
        ((feats, tokens), BF),
        ((feats, tokens), BF),
        ((half, tokens), F32),
        ((half, tokens), BF),
        ((half, tokens), BF),
        ((half, tokens), BF),
        ((3, 2) + piece[2:], BF),
        ((1, 2, last_total, half), BF),
    ]
    return pl.pallas_call(
        functools.partial(
            back_body, lines=lines, wide_rows=wide_rows, last_rows=last_rows, last_count=last_count
        ),
        in_specs=[ANY] * (len(args) + len(pieces)) + [vmem] * len(smalls),
        out_specs=[ANY] * len(shapes),
        out_shape=[jax.ShapeDtypeStruct(*shape) for shape in shapes],
        scratch_shapes=[
            pltpu.VMEM((feats, tokens), F32),
            pltpu.VMEM((proj, tokens), BF),
            pltpu.VMEM((feats, proj), BF),
            pltpu.VMEM((feats, TB), F32),
            pltpu.VMEM((tokens // QB, REACH + QB, QB), F32),
            pltpu.VMEM((HD, tokens), F32),
            pltpu.VMEM((HD, tokens), F32),
            pltpu.VMEM((feats, 1), F32),
            pltpu.VMEM((feats, 1), F32),
            pltpu.VMEM((2, 2, last_total, half), BF),
            pltpu.VMEM((2, 2, last_total, half), BF),
            pltpu.VMEM((wide_count, 2, 2, 2) + wide_unit, BF),
            pltpu.SemaphoreType.DMA((wide_count, 2)),
            pltpu.SemaphoreType.DMA((2, 2)),
        ]
        + Reducer.scratch(wide_count, wide_unit)
        + Reducer.scratch(last_count, last_unit),
        compiler_params=pltpu.CompilerParams(
            collective_id=1, has_side_effects=True, vmem_limit_bytes=63 << 20
        ),
    )(*args, *pieces, *smalls)


def shards(mesh, tokens, doc_ids, norm_gain, w_qkv, w_out, ffn_gain, w_gate_up, w_down, grad_out):
    row, col, dp = (lax.axis_index(name) for name in ("row", "col", "dp"))
    at = jnp.stack((row, col, dp % 2)).astype(jnp.int32)

    forwards = forward(
        *(tokens.T, grad_out.T, w_qkv.T, w_out, w_gate_up, w_down.T),
        *(doc_ids, norm_gain.reshape(1, -1), ffn_gain.reshape(1, -1)),
    )
    x, go_t, qkv, out_w, gate_up, down_w, nt, qt, kt, vt, blended, lse = forwards[:12]
    middle, n2t, n2, go, hidden, by_gate, by_up, gain_one, gain_two, dcol, cos, sin = forwards[12:]
    pieces = list(weight_grad(at, go_t, hidden, False))
    d_gate, d_up, y_keep, y_send = down(at, hidden, by_gate, by_up, down_w, go, middle)
    pieces += weight_grad(at, n2t, d_gate, True)
    pieces += weight_grad(at, n2t, d_up, True)
    _, _, _, g_keep, _, g_came, y_came, sums, tail = back(
        mesh,
        *(d_gate, d_up, gate_up, middle, go_t, out_w, qt, kt, vt, lse, qkv, x, nt, blended, y_send),
        pieces=pieces,
        smalls=(gain_one, gain_two, doc_ids, dcol, cos, sin),
        wide_rows=80,
        last_rows=48,
    )
    sums, tail = sums.astype(F32), tail[0]
    nq, no = w_qkv.shape[1] // 2, w_out.shape[0] // 2
    gain_rows = tail[0, nq + no : nq + no + 4].astype(F32)

    def both(own, other):
        return jnp.where(
            col == 0, jnp.concatenate((own, other), axis=1), jnp.concatenate((other, own), axis=1)
        ).T

    sums = sums.reshape(3, *w_down.T.shape)
    return (
        both(y_keep, y_came),
        both(g_keep, g_came.astype(F32)),
        gain_rows[:2].reshape(-1),
        tail[:, :nq].astype(F32).reshape(2 * nq, -1).T,
        tail[:, nq : nq + no].astype(F32).reshape(2 * no, -1),
        gain_rows[2:].reshape(-1),
        sums[1:],
        sums[0].T,
    )


def solution(mesh):
    placed = (
        P(("dp", "row"), "col"),
        P(("dp", "row", "col"), None),
        P(),
        P("row", "col"),
        P("row", "col"),
        P(),
        P(None, "row", "col"),
        P("row", "col"),
        P(("dp", "row"), "col"),
    )
    return jax.shard_map(
        functools.partial(shards, mesh),
        mesh=mesh,
        in_specs=placed,
        out_specs=(
            P(("dp", "row"), "col"),
            P(("dp", "row"), "col"),
            P(),
            P("row", "col"),
            P("row", "col"),
            P(),
            P(None, "row", "col"),
            P("row", "col"),
        ),
        check_vma=False,
    )
```

```python
import functools
import math

import jax
import jax.numpy as jnp
from jax import lax
from jax.experimental import pallas as pl
from jax.experimental.pallas import tpu as pltpu
from jax.sharding import PartitionSpec as P

HEADS = 15
KV_HEADS = 5
HD = 64
REP = HEADS // KV_HEADS
EPS = 1e-05
BF = jnp.bfloat16
F32 = jnp.float32
TB = 256
FB = 640
QB = 128
REACH = 384
MESH = pl.DeviceIdType.MESH
ANY = pl.BlockSpec(memory_space=pl.ANY)


def mm(a, b):
    return jnp.dot(a, b, preferred_element_type=F32)


def mm_nt(a, b):
    return lax.dot_general(a, b, (((1,), (1,)), ((), ())), preferred_element_type=F32)


def swap_pairs(rows):
    count = rows.shape[0]
    after = pltpu.roll(rows, count - 1, 0)
    before = pltpu.roll(rows, 1, 0)
    even = lax.broadcasted_iota(jnp.int32, rows.shape, 0) % 2 == 0
    return jnp.where(even, after, before)


def flip(bit, static):
    return bit if static == 0 else 1 - bit


def project_chunk(x, gain, w, c, s, nt, qt, kt, vt):
    feats = x.shape[0]
    v = x[...].astype(F32)
    square = jnp.sum(v * v, axis=0, keepdims=True)
    scale = lax.rsqrt(square / feats + EPS)
    normed = (v * scale * gain[...]).astype(BF)
    nt[...] = normed
    half = feats // 2
    flat = mm(w[0], normed[:half]) + mm(w[1], normed[half:])
    turned = KV_HEADS + HEADS
    for head in range(turned):
        part = flat[head * HD : (head + 1) * HD]
        part = part * c + swap_pairs(part) * s
        if head < HEADS:
            qt[head * HD : (head + 1) * HD] = (part.astype(BF).astype(F32) * HD**-0.5).astype(BF)
        else:
            kt[(head - HEADS) * HD : (head - HEADS + 1) * HD] = part.astype(BF)
    vt[...] = flat[turned * HD :].astype(BF)


def blocks(tokens):
    for i in range(tokens // QB):
        first = max(0, i - REACH // QB)
        yield i, first * QB, (i + 1 - first) * QB


def fill_bias(drow, dcol, bias):
    for i, start, extent in blocks(drow.shape[1]):
        keys = lax.broadcasted_iota(jnp.int32, (extent, QB), 0) + start
        queries = lax.broadcasted_iota(jnp.int32, (extent, QB), 1) + i * QB
        same = dcol[start : start + extent, :] == drow[:, i * QB : (i + 1) * QB]
        bias[i, :extent] = jnp.where(same & (keys <= queries), 0.0, -1e30)


def side_by_side(ref, i):
    return jnp.concatenate([ref[j * HD : (j + 1) * HD, i * QB : (i + 1) * QB] for j in range(REP)], axis=1)


def attend_group(qt, kt, vt, out, lse, bias):
    keys = kt[...].T
    for i, start, extent in blocks(kt.shape[1]):
        scores = mm(keys[start : start + extent], side_by_side(qt, i))
        scores = scores + jnp.concatenate([bias[i, :extent]] * REP, axis=1)
        top = jnp.max(scores, axis=0, keepdims=True)
        raised = jnp.exp(scores - top)
        total = jnp.sum(raised, axis=0, keepdims=True)
        shares = (raised * (1.0 / total)).astype(BF)
        blended = mm(vt[:, start : start + extent], shares).astype(BF)
        for j in range(REP):
            out[j * HD : (j + 1) * HD, i * QB : (i + 1) * QB] = blended[:, j * QB : (j + 1) * QB]
        lse[0, :, i * REP * QB : (i + 1) * REP * QB] = top + jnp.log(total)


def attend_back_group(group, qt, kt, vt, dot, lse, cos, sin, out, bias, dk, dv):
    keys, values = kt[...].T, vt[...].T
    dk[...] = jnp.zeros_like(dk)
    dv[...] = jnp.zeros_like(dv)
    base = group * REP * HD
    for i, start, extent in blocks(kt.shape[1]):
        span = slice(start, start + extent)
        lanes = slice(i * QB, (i + 1) * QB)
        queries, upper = side_by_side(qt, i), side_by_side(dot, i)
        scores = mm(keys[span], queries)
        scores = scores + jnp.concatenate([bias[i, :extent]] * REP, axis=1)
        shares = jnp.exp(scores - lse[0, :, i * REP * QB : (i + 1) * REP * QB])
        dp = mm(values[span], upper)
        inner = jnp.sum(shares * dp, axis=0, keepdims=True)
        ds = (shares * (dp - inner)).astype(BF)
        dq = mm(kt[:, span], ds) * HD**-0.5
        dk[:, span] += mm_nt(queries, ds)
        dv[:, span] += mm_nt(upper, shares.astype(BF))
        c, s = cos[:, lanes], sin[:, lanes]
        for j in range(REP):
            part = dq[:, j * QB : (j + 1) * QB]
            part = part * c - swap_pairs(part) * s
            out[pl.ds(pl.multiple_of(base + j * HD, HD), HD), lanes] = part.astype(BF)
    part = dk[...]
    part = part * cos[...] - swap_pairs(part) * sin[...]
    out[pl.ds(pl.multiple_of((HEADS + group) * HD, HD), HD), :] = part.astype(BF)
    out[pl.ds(pl.multiple_of((HEADS + KV_HEADS + group) * HD, HD), HD), :] = dv[...].astype(BF)


def gate_chunk(n, w, hidden, by_gate, by_up):
    gate = mm(n[...], w[0, 0])
    up = mm(n[...], w[1, 0])
    sig = 1.0 / (1.0 + jnp.exp(-gate))
    act = gate * sig
    hidden[...] = (act * up).astype(BF)
    by_gate[...] = (up * sig * (1.0 + gate * (1.0 - sig))).astype(BF)
    by_up[...] = act.astype(BF)


def place(keep, send, core, h, put):
    @pl.when(core == h)
    def _():
        put(keep)

    @pl.when(core != h)
    def _():
        put(send)


def greet(devices):
    barrier = pltpu.get_barrier_semaphore()
    for device in devices:
        pl.semaphore_signal(barrier, inc=1, device_id=device, device_id_type=MESH)
    pl.semaphore_wait(barrier, len(devices))


def pipe(body, grid, ins, outs):
    return pltpu.emit_pipeline(
        body,
        grid=grid,
        in_specs=[pl.BlockSpec(*spec) for spec in ins],
        out_specs=[pl.BlockSpec(*spec) for spec in outs],
        _explicit_indices=True,
    )


def column_of(row, out):
    lanes = jnp.broadcast_to(row.astype(F32), (128, row.shape[1])).T
    out[...] = lanes[:, : out.shape[1]].astype(out.dtype)


def forward_body(*refs):
    (xt, gt, wq, wo, wg, wd, doc, gain_rows), refs = refs[:8], refs[8:]
    (x, g, q, o, gu, d, nt, qt, kt, vt, blended, lse, middle, n2t, n2, go_n, hidden, by_gate, by_up, q_t), refs = refs[:20], refs[20:]
    (gain_one, gain_two, dcol, cos, sin), refs = refs[:5], refs[5:]
    bx, bg, bq, bo, bw, bd, bias, turned, here, there, send, recv = refs
    row, col, dp = (lax.axis_index(name) for name in ("row", "col", "dp"))
    core = lax.rem(dp, 2)
    side = lax.rem(lax.div(dp, 2), 2)
    over_x, over_y, over_core = {"row": 1 - row}, {"col": 1 - col}, {"dp": dp + 1 - 2 * core}
    over_z = {"dp": dp + 2 - 4 * side}
    feats_all, group = x.shape
    width = xt.shape[0]
    nq, no, ng, nd = wq.shape[0] // 2, wo.shape[0] // 2, wg.shape[1] // 2, wd.shape[0] // 2

    def rows_q(k, r, c, part):
        n = nq // 2
        return q.at[r, pl.ds(pl.multiple_of(c * 2 * nq + k * nq + part * n, 8), n), :]

    def rows_o(k, r, c, part):
        return o.at[c, pl.ds(pl.multiple_of(r * 2 * no + k * no, 16), no), :]

    def rows_g(k, r, c, part):
        return gu.at[k, c, pl.ds(pl.multiple_of(r * 2 * ng + part * ng, 16), ng), :]

    def rows_d(k, r, c, part):
        return d.at[r, pl.ds(pl.multiple_of(c * 2 * nd + k * nd, 16), nd), :]

    def rows_e(k, r, c, part):
        n = nd // 2
        return d.at[r, pl.ds(pl.multiple_of(c * 2 * nd + k * nd + part * n, 8), n), :]

    def lanes(c):
        return pl.ds(pl.multiple_of(c * group, 128), group)

    def feats(c):
        return pl.ds(pl.multiple_of(c * width, 16), width)

    own = (
        (xt.at[:, lanes(col)], bx, x.at[feats(col), :]),
        (wq, bq, q.at[row, pl.ds(pl.multiple_of(col * 2 * nq, 16), 2 * nq), :]),
        (wo, bo, o.at[col, pl.ds(pl.multiple_of(row * 2 * no, 16), 2 * no), :]),
        (wg, bw, gu.at[:, col, pl.ds(pl.multiple_of(row * 2 * ng, 16), 2 * ng), :]),
        (gt.at[:, lanes(col)], bg, g.at[feats(col), :]),
        (wd, bd, d.at[row, pl.ds(pl.multiple_of(col * 2 * nd, 16), 2 * nd), :]),
    )
    loads = [pltpu.make_async_copy(a, b, here.at[i]) for i, (a, b, _) in enumerate(own)]
    stores = [pltpu.make_async_copy(b, c, there.at[i]) for i, (_, b, c) in enumerate(own)]
    for load in loads:
        load.start()

    greet((over_x, over_y, over_z, over_core))
    begun = []

    def ready(src, dst, device):
        i = len(begun)
        copy = pltpu.make_async_remote_copy(
            src_ref=src, dst_ref=dst, send_sem=send.at[i], recv_sem=recv.at[i], device_id=device, device_id_type=MESH
        )
        begun.append(copy)
        return copy

    def go(src, dst, device):
        copy = ready(src, dst, device)
        copy.start()
        return copy

    x_cell, y_cell, corner = (1 - row, col), (row, 1 - col), (1 - row, 1 - col)

    def again(at, cell, part, device):
        return go(at(core, *cell, part), at(core, *cell, part), device)

    def later(at, cell, part, device):
        return ready(at(core, *cell, part), at(core, *cell, part), device)

    def arrive(copies):
        for copy in copies:
            copy.wait_recv()

    mine_q = wq.at[pl.ds(pl.multiple_of(core * nq + side * (nq // 2), 8), nq // 2), :]
    mine_o = wo.at[pl.ds(pl.multiple_of(core * no, 16), no), :]
    mine_d = wd.at[pl.ds(pl.multiple_of(core * nd, 16), nd), :]
    mine_e = [wd.at[pl.ds(pl.multiple_of(core * nd + part * (nd // 2), 8), nd // 2), :] for part in range(2)]
    mine_g = wg.at[core, pl.ds(pl.multiple_of(side * ng, 16), ng), :]

    q_x = go(mine_q, rows_q(core, row, col, side), over_x)
    q_y = go(mine_q, rows_q(core, row, col, side), over_y)
    tok = go(xt.at[:, lanes(1 - col)], x.at[feats(col), :], over_y)
    for load, store in zip(loads, stores):
        load.wait()
        store.start()

    column_of(gain_rows[0:1], gain_one)
    column_of(gain_rows[1:2], gain_two)
    column_of(doc[...], dcol)
    rate = jnp.exp(
        (lax.broadcasted_iota(jnp.int32, (HD, 1), 0) // 2).astype(F32) * (-2.0 * math.log(10000.0) / HD)
    )
    sign = jnp.where(lax.broadcasted_iota(jnp.int32, (HD, QB), 0) % 2 == 0, -1.0, 1.0)
    for i in range(group // QB):
        span = slice(i * QB, (i + 1) * QB)
        first = jnp.sum((dcol[...] < doc[:, span]).astype(F32), axis=0, keepdims=True)
        position = (lax.broadcasted_iota(jnp.int32, (1, QB), 1) + i * QB).astype(F32) - first
        angles = rate * position
        cos[:, span] = jnp.cos(angles)
        sin[:, span] = jnp.sin(angles) * sign
    fill_bias(doc, dcol, bias)

    def share(copy, at, cell, ends):
        copy.wait_recv()
        along = again(at, cell, side, over_z)
        ends.append(again(at, cell, side, over_core))
        return along

    def hand(copy, at, cell, part, ends):
        copy.wait_recv()
        ends.append(again(at, cell, part, over_core))

    q_ends, o_ends, gx_ends, g_ends, d_ends = [], [], [], [], []
    q_y.wait_recv()
    q_c = again(rows_q, y_cell, side, over_x)
    o_x = go(mine_o, rows_o(core, row, col, 0), over_x)
    o_y = go(mine_o, rows_o(core, row, col, 0), over_y)
    g_x = go(mine_g, rows_g(core, row, col, side), over_x)
    g_y = go(mine_g, rows_g(core, row, col, side), over_y)
    q_yz = again(rows_q, y_cell, side, over_z)
    q_ends.append(again(rows_q, y_cell, side, over_core))
    q_xz = share(q_x, rows_q, x_cell, q_ends)
    q_cz = share(q_c, rows_q, corner, q_ends)
    hand(q_yz, rows_q, y_cell, 1 - side, q_ends)
    hand(q_xz, rows_q, x_cell, 1 - side, q_ends)
    hand(q_cz, rows_q, corner, 1 - side, q_ends)
    arrive(q_ends + [tok])
    stores[0].wait()
    stores[1].wait()

    column = ((feats_all, TB), lambda i: (0, i))
    qrows, krows = HEADS * HD, KV_HEADS * HD

    def project(step, x, w, nt, qt, kt, vt):
        (i,) = step.index
        here = pl.ds(pl.multiple_of(i * TB, TB), TB)
        project_chunk(x, gain_one, w, cos[:, here], sin[:, here], nt, qt, kt, vt)

    pipe(
        project,
        (group // TB,),
        [column, (q.shape, lambda i: (0, 0, 0))],
        [((n, TB), lambda i: (0, i)) for n in (feats_all, qrows, krows, krows)],
    )(x, q, nt, qt, kt, vt)

    o_y.wait_recv()
    o_c = again(rows_o, y_cell, 0, over_x)
    o_ends.append(again(rows_o, y_cell, 0, over_core))
    d_x = [go(mine_e[0], rows_e(core, row, col, 0), over_x), None]
    hand(o_x, rows_o, x_cell, 0, o_ends)
    g_xz = share(g_x, rows_g, x_cell, gx_ends)

    g_c = later(rows_g, y_cell, side, over_x)
    g_yz = later(rows_g, y_cell, side, over_z)
    g_ends.append(later(rows_g, y_cell, side, over_core))
    d_y = ready(mine_d, rows_d(core, row, col, 0), over_y)
    grads = ready(gt.at[:, lanes(1 - col)], g.at[feats(col), :], over_y)
    d_x[1] = ready(mine_e[1], rows_e(core, row, col, 1), over_x)
    o_ends.append(later(rows_o, corner, 0, over_core))
    soon = (g_c, g_yz, g_ends[-1], d_y, grads, d_x[1])

    def attend(step, qt, kt, vt, blended, lse):
        attend_group(qt, kt, vt, blended, lse, bias)

        @pl.when(step.index[0] == KV_HEADS - 2)
        def _():
            g_y.wait_recv()
            for copy in soon:
                copy.start()
            o_c.wait_recv()
            o_ends[-1].start()

    three = ((REP * HD, group), lambda i: (i, 0))
    one = ((HD, group), lambda i: (i, 0))
    pipe(
        attend,
        (KV_HEADS,),
        [three, one, one],
        [three, ((1, 1, REP * group), lambda i: (i, 0, 0))],
    )(qt, kt, vt, blended, lse)
    hand(g_xz, rows_g, x_cell, 1 - side, gx_ends)
    arrive(o_ends)
    stores[2].wait()

    def mix(step, blended, x, w, middle, nt, n):
        (i,) = step.index

        @pl.when(i == 0)
        def _():
            turned[:width] = w[0].T
            turned[width:] = w[1].T

        m = x[...].astype(F32) + mm(turned[...], blended[...])
        middle[...] = m
        scale = lax.rsqrt(jnp.sum(m * m, axis=0, keepdims=True) / feats_all + EPS)
        normed = (m * scale * gain_two[...]).astype(BF)
        nt[...] = normed
        n[...] = normed.T

    across = ((TB, feats_all), lambda i: (i, 0))
    pipe(
        mix,
        (group // TB,),
        [column, column, (o.shape, lambda i: (0, 0, 0))],
        [column, column, across],
    )(blended, x, o, middle, n2t, n2)

    g_cz = share(g_c, rows_g, corner, g_ends)
    d_y.wait_recv()
    d_c = again(rows_d, y_cell, 0, over_x)
    d_ends.append(again(rows_d, y_cell, 0, over_core))
    arrive(gx_ends)
    stores[3].wait()

    per = wg.shape[2] // FB

    def gate(step, n, w, hidden, by_gate, by_up):
        gate_chunk(n, w, hidden, by_gate, by_up)

    def gate_half(b):
        pipe(
            gate,
            (per,),
            [
                ((group, feats_all), lambda i: (0, 0)),
                ((2, 1, feats_all, FB), lambda i: (0, b, 0, i)),
            ],
            [((group, FB), lambda i: (0, b * per + i))] * 3,
        )(n2, gu, hidden, by_gate, by_up)

    def turn_q(step, q, q_t):
        q_t[...] = q[0].T

    pipe(
        turn_q,
        (2,),
        [((1,) + q.shape[1:], lambda i: (i, 0, 0))],
        [((q.shape[2], q.shape[1]), lambda i: (i, 0))],
    )(q, q_t)
    waiting = [g_yz, g_cz] + d_x
    moves = (
        later(rows_g, y_cell, 1 - side, over_core),
        later(rows_g, corner, 1 - side, over_core),
        later(rows_e, x_cell, 0, over_core),
        later(rows_e, x_cell, 1, over_core),
    )
    g_ends += moves[:2]
    d_ends += moves[2:]

    def halves(h, carry):
        gate_half(jnp.where(h == 0, col, 1 - col))

        @pl.when(h == 0)
        def _():
            for copy, move in zip(waiting, moves):
                copy.wait_recv()
                move.start()
            arrive(g_ends)

        return carry

    lax.fori_loop(0, 2, halves, 0)
    grads.wait_recv()
    stores[4].wait()

    def turn(step, g, go_n):
        go_n[...] = g[...].T

    pipe(turn, (group // TB,), [column], [across])(g, go_n)
    hand(d_c, rows_d, corner, 0, d_ends)
    arrive(d_ends)
    stores[5].wait()
    for copy in begun:
        copy.wait_send()


def forward(xt, gt, wq, wo, wg, wd, doc, gains):
    width, group = xt.shape[0], xt.shape[1] // 2
    feats = 2 * width
    full = (feats, group)
    units = 2 * wg.shape[2]
    qrows, krows = HEADS * HD, KV_HEADS * HD
    shapes = (
        (full, BF),
        (full, BF),
        ((2, 2 * wq.shape[0], wq.shape[1]), BF),
        ((2, 2 * wo.shape[0], wo.shape[1]), BF),
        ((2, 2, 2 * wg.shape[1], wg.shape[2]), BF),
        ((2, 2 * wd.shape[0], wd.shape[1]), BF),
        (full, BF),
        ((qrows, group), BF),
        ((krows, group), BF),
        ((krows, group), BF),
        (full, BF),
        ((KV_HEADS, 1, REP * group), F32),
        (full, F32),
        (full, BF),
        ((group, feats), BF),
        ((group, feats), BF),
        ((group, units), BF),
        ((group, units), BF),
        ((group, units), BF),
        ((feats, 2 * wq.shape[0]), BF),
        ((feats, 1), F32),
        ((feats, 1), F32),
        ((group, QB), jnp.int32),
        ((HD, group), F32),
        ((HD, group), F32),
    )
    held = ((width, group), (width, group), wq.shape, wo.shape, wg.shape, wd.shape)
    copies = 2 + 12 + 6 + 12 + 8
    vmem = pl.BlockSpec(memory_space=pltpu.VMEM)
    return pl.pallas_call(
        forward_body,
        in_specs=[ANY] * 6 + [vmem] * 2,
        out_specs=[ANY] * 20 + [vmem] * 5,
        out_shape=[jax.ShapeDtypeStruct(*shape) for shape in shapes],
        scratch_shapes=[pltpu.VMEM(shape, BF) for shape in held]
        + [pltpu.VMEM((group // QB, REACH + QB, QB), F32), pltpu.VMEM((feats, feats), BF)]
        + [pltpu.SemaphoreType.DMA((6,))] * 2
        + [pltpu.SemaphoreType.DMA((copies,))] * 2,
        compiler_params=pltpu.CompilerParams(
            collective_id=0, has_side_effects=True, vmem_limit_bytes=62 << 20
        ),
    )(xt, gt, wq, wo, wg, wd, doc, gains)


class Lines:
    def __init__(self, lines):
        row, col, dp = (lax.axis_index(name) for name in ("row", "col", "dp"))
        self.row, self.col, self.core, line = row, col, lax.rem(dp, 2), lax.div(dp, 2)
        self.over_core = {"dp": dp + 1 - 2 * self.core}
        self.over = ({"row": 1 - row}, {"col": 1 - col})
        step = jnp.where(line < lines // 2, 2, -2)
        self.inner, self.outer = {"dp": dp + step}, {"dp": dp - step}
        self.is_end = (line == 0) | (line == lines - 1)
        self.is_mid = (line == lines // 2 - 1) | (line == lines // 2)
        self.lines = lines

    def greet(self):
        barrier = pltpu.get_barrier_semaphore()
        for device in (self.over_core, *self.over) + ((self.inner,) if self.lines > 1 else ()):
            pl.semaphore_signal(barrier, inc=1, device_id=device, device_id_type=MESH)

        @pl.when(jnp.logical_not(self.is_end))
        def _():
            pl.semaphore_signal(barrier, inc=1, device_id=self.outer, device_id_type=MESH)

        pl.semaphore_wait(barrier, jnp.where(self.is_end, 3 + (self.lines > 1), 5))


class Reducer:
    BUFFERS = ((2, 2), (2,), (), (), (), ())

    def __init__(self, at, count, step, send, kept, landing, buffers, sems, load=None, apart=None):
        self.apart = apart
        self.first = lambda q, p: p
        self.step = step
        self.at, self.count, self.send, self.kept, self.landing, self.load = at, count, send, kept, landing, load
        self.near, self.came, self.met, self.joined, self.middle, self.final = buffers
        self.stores, self.sent, self.recv = sems
        self.length = count + 5

    @staticmethod
    def scratch(count, unit):
        return [pltpu.VMEM((count, 2) + size + unit, BF) for size in Reducer.BUFFERS] + [
            pltpu.SemaphoreType.DMA((count, 2)),
            pltpu.SemaphoreType.DMA((7, count, 2)),
            pltpu.SemaphoreType.DMA((7, count, 2)),
        ]

    def copy(self, stage, q, p, src, dst, device):
        return pltpu.make_async_remote_copy(
            src_ref=src,
            dst_ref=dst,
            send_sem=self.sent.at[stage, q, p],
            recv_sem=self.recv.at[stage, q, p],
            device_id=device,
            device_id_type=MESH,
        )

    def c_copy(self, q, p, src):
        return self.copy(0, q, p, src, self.near.at[q, p], self.at.over_core)

    def a_copy(self, q, p):
        axis = self.first(q, p)
        src = self.near.at[q, p, 1] if axis == 0 else self.near.at[q, p, :, 1]
        return self.copy(1, q, p, src, self.came.at[q, p], self.at.over[axis])

    def b_copy(self, q, p):
        axis = self.first(q, p)
        src = self.near.at[q, p, 0, 1] if axis == 0 else self.near.at[q, p, 1, 0]
        return self.copy(2, q, p, src, self.met.at[q, p], self.at.over[1 - axis])

    def in_copy(self, q, p):
        return self.copy(3, q, p, self.near.at[q, p, 0, 0], self.joined.at[q, p], self.at.inner)

    def mid_copy(self, q, p):
        return self.copy(4, q, p, self.near.at[q, p, 0, 0], self.middle.at[q, p], self.at.inner)

    def out_copy(self, q, p):
        return self.copy(5, q, p, self.final.at[q, p], self.final.at[q, p], self.at.outer)

    def place(self, q, p, group):
        return self.landing(q, p, self.at.core) if group is None else self.landing(q, p, self.at.core, group)

    def d_copy(self, q, p, group=None):
        return self.copy(6, q, p, self.final.at[q, p], self.place(q, p, group), self.at.over_core)

    def store(self, q, p, group=None):
        return pltpu.make_async_copy(self.final.at[q, p], self.place(q, p, group), self.stores.at[q, p])

    def begin(self, chunks):
        for q in chunks:
            for p in range(2):
                if self.load is not None:
                    self.load(q, p).start()
                self.c_copy(q, p, self.send(q, p)).start()

    def add(self, out, a, b):
        rows = out.shape[0]
        step = self.step
        if rows == step:
            out[...] = a[...] + b[...]
            return

        def some(n, carry):
            part = pl.ds(pl.multiple_of(n * step, 16), step)
            out[part, :] = a[part, :] + b[part, :]
            return carry

        lax.fori_loop(0, rows // step, some, 0)

    def sum_core(self, q):
        for p in range(2):
            if self.load is not None:
                self.load(q, p).wait()
            self.c_copy(q, p, self.near.at[q, p]).wait_recv()
            for i in ((1, 0), (1, 1)) if self.first(q, p) == 0 else ((0, 1), (1, 1)):
                near = self.near.at[(q, p) + i]
                self.add(near, self.kept(q, p, *i), near)
            self.a_copy(q, p).start()
        for p in range(2):
            for i in ((0, 0), (0, 1)) if self.first(q, p) == 0 else ((0, 0), (1, 0)):
                near = self.near.at[(q, p) + i]
                self.add(near, self.kept(q, p, *i), near)

    def sum_first(self, q):
        for p in range(2):
            self.a_copy(q, p).wait_recv()
            for j in (1, 0):
                near = self.near.at[(q, p) + ((0, j) if self.first(q, p) == 0 else (j, 0))]
                self.add(near, near, self.came.at[q, p, j])
                if j == 1:
                    self.b_copy(q, p).start()

    def sum_second(self, q):
        for p in range(2):
            self.b_copy(q, p).wait_recv()
            near = self.near.at[q, p, 0, 0]
            if self.at.lines == 1:
                self.add(self.final.at[q, p], near, self.met.at[q, p])
                self.done(q, p)
            else:
                self.add(near, near, self.met.at[q, p])

                @pl.when(self.at.is_end)
                def _():
                    (self.in_copy if self.at.lines > 2 else self.mid_copy)(q, p).start()

    def done(self, q, p):
        if self.apart is None:
            self.d_copy(q, p).start()
            self.store(q, p).start()
            return
        for group, here in ((0, q < self.apart), (None, q >= self.apart)):

            @pl.when(here)
            def _():
                self.d_copy(q, p, group).start()
                self.store(q, p, group).start()

    def sum_in(self, q):
        if self.at.lines <= 2:
            return
        for p in range(2):

            @pl.when(jnp.logical_not(self.at.is_end))
            def _():
                self.in_copy(q, p).wait_recv()
                self.add(self.near.at[q, p, 0, 0], self.near.at[q, p, 0, 0], self.joined.at[q, p])

                @pl.when(self.at.is_mid)
                def _():
                    self.mid_copy(q, p).start()

                @pl.when(jnp.logical_not(self.at.is_mid))
                def _():
                    self.in_copy(q, p).start()

    def sum_middle(self, q):
        if self.at.lines == 1:
            return
        for p in range(2):

            @pl.when(self.at.is_mid)
            def _():
                self.mid_copy(q, p).wait_recv()
                self.add(self.final.at[q, p], self.near.at[q, p, 0, 0], self.middle.at[q, p])

                @pl.when(jnp.logical_not(self.at.is_end))
                def _():
                    self.out_copy(q, p).start()

                self.done(q, p)

    def bring_out(self, q):
        if self.at.lines <= 2:
            return
        for p in range(2):

            @pl.when(jnp.logical_not(self.at.is_mid))
            def _():
                self.out_copy(q, p).wait_recv()

                @pl.when(jnp.logical_not(self.at.is_end))
                def _():
                    self.out_copy(q, p).start()

                self.done(q, p)

    def tick(self, t):
        for lag, stage in (
            (0, self.sum_core),
            (2, self.sum_second),
            (3, self.sum_in),
            (4, self.sum_middle),
            (5, self.bring_out),
            (1, self.sum_first),
        ):
            q = t - lag

            @pl.when((q >= 0) & (q < self.count))
            def _():
                stage(q)

    def finish(self):
        lines = self.at.lines

        def one(q, carry):
            for p in range(2):
                self.d_copy(q, p).wait_recv()
                self.c_copy(q, p, self.near.at[q, p]).wait_send()
                self.a_copy(q, p).wait_send()
                self.b_copy(q, p).wait_send()
                self.d_copy(q, p).wait_send()
                self.store(q, p).wait()
                if lines > 2:

                    @pl.when(jnp.logical_not(self.at.is_mid))
                    def _():
                        self.in_copy(q, p).wait_send()

                    @pl.when(jnp.logical_not(self.at.is_end))
                    def _():
                        self.out_copy(q, p).wait_send()

                if lines > 1:

                    @pl.when(self.at.is_mid)
                    def _():
                        self.mid_copy(q, p).wait_send()

            return carry

        lax.fori_loop(0, self.count, one, 0)


def back_body(*refs, lines, wide_rows, last_rows, last_count):
    names = (
        "hidden",
        "by_gate",
        "by_up",
        "down_w",
        "go",
        "n2t",
        "gate_up",
        "middle",
        "go_t",
        "out_w",
        "qt",
        "kt",
        "vt",
        "lse",
        "q_t",
        "x",
        "nt",
        "blended",
    )
    a, refs = dict(zip(names, refs)), refs[len(names) :]
    (gain_one, gain_two, drow, dcol, cos, sin), refs = refs[:6], refs[6:]
    (d_gate, d_up, d_middle, y_keep, y_send, y_came, g_keep, g_came), refs = refs[:8], refs[8:]
    (downs, ups, tail), sources, refs = refs[:3], refs[3:9], refs[9:]
    (d_gain_one, d_gain_two, keep, send, wide_kept, g_parts, d_branch, dot), refs = refs[:8], refs[8:]
    wide_loads, row_sems, refs = refs[0], refs[1], refs[2:]
    wide_bufs, wide_sems, last_bufs, last_sems = refs[:6], refs[6:9], refs[9:15], refs[15:18]

    at = Lines(lines)
    feats, tokens = a["middle"].shape
    half = feats // 2
    units = a["hidden"].shape[1]
    per_half = units // 2 // FB

    wide_cols = ups.shape[3] // 2
    per = ups.shape[2] // wide_rows

    def wide_region(q, p):
        index = q % per if isinstance(q, int) else lax.rem(q, per)
        return pl.ds(pl.multiple_of(index * wide_rows, 16), wide_rows), pl.ds(p * wide_cols, wide_cols)

    def wide_load(q, p):
        if not isinstance(q, int):
            return pltpu.make_async_copy(wide_kept.at[q, p], wide_kept.at[q, p], wide_loads.at[q, p])
        return pltpu.make_async_copy(
            sources[2 * (q // per)].at[(slice(None), slice(None)) + wide_region(q, p)],
            wide_kept.at[q, p],
            wide_loads.at[q, p],
        )

    def wide_landing(q, p, k, group=None):
        if group is None:
            return ups.at[(jnp.maximum(lax.div(q, per) - 1, 0), k) + wide_region(q, p)]
        return downs.at[(0, k) + wide_region(q, p)]

    wide = Reducer(
        at,
        3 * per,
        80,
        lambda q, p: sources[2 * (q // per) + 1].at[(slice(None), slice(None)) + wide_region(q, p)],
        lambda q, p, i, j: wide_kept.at[q, p, i, j],
        wide_landing,
        wide_bufs,
        wide_sems,
        wide_load,
        per,
    )

    def last_region(q, p):
        return pl.ds(pl.multiple_of((2 * q + p) * last_rows, 16), last_rows)

    last = Reducer(
        at,
        last_count,
        last_rows,
        lambda q, p: send.at[:, :, last_region(q, p), :],
        lambda q, p, i, j: keep.at[i, j, last_region(q, p), :],
        lambda q, p, k: tail.at[0, k, last_region(q, p), :],
        last_bufs,
        last_sems,
    )

    def over_y(src, dst, i):
        return pltpu.make_async_remote_copy(
            src_ref=src,
            dst_ref=dst,
            send_sem=row_sems.at[0, i],
            recv_sem=row_sems.at[1, i],
            device_id=at.over[1],
            device_id_type=MESH,
        )

    def tick_from(j, t):
        @pl.when(lax.rem(j, 2) == 1)
        def _():
            wide.tick(t + lax.div(j, 2))

    def tick_at(j, when, t):
        @pl.when(j == when)
        def _():
            wide.tick(jnp.int32(t))

    flat = ((tokens, FB), lambda j: (0, j))
    column = ((feats, TB), lambda i: (0, i))
    part = ((half, TB), lambda i: (0, i))
    down_block = ((1, feats, FB), lambda j: (j // per_half, 0, j % per_half))
    gate_block = ((2, 1, feats, FB), lambda j: (0, j // per_half, 0, j % per_half))
    at.greet()

    def weight_grad(xt, dy, keep, send, rows_over_x, ticks=lambda j: None):
        quarter = feats // 4

        def body(step, xt, dy, keep, send):
            (j,) = step.index
            product = mm(xt[...], dy[...]).astype(BF)
            for n in range(2):
                where = flip(at.row if rows_over_x else at.col, n)
                for h in range(2):
                    piece = product[(2 * n + h) * quarter : (2 * n + h + 1) * quarter]

                    def put(ref, where=where, piece=piece):
                        if rows_over_x:
                            ref[where, 0] = piece
                        else:
                            ref[0, where] = piece

                    place(keep, send, at.core, h, put)
            ticks(j)

        def across(j):
            other = at.col if rows_over_x else at.row
            return jnp.where(j // per_half == other, 0, 1)

        if rows_over_x:
            block = ((2, 1, quarter, FB), lambda j: (0, across(j), 0, j % per_half))
        else:
            block = ((1, 2, quarter, FB), lambda j: (across(j), 0, 0, j % per_half))
        pipe(body, (units // FB,), [((feats, tokens), lambda j: (0, 0)), flat], [block, block])(xt, dy, keep, send)

    weight_grad(a["go_t"], a["hidden"], sources[0], sources[1], False)
    wide.begin(range(per))

    steps = tokens // TB

    def y_copy(i):
        lanes = pl.ds(pl.multiple_of(i * TB, TB), TB)
        return over_y(y_send.at[:, lanes], y_came.at[:, lanes], i)


    def feed_forward(total, hold):
        total[...] = jnp.zeros_like(total)

        def down(step, hidden, by_gate, by_up, w, go, d_gate, d_up):
            (j,) = step.index
            back = mm(go[...], w[0])
            d_gate[...] = (back * by_gate[...].astype(F32)).astype(BF)
            d_up[...] = (back * by_up[...].astype(F32)).astype(BF)
            total[...] += mm_nt(w[0], hidden[...])
            tick_from(j, 0)

        pipe(
            down, (units // FB,), [flat, flat, flat, down_block, ((tokens, feats), lambda j: (0, 0))], [flat, flat]
        )(a["hidden"], a["by_gate"], a["by_up"], a["down_w"], a["go"], d_gate, d_up)

        def result(step, middle, y_keep, y_send):
            (i,) = step.index
            hold[...] = middle[...] + total[:, pl.ds(pl.multiple_of(i * TB, TB), TB)]
            y_keep[...] = hold[pl.ds(pl.multiple_of(at.col * half, 16), half), :].astype(BF)
            y_send[...] = hold[pl.ds(pl.multiple_of((1 - at.col) * half, 16), half), :].astype(BF)

        pipe(result, (tokens // TB,), [column], [part, part])(a["middle"], y_keep, y_send)
        y_copy(0).start()

        weight_grad(a["n2t"], d_gate, sources[2], sources[3], True, lambda j: tick_at(j, 2, 2))
        wide.begin(range(per, 2 * per))
        weight_grad(a["n2t"], d_up, sources[4], sources[5], True, lambda j: tick_from(j, 3))
        wide.begin(range(2 * per, 3 * per))

        total[...] = jnp.zeros_like(total)

        def feed(step, d_gate, d_up, w):
            (j,) = step.index
            total[...] += mm_nt(w[0, 0], d_gate[...]) + mm_nt(w[1, 0], d_up[...])
            tick_from(j, 5)

        pipe(feed, (units // FB,), [flat, flat, gate_block], [])(d_gate, d_up, a["gate_up"])
        d_gain_two[...] = jnp.zeros_like(d_gain_two)
        d_gain_one[...] = jnp.zeros_like(d_gain_one)

        def second_norm(step, middle, go_t, d_middle):
            (i,) = step.index
            here = pl.ds(pl.multiple_of(i * TB, TB), TB)
            m, u = middle[...], total[:, here]
            scale = lax.rsqrt(jnp.sum(m * m, axis=0, keepdims=True) / feats + EPS)
            weighted = u * gain_two[...]
            inner = jnp.sum(weighted * m, axis=0, keepdims=True) / feats
            out = go_t[...].astype(F32) + (scale * weighted - m * (scale * scale * scale * inner))
            d_middle[...] = out
            d_branch[:, here] = out.astype(BF)
            d_gain_two[...] += jnp.sum(u * m * scale, axis=1, keepdims=True)
            tick_at(i, tokens // TB - 1, 7)

        pipe(second_norm, (tokens // TB,), [column, column], [column])(a["middle"], a["go_t"], d_middle)

    pl.run_scoped(feed_forward, pltpu.VMEM((feats, tokens), F32), pltpu.VMEM((feats, TB), F32))
    third = feats // 3

    def branch(step, w):
        (i,) = step.index
        out = mm(w[0], d_branch[:half]) + mm(w[1], d_branch[half:])
        dot[pl.ds(pl.multiple_of(i * third, 16), third), :] = out.astype(BF)

    pipe(branch, (3,), [((2, third, half), lambda i: (0, i, 0))], [])(a["out_w"])

    nq, no = a["q_t"].shape[1] // 4, half // 2
    rows_of_half = ((half, tokens), lambda i: (i, 0))

    def out_weights(step, blended):
        (n,) = step.index
        where_a = jnp.where(n == 0, at.row, 1 - at.row)
        for b in range(2):
            product = mm_nt(blended[...], d_branch[b * half : (b + 1) * half]).astype(BF)
            for h in range(2):

                def put(ref, b=b, piece=product[h * no : (h + 1) * no]):
                    ref[where_a, flip(at.col, b), :no] = piece

                place(keep, send, at.core, h, put)
        tick_at(n, 1, 8)

    pipe(out_weights, (2,), [rows_of_half], [])(a["blended"])
    early = no // (2 * last_rows)
    last.begin(range(early))

    def g_copy(i):
        lanes = pl.ds(pl.multiple_of(i * TB, TB), TB)
        return over_y(g_parts.at[i], g_came.at[:, lanes], steps + i)

    def through_attention(dproj, bias, dk, dv, hold):
        fill_bias(drow, dcol, bias)

        def attention(step, qt, kt, vt, lse):
            (g,) = step.index
            part_of_dot = dot.at[pl.ds(pl.multiple_of(g * REP * HD, 16), REP * HD), :]
            attend_back_group(g, qt, kt, vt, part_of_dot, lse, cos, sin, dproj, bias, dk, dv)
            wide.tick(9 + g)

            @pl.when((g >= 1) & (g < steps))
            def _():
                y_copy(g).start()


            @pl.when(g >= KV_HEADS - early)
            def _():
                last.tick(g - (KV_HEADS - early))

        group = ((REP * HD, tokens), lambda g: (g, 0))
        single = ((HD, tokens), lambda g: (g, 0))
        pipe(
            attention,
            (KV_HEADS,),
            [group, single, single, ((1, 1, REP * tokens), lambda g: (g, 0, 0))],
            [],
        )(a["qt"], a["kt"], a["vt"], a["lse"])

        def qkv_weights(step, nt):
            (n,) = step.index
            where_a = jnp.where(n == 0, at.row, 1 - at.row)
            for b in range(2):
                product = mm_nt(dproj[b * 2 * nq : (b + 1) * 2 * nq], nt[...]).astype(BF)
                for h in range(2):

                    def put(ref, b=b, piece=product[h * nq : (h + 1) * nq]):
                        ref[where_a, flip(at.col, b), no : no + nq] = piece

                    place(keep, send, at.core, h, put)

        pipe(qkv_weights, (2,), [rows_of_half], [])(a["nt"])
        last.begin(range(early, last_count - 1))


        def first_norm(step, w, x, d_middle, g_keep):
            (i,) = step.index

            v = x[...].astype(F32)
            u = mm(w[...], dproj[:, pl.ds(pl.multiple_of(i * TB, TB), TB)])
            scale = lax.rsqrt(jnp.sum(v * v, axis=0, keepdims=True) / feats + EPS)
            weighted = u * gain_one[...]
            inner = jnp.sum(weighted * v, axis=0, keepdims=True) / feats
            d_gain_one[...] += jnp.sum(u * v * scale, axis=1, keepdims=True)
            hold[...] = d_middle[...] + (scale * weighted - v * (scale * scale * scale * inner))
            g_keep[...] = hold[pl.ds(pl.multiple_of(at.col * half, 16), half), :]
            g_parts[i] = hold[pl.ds(pl.multiple_of((1 - at.col) * half, 16), half), :].astype(BF)
            last.tick(early + i)

        pipe(first_norm, (steps,), [(a["q_t"].shape, lambda i: (0, 0)), column, column], [part])(
            a["q_t"], a["x"], d_middle, g_keep
        )

    pl.run_scoped(
        through_attention,
        pltpu.VMEM((4 * nq, tokens), BF),
        pltpu.VMEM((tokens // QB, REACH + QB, QB), F32),
        pltpu.VMEM((HD, tokens), F32),
        pltpu.VMEM((HD, tokens), F32),
        pltpu.VMEM((feats, TB), F32),
    )

    lanes = []
    for gain in (d_gain_one, d_gain_two):
        for b in range(2):
            lanes.append(jnp.broadcast_to(gain[b * half : (b + 1) * half], (half, 128)).T[:1])
    spare = keep.shape[2] - nq - no
    rows = lax.broadcasted_iota(jnp.int32, (spare, half), 0)
    gains = jnp.zeros((spare, half), F32)
    for n, lane in enumerate(lanes):
        gains = jnp.where(rows == n, lane, gains)
    gains = gains.astype(BF)
    for i in range(2):
        for j in range(2):
            keep[i, j, no + nq :] = gains
            send[i, j, no + nq :] = gains
    last.begin([last_count - 1])

    def rest(t, carry):
        last.tick(t)
        chunk = t - (last_count - 1)

        @pl.when((chunk >= 0) & (chunk < steps))
        def _():
            g_copy(chunk).start()

        return carry

    lax.fori_loop(early + steps, last.length, rest, 0)
    wide.finish()
    last.finish()
    for i in range(steps):
        y_copy(i).wait()
        g_copy(i).wait()


def back(mesh, args, smalls, wide_rows, last_rows):
    hidden, down_w, gate_up, middle, q_t = args[0], args[3], args[6], args[7], args[14]
    feats, tokens = middle.shape
    half = feats // 2
    lines = mesh.shape["dp"] // 2
    piece = (2, 2, half // 2, gate_up.shape[3])
    need = q_t.shape[1] // 4 + half // 2 + 16
    last_total = -(-need // (2 * last_rows)) * 2 * last_rows
    last_count = last_total // 2 // last_rows
    wide_count = 3 * (piece[2] // wide_rows)
    wide_unit, last_unit = (wide_rows, piece[3] // 2), (last_rows, half)
    vmem = pl.BlockSpec(memory_space=pltpu.VMEM)
    shapes = [
        (hidden.shape, BF),
        (hidden.shape, BF),
        ((feats, tokens), F32),
        ((half, tokens), BF),
        ((half, tokens), BF),
        ((half, tokens), BF),
        ((half, tokens), F32),
        ((half, tokens), BF),
        ((1, 2) + piece[2:], BF),
        ((2, 2) + piece[2:], BF),
        ((1, 2, last_total, half), BF),
    ] + [(piece, BF)] * 6
    return pl.pallas_call(
        functools.partial(
            back_body, lines=lines, wide_rows=wide_rows, last_rows=last_rows, last_count=last_count
        ),
        in_specs=[ANY] * len(args) + [vmem] * len(smalls),
        out_specs=[ANY] * len(shapes),
        out_shape=[jax.ShapeDtypeStruct(*shape) for shape in shapes],
        scratch_shapes=[
            pltpu.VMEM((feats, 1), F32),
            pltpu.VMEM((feats, 1), F32),
            pltpu.VMEM((2, 2, last_total, half), BF),
            pltpu.VMEM((2, 2, last_total, half), BF),
            pltpu.VMEM((wide_count, 2, 2, 2) + wide_unit, BF),
            pltpu.VMEM((tokens // TB, half, TB), BF),
            pltpu.VMEM((feats, tokens), BF),
            pltpu.VMEM((feats, tokens), BF),
            pltpu.SemaphoreType.DMA((wide_count, 2)),
            pltpu.SemaphoreType.DMA((2, 2 * (tokens // TB))),
        ]
        + Reducer.scratch(wide_count, wide_unit)
        + Reducer.scratch(last_count, last_unit),
        compiler_params=pltpu.CompilerParams(
            collective_id=1, has_side_effects=True, vmem_limit_bytes=63 << 20
        ),
    )(*args, *smalls)


def shards(mesh, tokens, doc_ids, norm_gain, w_qkv, w_out, ffn_gain, w_gate_up, w_down, grad_out):
    col = lax.axis_index("col")
    forwards = forward(
        *(tokens.T, grad_out.T, w_qkv.T, w_out, w_gate_up, w_down.T),
        *(doc_ids, jnp.stack((norm_gain, ffn_gain)).astype(F32)),
    )
    x, go_t, _, out_w, gate_up, down_w, nt, qt, kt, vt, blended, lse = forwards[:12]
    middle, n2t, n2, go, hidden, by_gate, by_up, q_t, gain_one, gain_two, dcol, cos, sin = forwards[12:]
    outs = back(
        mesh,
        (hidden, by_gate, by_up, down_w, go, n2t, gate_up, middle, go_t, out_w, qt, kt, vt, lse, q_t, x, nt, blended),
        (gain_one, gain_two, doc_ids, dcol, cos, sin),
        wide_rows=80,
        last_rows=48,
    )
    y_keep, _, y_came, g_keep, g_came, downs, ups, tail = outs[3:11]
    tail = tail[0]
    nq, no = w_qkv.shape[1] // 2, w_out.shape[0] // 2
    gain_rows = tail[0, nq + no : nq + no + 4].astype(F32)

    def both(own, other):
        return jnp.where(
            col == 0, jnp.concatenate((own, other), axis=1), jnp.concatenate((other, own), axis=1)
        ).T

    return (
        both(y_keep, y_came),
        both(g_keep, g_came.astype(F32)),
        gain_rows[:2].reshape(-1),
        tail[:, no : no + nq].astype(F32).reshape(2 * nq, -1).T,
        tail[:, :no].astype(F32).reshape(2 * no, -1),
        gain_rows[2:].reshape(-1),
        ups.reshape(w_gate_up.shape).astype(F32),
        downs.reshape(w_down.T.shape).astype(F32).T,
    )


def solution(mesh):
    placed = (
        P(("dp", "row"), "col"),
        P(("dp", "row", "col"), None),
        P(),
        P("row", "col"),
        P("row", "col"),
        P(),
        P(None, "row", "col"),
        P("row", "col"),
        P(("dp", "row"), "col"),
    )
    return jax.shard_map(
        functools.partial(shards, mesh),
        mesh=mesh,
        in_specs=placed,
        out_specs=(
            P(("dp", "row"), "col"),
            P(("dp", "row"), "col"),
            P(),
            P("row", "col"),
            P("row", "col"),
            P(),
            P(None, "row", "col"),
            P("row", "col"),
        ),
        check_vma=False,
    )
```

```python
import functools
import math

import jax
import jax.numpy as jnp
from jax import lax
from jax.experimental import pallas as pl
from jax.experimental.pallas import tpu as pltpu
from jax.sharding import PartitionSpec as P

HEADS = 15
KV_HEADS = 5
HD = 64
REP = HEADS // KV_HEADS
EPS = 1e-05
BF = jnp.bfloat16
F32 = jnp.float32
TB = 256
FB = 640
QB = 128
REACH = 384
MESH = pl.DeviceIdType.MESH
ANY = pl.BlockSpec(memory_space=pl.ANY)


def mm(a, b):
    return jnp.dot(a, b, preferred_element_type=F32)


def mm_nt(a, b):
    return lax.dot_general(a, b, (((1,), (1,)), ((), ())), preferred_element_type=F32)


def swap_pairs(rows):
    count = rows.shape[0]
    after = pltpu.roll(rows, count - 1, 0)
    before = pltpu.roll(rows, 1, 0)
    even = lax.broadcasted_iota(jnp.int32, rows.shape, 0) % 2 == 0
    return jnp.where(even, after, before)


def flip(bit, static):
    return bit if static == 0 else 1 - bit


def project_chunk(x, gain, w, c, s, nt, qt, kt, vt):
    feats = x.shape[0]
    v = x[...].astype(F32)
    square = jnp.sum(v * v, axis=0, keepdims=True)
    scale = lax.rsqrt(square / feats + EPS)
    normed = (v * scale * gain[...]).astype(BF)
    nt[...] = normed
    half = feats // 2
    flat = mm(w[0], normed[:half]) + mm(w[1], normed[half:])
    turned = KV_HEADS + HEADS
    for head in range(turned):
        part = flat[head * HD : (head + 1) * HD]
        part = part * c + swap_pairs(part) * s
        if head < HEADS:
            qt[head * HD : (head + 1) * HD] = (part.astype(BF).astype(F32) * HD**-0.5).astype(BF)
        else:
            kt[(head - HEADS) * HD : (head - HEADS + 1) * HD] = part.astype(BF)
    vt[...] = flat[turned * HD :].astype(BF)


def blocks(tokens):
    for i in range(tokens // QB):
        first = max(0, i - REACH // QB)
        yield i, first * QB, (i + 1 - first) * QB


def fill_bias(drow, dcol, bias):
    for i, start, extent in blocks(drow.shape[1]):
        keys = lax.broadcasted_iota(jnp.int32, (extent, QB), 0) + start
        queries = lax.broadcasted_iota(jnp.int32, (extent, QB), 1) + i * QB
        same = dcol[start : start + extent, :] == drow[:, i * QB : (i + 1) * QB]
        bias[i, :extent] = jnp.where(same & (keys <= queries), 0.0, -1e30)


def side_by_side(ref, i):
    return jnp.concatenate([ref[j * HD : (j + 1) * HD, i * QB : (i + 1) * QB] for j in range(REP)], axis=1)


def attend_group(qt, kt, vt, out, lse, bias):
    keys = kt[...].T
    for i, start, extent in blocks(kt.shape[1]):
        scores = mm(keys[start : start + extent], side_by_side(qt, i))
        scores = scores + jnp.concatenate([bias[i, :extent]] * REP, axis=1)
        top = jnp.max(scores, axis=0, keepdims=True)
        raised = jnp.exp(scores - top)
        total = jnp.sum(raised, axis=0, keepdims=True)
        shares = (raised * (1.0 / total)).astype(BF)
        blended = mm(vt[:, start : start + extent], shares).astype(BF)
        for j in range(REP):
            out[j * HD : (j + 1) * HD, i * QB : (i + 1) * QB] = blended[:, j * QB : (j + 1) * QB]
        lse[0, :, i * REP * QB : (i + 1) * REP * QB] = top + jnp.log(total)


def attend_back_group(group, qt, kt, vt, dot, lse, cos, sin, out, bias, dk, dv):
    keys, values = kt[...].T, vt[...].T
    dk[...] = jnp.zeros_like(dk)
    dv[...] = jnp.zeros_like(dv)
    base = group * REP * HD
    for i, start, extent in blocks(kt.shape[1]):
        span = slice(start, start + extent)
        lanes = slice(i * QB, (i + 1) * QB)
        queries, upper = side_by_side(qt, i), side_by_side(dot, i)
        scores = mm(keys[span], queries)
        scores = scores + jnp.concatenate([bias[i, :extent]] * REP, axis=1)
        shares = jnp.exp(scores - lse[0, :, i * REP * QB : (i + 1) * REP * QB])
        dp = mm(values[span], upper)
        inner = jnp.sum(shares * dp, axis=0, keepdims=True)
        ds = (shares * (dp - inner)).astype(BF)
        dq = mm(kt[:, span], ds) * HD**-0.5
        dk[:, span] += mm_nt(queries, ds)
        dv[:, span] += mm_nt(upper, shares.astype(BF))
        c, s = cos[:, lanes], sin[:, lanes]
        for j in range(REP):
            part = dq[:, j * QB : (j + 1) * QB]
            part = part * c - swap_pairs(part) * s
            out[pl.ds(pl.multiple_of(base + j * HD, HD), HD), lanes] = part.astype(BF)
    part = dk[...]
    part = part * cos[...] - swap_pairs(part) * sin[...]
    out[pl.ds(pl.multiple_of((HEADS + group) * HD, HD), HD), :] = part.astype(BF)
    out[pl.ds(pl.multiple_of((HEADS + KV_HEADS + group) * HD, HD), HD), :] = dv[...].astype(BF)


def gate_chunk(n, w, hidden, by_gate, by_up):
    gate = mm(n[...], w[0, 0])
    up = mm(n[...], w[1, 0])
    sig = 1.0 / (1.0 + jnp.exp(-gate))
    act = gate * sig
    hidden[...] = (act * up).astype(BF)
    by_gate[...] = (up * sig * (1.0 + gate * (1.0 - sig))).astype(BF)
    by_up[...] = act.astype(BF)


def place(keep, send, core, h, put):
    @pl.when(core == h)
    def _():
        put(keep)

    @pl.when(core != h)
    def _():
        put(send)


def greet(devices):
    barrier = pltpu.get_barrier_semaphore()
    for device in devices:
        pl.semaphore_signal(barrier, inc=1, device_id=device, device_id_type=MESH)
    pl.semaphore_wait(barrier, len(devices))


def pipe(body, grid, ins, outs):
    return pltpu.emit_pipeline(
        body,
        grid=grid,
        in_specs=[pl.BlockSpec(*spec) for spec in ins],
        out_specs=[pl.BlockSpec(*spec) for spec in outs],
        _explicit_indices=True,
    )


def column_of(row, out):
    lanes = jnp.broadcast_to(row.astype(F32), (128, row.shape[1])).T
    out[...] = lanes[:, : out.shape[1]].astype(out.dtype)


def forward_body(*refs):
    (xt, gt, wq, wo, wg, wd, doc, gain_one_row, gain_two_row), refs = refs[:9], refs[9:]
    (x, g, q, o, gu, d, nt, qt, kt, vt, blended, lse, middle, n2t, n2, go_n, hidden, by_gate, by_up, q_t), refs = refs[:20], refs[20:]
    (gain_one, gain_two, dcol, cos, sin), refs = refs[:5], refs[5:]
    bx, bg, bq, bo, bw, bd, bias, turned, here, there, send, recv = refs
    row, col, dp = (lax.axis_index(name) for name in ("row", "col", "dp"))
    core = lax.rem(dp, 2)
    side = lax.rem(lax.div(dp, 2), 2)
    over_x, over_y, over_core = {"row": 1 - row}, {"col": 1 - col}, {"dp": dp + 1 - 2 * core}
    over_z = {"dp": dp + 2 - 4 * side}
    feats_all, group = x.shape
    width = xt.shape[0]
    nq, no, ng, nd = wq.shape[0] // 2, wo.shape[0] // 2, wg.shape[1] // 2, wd.shape[0] // 2

    def rows_q(k, r, c, part):
        n = nq // 2
        return q.at[r, pl.ds(pl.multiple_of(c * 2 * nq + k * nq + part * n, 8), n), :]

    def rows_o(k, r, c, part):
        return o.at[c, pl.ds(pl.multiple_of(r * 2 * no + k * no, 16), no), :]

    def rows_g(k, r, c, part):
        return gu.at[k, c, pl.ds(pl.multiple_of(r * 2 * ng + part * ng, 16), ng), :]

    def rows_d(k, r, c, part):
        return d.at[r, pl.ds(pl.multiple_of(c * 2 * nd + k * nd, 16), nd), :]

    def rows_e(k, r, c, part):
        n = nd // 2
        return d.at[r, pl.ds(pl.multiple_of(c * 2 * nd + k * nd + part * n, 8), n), :]

    def lanes(c):
        return pl.ds(pl.multiple_of(c * group, 128), group)

    def feats(c):
        return pl.ds(pl.multiple_of(c * width, 16), width)

    own = (
        (xt.at[:, lanes(col)], bx, x.at[feats(col), :]),
        (wq, bq, q.at[row, pl.ds(pl.multiple_of(col * 2 * nq, 16), 2 * nq), :]),
        (wo, bo, o.at[col, pl.ds(pl.multiple_of(row * 2 * no, 16), 2 * no), :]),
        (wg, bw, gu.at[:, col, pl.ds(pl.multiple_of(row * 2 * ng, 16), 2 * ng), :]),
        (gt.at[:, lanes(col)], bg, g.at[feats(col), :]),
        (wd, bd, d.at[row, pl.ds(pl.multiple_of(col * 2 * nd, 16), 2 * nd), :]),
    )
    loads = [pltpu.make_async_copy(a, b, here.at[i]) for i, (a, b, _) in enumerate(own)]
    stores = [pltpu.make_async_copy(b, c, there.at[i]) for i, (_, b, c) in enumerate(own)]
    for load in loads:
        load.start()

    greet((over_x, over_y, over_z, over_core))
    begun = []

    def ready(src, dst, device):
        i = len(begun)
        copy = pltpu.make_async_remote_copy(
            src_ref=src, dst_ref=dst, send_sem=send.at[i], recv_sem=recv.at[i], device_id=device, device_id_type=MESH
        )
        begun.append(copy)
        return copy

    def go(src, dst, device):
        copy = ready(src, dst, device)
        copy.start()
        return copy

    x_cell, y_cell, corner = (1 - row, col), (row, 1 - col), (1 - row, 1 - col)

    def again(at, cell, part, device):
        return go(at(core, *cell, part), at(core, *cell, part), device)

    def later(at, cell, part, device):
        return ready(at(core, *cell, part), at(core, *cell, part), device)

    def arrive(copies):
        for copy in copies:
            copy.wait_recv()

    mine_q = wq.at[pl.ds(pl.multiple_of(core * nq + side * (nq // 2), 8), nq // 2), :]
    mine_o = wo.at[pl.ds(pl.multiple_of(core * no, 16), no), :]
    mine_d = wd.at[pl.ds(pl.multiple_of(core * nd, 16), nd), :]
    mine_e = [wd.at[pl.ds(pl.multiple_of(core * nd + part * (nd // 2), 8), nd // 2), :] for part in range(2)]
    mine_g = wg.at[core, pl.ds(pl.multiple_of(side * ng, 16), ng), :]

    q_x = go(mine_q, rows_q(core, row, col, side), over_x)
    q_y = go(mine_q, rows_q(core, row, col, side), over_y)
    tok = go(xt.at[:, lanes(1 - col)], x.at[feats(col), :], over_y)
    for load, store in zip(loads, stores):
        load.wait()
        store.start()

    column_of(gain_one_row[...].astype(F32)[None, :], gain_one)
    column_of(gain_two_row[...].astype(F32)[None, :], gain_two)
    column_of(doc[...], dcol)
    rate = jnp.exp(
        (lax.broadcasted_iota(jnp.int32, (HD, 1), 0) // 2).astype(F32) * (-2.0 * math.log(10000.0) / HD)
    )
    sign = jnp.where(lax.broadcasted_iota(jnp.int32, (HD, QB), 0) % 2 == 0, -1.0, 1.0)
    for i in range(group // QB):
        span = slice(i * QB, (i + 1) * QB)
        first = jnp.sum((dcol[...] < doc[:, span]).astype(F32), axis=0, keepdims=True)
        position = (lax.broadcasted_iota(jnp.int32, (1, QB), 1) + i * QB).astype(F32) - first
        angles = rate * position
        cos[:, span] = jnp.cos(angles)
        sin[:, span] = jnp.sin(angles) * sign
    fill_bias(doc, dcol, bias)

    def share(copy, at, cell, ends):
        copy.wait_recv()
        along = again(at, cell, side, over_z)
        ends.append(again(at, cell, side, over_core))
        return along

    def hand(copy, at, cell, part, ends):
        copy.wait_recv()
        ends.append(again(at, cell, part, over_core))

    q_ends, o_ends, gx_ends, g_ends, d_ends = [], [], [], [], []
    q_y.wait_recv()
    q_c = again(rows_q, y_cell, side, over_x)
    o_x = go(mine_o, rows_o(core, row, col, 0), over_x)
    o_y = go(mine_o, rows_o(core, row, col, 0), over_y)
    g_x = go(mine_g, rows_g(core, row, col, side), over_x)
    g_y = go(mine_g, rows_g(core, row, col, side), over_y)
    q_yz = again(rows_q, y_cell, side, over_z)
    q_ends.append(again(rows_q, y_cell, side, over_core))
    q_xz = share(q_x, rows_q, x_cell, q_ends)
    q_cz = share(q_c, rows_q, corner, q_ends)
    hand(q_yz, rows_q, y_cell, 1 - side, q_ends)
    hand(q_xz, rows_q, x_cell, 1 - side, q_ends)
    hand(q_cz, rows_q, corner, 1 - side, q_ends)
    arrive(q_ends + [tok])
    stores[0].wait()
    stores[1].wait()

    column = ((feats_all, TB), lambda i: (0, i))
    qrows, krows = HEADS * HD, KV_HEADS * HD

    def project(step, x, w, nt, qt, kt, vt):
        (i,) = step.index
        here = pl.ds(pl.multiple_of(i * TB, TB), TB)
        project_chunk(x, gain_one, w, cos[:, here], sin[:, here], nt, qt, kt, vt)

    pipe(
        project,
        (group // TB,),
        [column, (q.shape, lambda i: (0, 0, 0))],
        [((n, TB), lambda i: (0, i)) for n in (feats_all, qrows, krows, krows)],
    )(x, q, nt, qt, kt, vt)

    o_y.wait_recv()
    o_c = again(rows_o, y_cell, 0, over_x)
    o_ends.append(again(rows_o, y_cell, 0, over_core))
    d_x = [go(mine_e[0], rows_e(core, row, col, 0), over_x), None]
    hand(o_x, rows_o, x_cell, 0, o_ends)
    g_xz = share(g_x, rows_g, x_cell, gx_ends)

    g_c = later(rows_g, y_cell, side, over_x)
    g_yz = later(rows_g, y_cell, side, over_z)
    g_ends.append(later(rows_g, y_cell, side, over_core))
    d_y = ready(mine_d, rows_d(core, row, col, 0), over_y)
    grads = ready(gt.at[:, lanes(1 - col)], g.at[feats(col), :], over_y)
    d_x[1] = ready(mine_e[1], rows_e(core, row, col, 1), over_x)
    o_ends.append(later(rows_o, corner, 0, over_core))
    soon = (g_c, g_yz, g_ends[-1], d_y, grads, d_x[1])

    def attend(step, qt, kt, vt, blended, lse):
        attend_group(qt, kt, vt, blended, lse, bias)

        @pl.when(step.index[0] == KV_HEADS - 2)
        def _():
            g_y.wait_recv()
            for copy in soon:
                copy.start()
            o_c.wait_recv()
            o_ends[-1].start()

    three = ((REP * HD, group), lambda i: (i, 0))
    one = ((HD, group), lambda i: (i, 0))
    pipe(
        attend,
        (KV_HEADS,),
        [three, one, one],
        [three, ((1, 1, REP * group), lambda i: (i, 0, 0))],
    )(qt, kt, vt, blended, lse)
    hand(g_xz, rows_g, x_cell, 1 - side, gx_ends)
    arrive(o_ends)
    stores[2].wait()

    def mix(step, blended, x, w, middle, nt, n):
        (i,) = step.index

        @pl.when(i == 0)
        def _():
            turned[:width] = w[0].T
            turned[width:] = w[1].T

        m = x[...].astype(F32) + mm(turned[...], blended[...])
        middle[...] = m
        scale = lax.rsqrt(jnp.sum(m * m, axis=0, keepdims=True) / feats_all + EPS)
        normed = (m * scale * gain_two[...]).astype(BF)
        nt[...] = normed
        n[...] = normed.T

    across = ((TB, feats_all), lambda i: (i, 0))
    pipe(
        mix,
        (group // TB,),
        [column, column, (o.shape, lambda i: (0, 0, 0))],
        [column, column, across],
    )(blended, x, o, middle, n2t, n2)

    g_cz = share(g_c, rows_g, corner, g_ends)
    d_y.wait_recv()
    d_c = again(rows_d, y_cell, 0, over_x)
    d_ends.append(again(rows_d, y_cell, 0, over_core))
    arrive(gx_ends)
    stores[3].wait()

    per = wg.shape[2] // FB

    def gate(step, n, w, hidden, by_gate, by_up):
        gate_chunk(n, w, hidden, by_gate, by_up)

    def gate_half(b):
        pipe(
            gate,
            (per,),
            [
                ((group, feats_all), lambda i: (0, 0)),
                ((2, 1, feats_all, FB), lambda i: (0, b, 0, i)),
            ],
            [((group, FB), lambda i: (0, b * per + i))] * 3,
        )(n2, gu, hidden, by_gate, by_up)

    def turn_q(step, q, q_t):
        q_t[...] = q[0].T

    pipe(
        turn_q,
        (2,),
        [((1,) + q.shape[1:], lambda i: (i, 0, 0))],
        [((q.shape[2], q.shape[1]), lambda i: (i, 0))],
    )(q, q_t)
    waiting = [g_yz, g_cz] + d_x
    moves = (
        later(rows_g, y_cell, 1 - side, over_core),
        later(rows_g, corner, 1 - side, over_core),
        later(rows_e, x_cell, 0, over_core),
        later(rows_e, x_cell, 1, over_core),
    )
    g_ends += moves[:2]
    d_ends += moves[2:]

    def halves(h, carry):
        gate_half(jnp.where(h == 0, col, 1 - col))

        @pl.when(h == 0)
        def _():
            for copy, move in zip(waiting, moves):
                copy.wait_recv()
                move.start()
            arrive(g_ends)

        return carry

    lax.fori_loop(0, 2, halves, 0)
    grads.wait_recv()
    stores[4].wait()

    def turn(step, g, go_n):
        go_n[...] = g[...].T

    pipe(turn, (group // TB,), [column], [across])(g, go_n)
    hand(d_c, rows_d, corner, 0, d_ends)
    arrive(d_ends)
    stores[5].wait()
    for copy in begun:
        copy.wait_send()


def forward(xt, gt, wq, wo, wg, wd, doc, gain_one, gain_two):
    width, group = xt.shape[0], xt.shape[1] // 2
    feats = 2 * width
    full = (feats, group)
    units = 2 * wg.shape[2]
    qrows, krows = HEADS * HD, KV_HEADS * HD
    shapes = (
        (full, BF),
        (full, BF),
        ((2, 2 * wq.shape[0], wq.shape[1]), BF),
        ((2, 2 * wo.shape[0], wo.shape[1]), BF),
        ((2, 2, 2 * wg.shape[1], wg.shape[2]), BF),
        ((2, 2 * wd.shape[0], wd.shape[1]), BF),
        (full, BF),
        ((qrows, group), BF),
        ((krows, group), BF),
        ((krows, group), BF),
        (full, BF),
        ((KV_HEADS, 1, REP * group), F32),
        (full, F32),
        (full, BF),
        ((group, feats), BF),
        ((group, feats), BF),
        ((group, units), BF),
        ((group, units), BF),
        ((group, units), BF),
        ((feats, 2 * wq.shape[0]), BF),
        ((feats, 1), F32),
        ((feats, 1), F32),
        ((group, QB), jnp.int32),
        ((HD, group), F32),
        ((HD, group), F32),
    )
    held = ((width, group), (width, group), wq.shape, wo.shape, wg.shape, wd.shape)
    copies = 2 + 12 + 6 + 12 + 8
    vmem = pl.BlockSpec(memory_space=pltpu.VMEM)
    return pl.pallas_call(
        forward_body,
        in_specs=[ANY] * 6 + [vmem] * 3,
        out_specs=[ANY] * 20 + [vmem] * 5,
        out_shape=[jax.ShapeDtypeStruct(*shape) for shape in shapes],
        scratch_shapes=[pltpu.VMEM(shape, BF) for shape in held]
        + [pltpu.VMEM((group // QB, REACH + QB, QB), F32), pltpu.VMEM((feats, feats), BF)]
        + [pltpu.SemaphoreType.DMA((6,))] * 2
        + [pltpu.SemaphoreType.DMA((copies,))] * 2,
        compiler_params=pltpu.CompilerParams(
            collective_id=0, has_side_effects=True, vmem_limit_bytes=62 << 20
        ),
    )(xt, gt, wq, wo, wg, wd, doc, gain_one, gain_two)


class Lines:
    def __init__(self, lines):
        row, col, dp = (lax.axis_index(name) for name in ("row", "col", "dp"))
        self.row, self.col, self.core, line = row, col, lax.rem(dp, 2), lax.div(dp, 2)
        self.over_core = {"dp": dp + 1 - 2 * self.core}
        self.over = ({"row": 1 - row}, {"col": 1 - col})
        step = jnp.where(line < lines // 2, 2, -2)
        self.inner, self.outer = {"dp": dp + step}, {"dp": dp - step}
        self.is_end = (line == 0) | (line == lines - 1)
        self.is_mid = (line == lines // 2 - 1) | (line == lines // 2)
        self.lines = lines

    def greet(self):
        barrier = pltpu.get_barrier_semaphore()
        for device in (self.over_core, *self.over) + ((self.inner,) if self.lines > 1 else ()):
            pl.semaphore_signal(barrier, inc=1, device_id=device, device_id_type=MESH)

        @pl.when(jnp.logical_not(self.is_end))
        def _():
            pl.semaphore_signal(barrier, inc=1, device_id=self.outer, device_id_type=MESH)

        pl.semaphore_wait(barrier, jnp.where(self.is_end, 3 + (self.lines > 1), 5))


class Reducer:
    BUFFERS = ((2, 2), (2,), (), (), (), ())

    def __init__(self, at, count, step, send, kept, landing, buffers, sems, load=None, apart=None):
        self.apart = apart
        self.first = lambda q, p: p
        self.step = step
        self.at, self.count, self.send, self.kept, self.landing, self.load = at, count, send, kept, landing, load
        self.near, self.came, self.met, self.joined, self.middle, self.final = buffers
        self.stores, self.sent, self.recv = sems
        self.length = count + 5

    @staticmethod
    def scratch(count, unit):
        return [pltpu.VMEM((count, 2) + size + unit, BF) for size in Reducer.BUFFERS] + [
            pltpu.SemaphoreType.DMA((count, 2)),
            pltpu.SemaphoreType.DMA((7, count, 2)),
            pltpu.SemaphoreType.DMA((7, count, 2)),
        ]

    def copy(self, stage, q, p, src, dst, device):
        return pltpu.make_async_remote_copy(
            src_ref=src,
            dst_ref=dst,
            send_sem=self.sent.at[stage, q, p],
            recv_sem=self.recv.at[stage, q, p],
            device_id=device,
            device_id_type=MESH,
        )

    def c_copy(self, q, p, src):
        return self.copy(0, q, p, src, self.near.at[q, p], self.at.over_core)

    def a_copy(self, q, p):
        axis = self.first(q, p)
        src = self.near.at[q, p, 1] if axis == 0 else self.near.at[q, p, :, 1]
        return self.copy(1, q, p, src, self.came.at[q, p], self.at.over[axis])

    def b_copy(self, q, p):
        axis = self.first(q, p)
        src = self.near.at[q, p, 0, 1] if axis == 0 else self.near.at[q, p, 1, 0]
        return self.copy(2, q, p, src, self.met.at[q, p], self.at.over[1 - axis])

    def in_copy(self, q, p):
        return self.copy(3, q, p, self.near.at[q, p, 0, 0], self.joined.at[q, p], self.at.inner)

    def mid_copy(self, q, p):
        return self.copy(4, q, p, self.near.at[q, p, 0, 0], self.middle.at[q, p], self.at.inner)

    def out_copy(self, q, p):
        return self.copy(5, q, p, self.final.at[q, p], self.final.at[q, p], self.at.outer)

    def place(self, q, p, group):
        return self.landing(q, p, self.at.core) if group is None else self.landing(q, p, self.at.core, group)

    def d_copy(self, q, p, group=None):
        return self.copy(6, q, p, self.final.at[q, p], self.place(q, p, group), self.at.over_core)

    def store(self, q, p, group=None):
        return pltpu.make_async_copy(self.final.at[q, p], self.place(q, p, group), self.stores.at[q, p])

    def begin(self, chunks):
        for q in chunks:
            for p in range(2):
                if self.load is not None:
                    self.load(q, p).start()
                self.c_copy(q, p, self.send(q, p)).start()

    def add(self, out, a, b):
        rows = out.shape[0]
        step = self.step
        if rows == step:
            out[...] = a[...] + b[...]
            return

        def some(n, carry):
            part = pl.ds(pl.multiple_of(n * step, 16), step)
            out[part, :] = a[part, :] + b[part, :]
            return carry

        lax.fori_loop(0, rows // step, some, 0)

    def sum_core(self, q):
        for p in range(2):
            if self.load is not None:
                self.load(q, p).wait()
            self.c_copy(q, p, self.near.at[q, p]).wait_recv()
            for i in ((1, 0), (1, 1)) if self.first(q, p) == 0 else ((0, 1), (1, 1)):
                near = self.near.at[(q, p) + i]
                self.add(near, self.kept(q, p, *i), near)
            self.a_copy(q, p).start()
        for p in range(2):
            for i in ((0, 0), (0, 1)) if self.first(q, p) == 0 else ((0, 0), (1, 0)):
                near = self.near.at[(q, p) + i]
                self.add(near, self.kept(q, p, *i), near)

    def sum_first(self, q):
        for p in range(2):
            self.a_copy(q, p).wait_recv()
            for j in (1, 0):
                near = self.near.at[(q, p) + ((0, j) if self.first(q, p) == 0 else (j, 0))]
                self.add(near, near, self.came.at[q, p, j])
                if j == 1:
                    self.b_copy(q, p).start()

    def sum_second(self, q):
        for p in range(2):
            self.b_copy(q, p).wait_recv()
            near = self.near.at[q, p, 0, 0]
            if self.at.lines == 1:
                self.add(self.final.at[q, p], near, self.met.at[q, p])
                self.done(q, p)
            else:
                self.add(near, near, self.met.at[q, p])

                @pl.when(self.at.is_end)
                def _():
                    (self.in_copy if self.at.lines > 2 else self.mid_copy)(q, p).start()

    def done(self, q, p):
        if self.apart is None:
            self.d_copy(q, p).start()
            self.store(q, p).start()
            return
        for group, here in ((0, q < self.apart), (None, q >= self.apart)):

            @pl.when(here)
            def _():
                self.d_copy(q, p, group).start()
                self.store(q, p, group).start()

    def sum_in(self, q):
        if self.at.lines <= 2:
            return
        for p in range(2):

            @pl.when(jnp.logical_not(self.at.is_end))
            def _():
                self.in_copy(q, p).wait_recv()
                self.add(self.near.at[q, p, 0, 0], self.near.at[q, p, 0, 0], self.joined.at[q, p])

                @pl.when(self.at.is_mid)
                def _():
                    self.mid_copy(q, p).start()

                @pl.when(jnp.logical_not(self.at.is_mid))
                def _():
                    self.in_copy(q, p).start()

    def sum_middle(self, q):
        if self.at.lines == 1:
            return
        for p in range(2):

            @pl.when(self.at.is_mid)
            def _():
                self.mid_copy(q, p).wait_recv()
                self.add(self.final.at[q, p], self.near.at[q, p, 0, 0], self.middle.at[q, p])

                @pl.when(jnp.logical_not(self.at.is_end))
                def _():
                    self.out_copy(q, p).start()

                self.done(q, p)

    def bring_out(self, q):
        if self.at.lines <= 2:
            return
        for p in range(2):

            @pl.when(jnp.logical_not(self.at.is_mid))
            def _():
                self.out_copy(q, p).wait_recv()

                @pl.when(jnp.logical_not(self.at.is_end))
                def _():
                    self.out_copy(q, p).start()

                self.done(q, p)

    def tick(self, t):
        for lag, stage in (
            (0, self.sum_core),
            (2, self.sum_second),
            (3, self.sum_in),
            (4, self.sum_middle),
            (5, self.bring_out),
            (1, self.sum_first),
        ):
            q = t - lag

            @pl.when((q >= 0) & (q < self.count))
            def _():
                stage(q)

    def finish(self):
        lines = self.at.lines

        def one(q, carry):
            for p in range(2):
                self.d_copy(q, p).wait_recv()
                self.c_copy(q, p, self.near.at[q, p]).wait_send()
                self.a_copy(q, p).wait_send()
                self.b_copy(q, p).wait_send()
                self.d_copy(q, p).wait_send()
                self.store(q, p).wait()
                if lines > 2:

                    @pl.when(jnp.logical_not(self.at.is_mid))
                    def _():
                        self.in_copy(q, p).wait_send()

                    @pl.when(jnp.logical_not(self.at.is_end))
                    def _():
                        self.out_copy(q, p).wait_send()

                if lines > 1:

                    @pl.when(self.at.is_mid)
                    def _():
                        self.mid_copy(q, p).wait_send()

            return carry

        lax.fori_loop(0, self.count, one, 0)


def back_body(*refs, lines, wide_rows, last_rows, last_count):
    names = (
        "hidden",
        "by_gate",
        "by_up",
        "down_w",
        "go",
        "n2t",
        "gate_up",
        "middle",
        "go_t",
        "out_w",
        "qt",
        "kt",
        "vt",
        "lse",
        "q_t",
        "x",
        "nt",
        "blended",
    )
    a, refs = dict(zip(names, refs)), refs[len(names) :]
    (gain_one, gain_two, drow, dcol, cos, sin), refs = refs[:6], refs[6:]
    (d_gate, d_up, d_middle, y_full, y_send, g_keep, g_came), refs = refs[:7], refs[7:]
    (downs, ups, tail), sources, refs = refs[:3], refs[3:9], refs[9:]
    (d_gain_one, d_gain_two, keep, send, wide_kept, g_parts, d_branch, dot), refs = refs[:8], refs[8:]
    wide_loads, row_sems, refs = refs[0], refs[1], refs[2:]
    wide_bufs, wide_sems, last_bufs, last_sems = refs[:6], refs[6:9], refs[9:15], refs[15:18]

    at = Lines(lines)
    feats, tokens = a["middle"].shape
    half = feats // 2
    units = a["hidden"].shape[1]
    per_half = units // 2 // FB

    wide_cols = ups.shape[3] // 2
    per = ups.shape[2] // wide_rows

    def wide_region(q, p):
        index = q % per if isinstance(q, int) else lax.rem(q, per)
        return pl.ds(pl.multiple_of(index * wide_rows, 16), wide_rows), pl.ds(p * wide_cols, wide_cols)

    def wide_load(q, p):
        if not isinstance(q, int):
            return pltpu.make_async_copy(wide_kept.at[q, p], wide_kept.at[q, p], wide_loads.at[q, p])
        return pltpu.make_async_copy(
            sources[2 * (q // per)].at[(slice(None), slice(None)) + wide_region(q, p)],
            wide_kept.at[q, p],
            wide_loads.at[q, p],
        )

    def wide_landing(q, p, k, group=None):
        if group is None:
            return ups.at[(jnp.maximum(lax.div(q, per) - 1, 0), k) + wide_region(q, p)]
        return downs.at[(0, k) + wide_region(q, p)]

    wide = Reducer(
        at,
        3 * per,
        80,
        lambda q, p: sources[2 * (q // per) + 1].at[(slice(None), slice(None)) + wide_region(q, p)],
        lambda q, p, i, j: wide_kept.at[q, p, i, j],
        wide_landing,
        wide_bufs,
        wide_sems,
        wide_load,
        per,
    )

    def last_region(q, p):
        return pl.ds(pl.multiple_of((2 * q + p) * last_rows, 16), last_rows)

    last = Reducer(
        at,
        last_count,
        last_rows,
        lambda q, p: send.at[:, :, last_region(q, p), :],
        lambda q, p, i, j: keep.at[i, j, last_region(q, p), :],
        lambda q, p, k: tail.at[0, k, last_region(q, p), :],
        last_bufs,
        last_sems,
    )

    def over_y(src, dst, i):
        return pltpu.make_async_remote_copy(
            src_ref=src,
            dst_ref=dst,
            send_sem=row_sems.at[0, i],
            recv_sem=row_sems.at[1, i],
            device_id=at.over[1],
            device_id_type=MESH,
        )

    def tick_from(j, t):
        @pl.when(lax.rem(j, 2) == 1)
        def _():
            wide.tick(t + lax.div(j, 2))

    def tick_at(j, when, t):
        @pl.when(j == when)
        def _():
            wide.tick(jnp.int32(t))

    flat = ((tokens, FB), lambda j: (0, j))
    column = ((feats, TB), lambda i: (0, i))
    part = ((half, TB), lambda i: (0, i))
    own_part = ((half, TB), lambda i: (0, at.col * (tokens // TB) + i))
    down_block = ((1, feats, FB), lambda j: (j // per_half, 0, j % per_half))
    gate_block = ((2, 1, feats, FB), lambda j: (0, j // per_half, 0, j % per_half))
    at.greet()

    def weight_grad(xt, dy, keep, send, rows_over_x, ticks=lambda j: None):
        quarter = feats // 4

        def body(step, xt, dy, keep, send):
            (j,) = step.index
            product = mm(xt[...], dy[...]).astype(BF)
            for n in range(2):
                where = flip(at.row if rows_over_x else at.col, n)
                for h in range(2):
                    piece = product[(2 * n + h) * quarter : (2 * n + h + 1) * quarter]

                    def put(ref, where=where, piece=piece):
                        if rows_over_x:
                            ref[where, 0] = piece
                        else:
                            ref[0, where] = piece

                    place(keep, send, at.core, h, put)
            ticks(j)

        def across(j):
            other = at.col if rows_over_x else at.row
            return jnp.where(j // per_half == other, 0, 1)

        if rows_over_x:
            block = ((2, 1, quarter, FB), lambda j: (0, across(j), 0, j % per_half))
        else:
            block = ((1, 2, quarter, FB), lambda j: (across(j), 0, 0, j % per_half))
        pipe(body, (units // FB,), [((feats, tokens), lambda j: (0, 0)), flat], [block, block])(xt, dy, keep, send)

    weight_grad(a["go_t"], a["hidden"], sources[0], sources[1], False)
    wide.begin(range(per))

    steps = tokens // TB

    def y_copy(i):
        lanes = pl.ds(pl.multiple_of(i * TB, TB), TB)
        there = pl.ds(pl.multiple_of(at.col * tokens + i * TB, TB), TB)
        return over_y(y_send.at[:, lanes], y_full.at[:, there], i)


    def feed_forward(total, hold):
        total[...] = jnp.zeros_like(total)

        def down(step, hidden, by_gate, by_up, w, go, d_gate, d_up):
            (j,) = step.index
            back = mm(go[...], w[0])
            d_gate[...] = (back * by_gate[...].astype(F32)).astype(BF)
            d_up[...] = (back * by_up[...].astype(F32)).astype(BF)
            total[...] += mm_nt(w[0], hidden[...])
            tick_from(j, 0)

        pipe(
            down, (units // FB,), [flat, flat, flat, down_block, ((tokens, feats), lambda j: (0, 0))], [flat, flat]
        )(a["hidden"], a["by_gate"], a["by_up"], a["down_w"], a["go"], d_gate, d_up)

        def result(step, middle, y_keep, y_send):
            (i,) = step.index
            hold[...] = middle[...] + total[:, pl.ds(pl.multiple_of(i * TB, TB), TB)]
            y_keep[...] = hold[pl.ds(pl.multiple_of(at.col * half, 16), half), :].astype(BF)
            y_send[...] = hold[pl.ds(pl.multiple_of((1 - at.col) * half, 16), half), :].astype(BF)

        pipe(result, (tokens // TB,), [column], [own_part, part])(a["middle"], y_full, y_send)
        y_copy(0).start()

        weight_grad(a["n2t"], d_gate, sources[2], sources[3], True, lambda j: tick_at(j, 2, 2))
        wide.begin(range(per, 2 * per))
        weight_grad(a["n2t"], d_up, sources[4], sources[5], True, lambda j: tick_from(j, 3))
        wide.begin(range(2 * per, 3 * per))

        total[...] = jnp.zeros_like(total)

        def feed(step, d_gate, d_up, w):
            (j,) = step.index
            total[...] += mm_nt(w[0, 0], d_gate[...]) + mm_nt(w[1, 0], d_up[...])
            tick_from(j, 5)

        pipe(feed, (units // FB,), [flat, flat, gate_block], [])(d_gate, d_up, a["gate_up"])
        d_gain_two[...] = jnp.zeros_like(d_gain_two)
        d_gain_one[...] = jnp.zeros_like(d_gain_one)

        def second_norm(step, middle, go_t, d_middle):
            (i,) = step.index
            here = pl.ds(pl.multiple_of(i * TB, TB), TB)
            m, u = middle[...], total[:, here]
            scale = lax.rsqrt(jnp.sum(m * m, axis=0, keepdims=True) / feats + EPS)
            weighted = u * gain_two[...]
            inner = jnp.sum(weighted * m, axis=0, keepdims=True) / feats
            out = go_t[...].astype(F32) + (scale * weighted - m * (scale * scale * scale * inner))
            d_middle[...] = out
            d_branch[:, here] = out.astype(BF)
            d_gain_two[...] += jnp.sum(u * m * scale, axis=1, keepdims=True)
            tick_at(i, tokens // TB - 1, 7)

        pipe(second_norm, (tokens // TB,), [column, column], [column])(a["middle"], a["go_t"], d_middle)

    pl.run_scoped(feed_forward, pltpu.VMEM((feats, tokens), F32), pltpu.VMEM((feats, TB), F32))
    third = feats // 3

    def branch(step, w):
        (i,) = step.index
        out = mm(w[0], d_branch[:half]) + mm(w[1], d_branch[half:])
        dot[pl.ds(pl.multiple_of(i * third, 16), third), :] = out.astype(BF)

    pipe(branch, (3,), [((2, third, half), lambda i: (0, i, 0))], [])(a["out_w"])

    nq, no = a["q_t"].shape[1] // 4, half // 2
    rows_of_half = ((half, tokens), lambda i: (i, 0))

    def out_weights(step, blended):
        (n,) = step.index
        where_a = jnp.where(n == 0, at.row, 1 - at.row)
        for b in range(2):
            product = mm_nt(blended[...], d_branch[b * half : (b + 1) * half]).astype(BF)
            for h in range(2):

                def put(ref, b=b, piece=product[h * no : (h + 1) * no]):
                    ref[where_a, flip(at.col, b), :no] = piece

                place(keep, send, at.core, h, put)
        tick_at(n, 1, 8)

    pipe(out_weights, (2,), [rows_of_half], [])(a["blended"])
    early = no // (2 * last_rows)
    last.begin(range(early))

    def g_copy(i):
        lanes = pl.ds(pl.multiple_of(i * TB, TB), TB)
        return over_y(g_parts.at[i], g_came.at[:, lanes], steps + i)

    def through_attention(dproj, bias, dk, dv, hold):
        fill_bias(drow, dcol, bias)

        def attention(step, qt, kt, vt, lse):
            (g,) = step.index
            part_of_dot = dot.at[pl.ds(pl.multiple_of(g * REP * HD, 16), REP * HD), :]
            attend_back_group(g, qt, kt, vt, part_of_dot, lse, cos, sin, dproj, bias, dk, dv)
            wide.tick(9 + g)

            @pl.when((g >= 1) & (g < steps))
            def _():
                y_copy(g).start()


            @pl.when(g >= KV_HEADS - early)
            def _():
                last.tick(g - (KV_HEADS - early))

        group = ((REP * HD, tokens), lambda g: (g, 0))
        single = ((HD, tokens), lambda g: (g, 0))
        pipe(
            attention,
            (KV_HEADS,),
            [group, single, single, ((1, 1, REP * tokens), lambda g: (g, 0, 0))],
            [],
        )(a["qt"], a["kt"], a["vt"], a["lse"])

        def qkv_weights(step, nt):
            (n,) = step.index
            where_a = jnp.where(n == 0, at.row, 1 - at.row)
            for b in range(2):
                product = mm_nt(dproj[b * 2 * nq : (b + 1) * 2 * nq], nt[...]).astype(BF)
                for h in range(2):

                    def put(ref, b=b, piece=product[h * nq : (h + 1) * nq]):
                        ref[where_a, flip(at.col, b), no : no + nq] = piece

                    place(keep, send, at.core, h, put)

        pipe(qkv_weights, (2,), [rows_of_half], [])(a["nt"])
        last.begin(range(early, last_count - 1))


        def first_norm(step, w, x, d_middle, g_keep):
            (i,) = step.index

            v = x[...].astype(F32)
            u = mm(w[...], dproj[:, pl.ds(pl.multiple_of(i * TB, TB), TB)])
            scale = lax.rsqrt(jnp.sum(v * v, axis=0, keepdims=True) / feats + EPS)
            weighted = u * gain_one[...]
            inner = jnp.sum(weighted * v, axis=0, keepdims=True) / feats
            d_gain_one[...] += jnp.sum(u * v * scale, axis=1, keepdims=True)
            hold[...] = d_middle[...] + (scale * weighted - v * (scale * scale * scale * inner))
            g_keep[...] = hold[pl.ds(pl.multiple_of(at.col * half, 16), half), :]
            g_parts[i] = hold[pl.ds(pl.multiple_of((1 - at.col) * half, 16), half), :].astype(BF)
            last.tick(early + i)

        pipe(first_norm, (steps,), [(a["q_t"].shape, lambda i: (0, 0)), column, column], [part])(
            a["q_t"], a["x"], d_middle, g_keep
        )

    pl.run_scoped(
        through_attention,
        pltpu.VMEM((4 * nq, tokens), BF),
        pltpu.VMEM((tokens // QB, REACH + QB, QB), F32),
        pltpu.VMEM((HD, tokens), F32),
        pltpu.VMEM((HD, tokens), F32),
        pltpu.VMEM((feats, TB), F32),
    )

    lanes = []
    for gain in (d_gain_one, d_gain_two):
        for b in range(2):
            lanes.append(jnp.broadcast_to(gain[b * half : (b + 1) * half], (half, 128)).T[:1])
    spare = keep.shape[2] - nq - no
    rows = lax.broadcasted_iota(jnp.int32, (spare, half), 0)
    gains = jnp.zeros((spare, half), F32)
    for n, lane in enumerate(lanes):
        gains = jnp.where(rows == n, lane, gains)
    gains = gains.astype(BF)
    for i in range(2):
        for j in range(2):
            keep[i, j, no + nq :] = gains
            send[i, j, no + nq :] = gains
    last.begin([last_count - 1])

    def rest(t, carry):
        last.tick(t)
        chunk = t - (last_count - 1)

        @pl.when((chunk >= 0) & (chunk < steps))
        def _():
            g_copy(chunk).start()

        return carry

    lax.fori_loop(early + steps, last.length, rest, 0)
    wide.finish()
    last.finish()
    for i in range(steps):
        y_copy(i).wait()
        g_copy(i).wait()


def back(mesh, args, smalls, wide_rows, last_rows):
    hidden, down_w, gate_up, middle, q_t = args[0], args[3], args[6], args[7], args[14]
    feats, tokens = middle.shape
    half = feats // 2
    lines = mesh.shape["dp"] // 2
    piece = (2, 2, half // 2, gate_up.shape[3])
    need = q_t.shape[1] // 4 + half // 2 + 16
    last_total = -(-need // (2 * last_rows)) * 2 * last_rows
    last_count = last_total // 2 // last_rows
    wide_count = 3 * (piece[2] // wide_rows)
    wide_unit, last_unit = (wide_rows, piece[3] // 2), (last_rows, half)
    vmem = pl.BlockSpec(memory_space=pltpu.VMEM)
    shapes = [
        (hidden.shape, BF),
        (hidden.shape, BF),
        ((feats, tokens), F32),
        ((half, 2 * tokens), BF),
        ((half, tokens), BF),
        ((half, tokens), F32),
        ((half, tokens), BF),
        ((1, 2) + piece[2:], BF),
        ((2, 2) + piece[2:], BF),
        ((1, 2, last_total, half), BF),
    ] + [(piece, BF)] * 6
    return pl.pallas_call(
        functools.partial(
            back_body, lines=lines, wide_rows=wide_rows, last_rows=last_rows, last_count=last_count
        ),
        in_specs=[ANY] * len(args) + [vmem] * len(smalls),
        out_specs=[ANY] * len(shapes),
        out_shape=[jax.ShapeDtypeStruct(*shape) for shape in shapes],
        scratch_shapes=[
            pltpu.VMEM((feats, 1), F32),
            pltpu.VMEM((feats, 1), F32),
            pltpu.VMEM((2, 2, last_total, half), BF),
            pltpu.VMEM((2, 2, last_total, half), BF),
            pltpu.VMEM((wide_count, 2, 2, 2) + wide_unit, BF),
            pltpu.VMEM((tokens // TB, half, TB), BF),
            pltpu.VMEM((feats, tokens), BF),
            pltpu.VMEM((feats, tokens), BF),
            pltpu.SemaphoreType.DMA((wide_count, 2)),
            pltpu.SemaphoreType.DMA((2, 2 * (tokens // TB))),
        ]
        + Reducer.scratch(wide_count, wide_unit)
        + Reducer.scratch(last_count, last_unit),
        compiler_params=pltpu.CompilerParams(
            collective_id=1, has_side_effects=True, vmem_limit_bytes=63 << 20
        ),
    )(*args, *smalls)


def shards(mesh, tokens, doc_ids, norm_gain, w_qkv, w_out, ffn_gain, w_gate_up, w_down, grad_out):
    col = lax.axis_index("col")
    forwards = forward(
        *(tokens.T, grad_out.T, w_qkv.T, w_out, w_gate_up, w_down.T),
        *(doc_ids, norm_gain, ffn_gain),
    )
    x, go_t, _, out_w, gate_up, down_w, nt, qt, kt, vt, blended, lse = forwards[:12]
    middle, n2t, n2, go, hidden, by_gate, by_up, q_t, gain_one, gain_two, dcol, cos, sin = forwards[12:]
    outs = back(
        mesh,
        (hidden, by_gate, by_up, down_w, go, n2t, gate_up, middle, go_t, out_w, qt, kt, vt, lse, q_t, x, nt, blended),
        (gain_one, gain_two, doc_ids, dcol, cos, sin),
        wide_rows=80,
        last_rows=48,
    )
    y_full, _, g_keep, g_came, downs, ups, tail = outs[3:10]
    tail = tail[0]
    nq, no = w_qkv.shape[1] // 2, w_out.shape[0] // 2
    gain_rows = tail[0, nq + no : nq + no + 4].astype(F32)

    def both(own, other):
        return jnp.where(
            col == 0, jnp.concatenate((own, other), axis=1), jnp.concatenate((other, own), axis=1)
        ).T

    return (
        y_full.T,
        both(g_keep, g_came.astype(F32)),
        gain_rows[:2].reshape(-1),
        tail[:, no : no + nq].astype(F32).reshape(2 * nq, -1).T,
        tail[:, :no].astype(F32).reshape(2 * no, -1),
        gain_rows[2:].reshape(-1),
        ups.reshape(w_gate_up.shape).astype(F32),
        downs.reshape(w_down.T.shape).astype(F32).T,
    )


def solution(mesh):
    placed = (
        P(("dp", "row"), "col"),
        P(("dp", "row", "col"), None),
        P(),
        P("row", "col"),
        P("row", "col"),
        P(),
        P(None, "row", "col"),
        P("row", "col"),
        P(("dp", "row"), "col"),
    )
    return jax.shard_map(
        functools.partial(shards, mesh),
        mesh=mesh,
        in_specs=placed,
        out_specs=(
            P(("dp", "row"), "col"),
            P(("dp", "row"), "col"),
            P(),
            P("row", "col"),
            P("row", "col"),
            P(),
            P(None, "row", "col"),
            P("row", "col"),
        ),
        check_vma=False,
    )
```
